32 devices in a mesh: tm: 8 (over z, x), pair: 4 (over y, core).
Axes of the slice: x: 2, y: 2, z: 4, core: 2. Of those that a mesh axis runs over, the one named last changes fastest.
Arguments:
- voltages: bfloat16 [2, 32, 262144], P(None, 'pair', 'tm'), may hold values from -3 to 3
- delays: int32 [32, 32], P('pair', 'tm'), may hold values from 0 to 49152, as said below
- phase_model: float32 [32, 8192], replicated, may hold values from -3.140625 to 3.140625
- phase_bins: int32 [32], P('tm'), may hold values from 0 to 31
- assignment: int32 [16], P('pair'), may hold values from 0 to 15, each once
Outputs:
- visibility: float32 [32, 16, 2, 64, 128], P('tm', 'pair')
The draws below stay inside these ranges and needn't reach their ends.
Inputs may be any that keep to these rules, and one draw needn't show every extreme that they name: `delays`: delay of each station in each recording block of 1 frames; both 0 and 49152 occur in every draw. `assignment`: each of the 16 station-pair blocks occurs once.
All inputs are finite; a program needn't handle non-finite values.
Results may differ from the reference program's by a relative error of at most 0.0085.
Values may be sent and summed in bfloat16 or wider, within the bound.
A program may use at most 128 MiB of HBM per device.

```python
import math
import jax
import jax.numpy as jnp
from jax import lax

NCHAN = 8192
STATIONS = 32
GROUP_ST = 8
RADIX_A = 16
CHAVG = 64
BINS = 32
FB = 1
NGRP = 4
NBLK = 16
OUTCH = 128
FRAMES = 32
BLOCKS = 32
SAMPLES = 262144
DELAY_MAX = 49152


def draw_delays(key, part):
    entries = STATIONS * BLOCKS
    values = jax.random.randint(jax.random.fold_in(key, 11), (entries,), 0, DELAY_MAX + 1, dtype=jnp.int32)
    highest = jax.random.randint(jax.random.fold_in(key, 12), (), 0, entries, dtype=jnp.int32)
    advance = jax.random.randint(jax.random.fold_in(key, 13), (), 1, entries, dtype=jnp.int32)
    lowest = (highest + advance) % entries
    places = jnp.arange(entries, dtype=jnp.int32)
    values = jnp.where(places == highest, DELAY_MAX, values)
    values = jnp.where(places == lowest, 0, values)
    return values.reshape(STATIONS, BLOCKS).astype(jnp.int32)


def touch_ends(values, rng, low, largest):
    extent = values.shape
    spot = [jax.random.randint(jax.random.fold_in(rng, axis), (), 0, extent[axis]) for axis in range(len(extent))]
    values = values.at[tuple(spot)].set(low)
    longest = extent.index(max(extent))
    spot[longest] = (spot[longest] + 1) % extent[longest]
    return values.at[tuple(spot)].set(largest)


def block_levels(rng, extent, split, smallest, high):
    loudness, own = 1.0, jax.random.fold_in(rng, 6)
    for position, shards_of in split:
        steps = jnp.exp(jax.random.uniform(jax.random.fold_in(own, position), (shards_of,), jnp.float32, smallest / len(split), high / len(split)))
        loudness = loudness * jnp.repeat(steps, extent[position] // shards_of).reshape([-1 if axis == position else 1 for axis in range(len(extent))])
    return loudness


def gaussian(rng, extent, deviation, limit, split=(), kind=jnp.bfloat16):
    values = jax.random.normal(rng, extent, jnp.float32) * deviation
    if len(split) > 0:
        values = block_levels(rng, extent, split, -0.22, 0.18) * values
    return jnp.clip(values, min=-limit, max=limit).astype(kind)


def setup_inputs(seed: int = 0) -> dict:
    keys = jax.random.split(jax.random.key(seed), 6)
    voltages = gaussian(keys[0], (2, STATIONS, SAMPLES), 0.5, 3.0, ((1, 4), (2, 8)))
    delays = draw_delays(jax.random.fold_in(keys[5], 71), 0)
    phase_model = jnp.clip(jax.random.uniform(keys[2], (STATIONS, NCHAN), jnp.float32, -3.140625, 3.140625), -3.140625, 3.140625)
    phase_bins = touch_ends(jax.random.randint(keys[3], (FRAMES,), 0, BINS), jax.random.fold_in(keys[3], 1), 0, BINS - 1).astype(jnp.int32)
    assignment = jax.random.permutation(keys[4], NBLK).astype(jnp.int32)
    return {"voltages": voltages, "delays": delays, "phase_model": phase_model, "phase_bins": phase_bins, "assignment": assignment}


def dft_tables(radix_small, radix_large):
    index_small = jnp.arange(radix_small, dtype=jnp.int32)
    index_large = jnp.arange(radix_large, dtype=jnp.int32)
    small_turns = index_small[:, None] * index_small[None, :] % radix_small
    small_angle = small_turns.astype(jnp.float32) * (2.0 * math.pi / radix_small)
    small_scale = 1.0 / math.sqrt(radix_small)
    small_cos = (jnp.cos(small_angle) * small_scale).astype(jnp.bfloat16)
    small_sin = (jnp.sin(small_angle) * small_scale).astype(jnp.bfloat16)
    twist_turns = index_small[:, None] * index_large[None, :]
    twist_angle = twist_turns.astype(jnp.float32) * (2.0 * math.pi / (radix_small * radix_large))
    twist_cos = jnp.cos(twist_angle)
    twist_sin = jnp.sin(twist_angle)
    large_turns = index_large[:, None] * index_large[None, :] % radix_large
    large_angle = large_turns.astype(jnp.float32) * (2.0 * math.pi / radix_large)
    large_scale = 1.0 / math.sqrt(radix_large)
    large_cos = (jnp.cos(large_angle) * large_scale).astype(jnp.bfloat16)
    large_sin = (jnp.sin(large_angle) * large_scale).astype(jnp.bfloat16)
    return (small_cos, small_sin, twist_cos, twist_sin, large_cos, large_sin)

def reference(voltages, delays, phase_model, phase_bins, assignment):
    radix_large = NCHAN // RADIX_A
    group_width = radix_large // OUTCH
    highest = lax.Precision.HIGHEST
    small_cos, small_sin, twist_cos, twist_sin, large_cos, large_sin = dft_tables(RADIX_A, radix_large)
    small_cos = small_cos.astype(jnp.float32)
    small_sin = small_sin.astype(jnp.float32)
    large_cos = large_cos.astype(jnp.float32)
    large_sin = large_sin.astype(jnp.float32)
    padded = jnp.pad(voltages, ((0, 0), (0, 0), (0, DELAY_MAX)))
    angles = phase_model.reshape(STATIONS, radix_large, RADIX_A).transpose(0, 2, 1)
    phase_cos = jnp.cos(angles)
    phase_sin = jnp.sin(angles)

    def cut(series, offset):
        return lax.dynamic_slice_in_dim(series, offset, NCHAN, 1)

    def frame_products(frame):
        offsets = (frame * NCHAN + delays[:, frame // FB]).astype(jnp.int32)
        window = jax.vmap(cut, in_axes=(1, 0), out_axes=1)(padded, offsets)
        samples = window.astype(jnp.float32).reshape(2, STATIONS, RADIX_A, radix_large)
        first_real = jnp.einsum('kn,snm->skm', small_cos, samples[0], precision=highest) + jnp.einsum('kn,snm->skm', small_sin, samples[1], precision=highest)
        first_imag = jnp.einsum('kn,snm->skm', small_cos, samples[1], precision=highest) - jnp.einsum('kn,snm->skm', small_sin, samples[0], precision=highest)
        turned = jnp.stack([first_real * twist_cos + first_imag * twist_sin, first_imag * twist_cos - first_real * twist_sin]).astype(jnp.bfloat16)
        turned = lax.optimization_barrier(turned).astype(jnp.float32)
        chan_real = jnp.einsum('skm,mc->skc', turned[0], large_cos, precision=highest) + jnp.einsum('skm,mc->skc', turned[1], large_sin, precision=highest)
        chan_imag = jnp.einsum('skm,mc->skc', turned[1], large_cos, precision=highest) - jnp.einsum('skm,mc->skc', turned[0], large_sin, precision=highest)
        spectra = jnp.stack([chan_real * phase_cos - chan_imag * phase_sin, chan_real * phase_sin + chan_imag * phase_cos]).astype(jnp.bfloat16)
        spectra = lax.optimization_barrier(spectra).astype(jnp.float32)
        grouped = spectra.reshape(2, STATIONS, RADIX_A, OUTCH, group_width)
        gram_terms = jnp.einsum('riagq,sjagq->rsgij', grouped, grouped, precision=highest)
        real_part = gram_terms[0, 0] + gram_terms[1, 1]
        imag_part = gram_terms[1, 0] - gram_terms[0, 1]
        return jnp.stack([real_part, imag_part]) * (1.0 / CHAVG)
    products = lax.map(frame_products, jnp.arange(FRAMES, dtype=jnp.int32))
    onehot = (phase_bins[:, None] == jnp.arange(BINS, dtype=jnp.int32)[None, :]).astype(jnp.float32)
    binned = jnp.dot(onehot.T, products.reshape(FRAMES, -1), precision=highest)
    binned = binned.reshape(BINS, 2, OUTCH, STATIONS, STATIONS)

    def pick(block):
        row_start = (block // NGRP * GROUP_ST).astype(jnp.int32)
        col_start = (block % NGRP * GROUP_ST).astype(jnp.int32)
        row_band = lax.dynamic_slice_in_dim(binned, row_start, GROUP_ST, 3)
        block_tile = lax.dynamic_slice_in_dim(row_band, col_start, GROUP_ST, 4)
        return block_tile.transpose(0, 1, 3, 4, 2).reshape(BINS, 2, GROUP_ST * GROUP_ST, OUTCH)
    return jax.vmap(pick, out_axes=1)(assignment)
```

```python
import functools
import math

import jax
import jax.numpy as jnp
import numpy as np
from jax import lax
from jax.experimental import pallas as pl
from jax.experimental.pallas import tpu as pltpu
from jax.sharding import PartitionSpec as P

NCHAN = 8192
GROUP_ST = 8
RADIX_A = 16
CHAVG = 64
NGRP = 4
NBLK = 16
OUTCH = 128
BINS = 32
DELAY_MAX = 49152
LANES = 128
RADIX_B = NCHAN // RADIX_A
QUADS = RADIX_B // LANES
UNIT = NCHAN // LANES
AHEAD = DELAY_MAX // NCHAN
SLICES = GROUP_ST * GROUP_ST // 2
F32, BF16, I32 = jnp.float32, jnp.bfloat16, jnp.int32
MESH = pl.DeviceIdType.MESH


def section_tables(stations):
    a, b = np.arange(RADIX_A), np.arange(RADIX_B)
    angle = ((a[:, None] * a[None, :]) % RADIX_A).astype(np.float32) * np.float32(2.0 * math.pi / RADIX_A)
    cos_a = (np.cos(angle) * np.float32(1.0 / math.sqrt(RADIX_A))).astype(np.float32)
    sin_a = (np.sin(angle) * np.float32(1.0 / math.sqrt(RADIX_A))).astype(np.float32)
    small = np.stack([np.stack([cos_a, sin_a], 1), np.stack([-sin_a, cos_a], 1)], 0)
    first = np.einsum("st,pkrn->psktrn", np.eye(stations, dtype=np.float32), small)
    rows = 2 * stations * RADIX_A
    first = first.reshape(rows, rows)
    turn = (a[:, None] * b[None, :]).astype(np.float32) * np.float32(2.0 * math.pi / NCHAN)
    twist = np.stack([np.cos(turn), np.sin(turn)]).astype(np.float32)
    twist = np.tile(twist, (1, stations, 1))
    angle = ((b[:, None] * b[None, :]) % RADIX_B).astype(np.float32) * np.float32(2.0 * math.pi / RADIX_B)
    cos_b = (np.cos(angle) * np.float32(1.0 / math.sqrt(RADIX_B))).astype(np.float32)
    sin_b = (np.sin(angle) * np.float32(1.0 / math.sqrt(RADIX_B))).astype(np.float32)
    second = np.stack([np.stack([cos_b, -sin_b], 1), np.stack([sin_b, cos_b], 1)], 0)
    second = second.reshape(2, RADIX_B, 2, OUTCH // 2, 2, QUADS).transpose(0, 1, 5, 2, 4, 3)
    second = second.reshape(2 * RADIX_B, 2 * RADIX_B)
    return jnp.asarray(first, BF16), jnp.asarray(twist), jnp.asarray(second, BF16)


def sin_cos(x):
    turns = jnp.round(x * (2.0 / math.pi))
    r = x - turns * 1.5703125
    r = r - turns * 4.837512969970703125e-4
    r = r - turns * 7.54978995489188216e-8
    z = r * r
    s = r + r * z * ((-1.9515295891e-4 * z + 8.3321608736e-3) * z - 1.6666654611e-1)
    c = 1.0 - 0.5 * z + z * z * ((2.443315711809948e-5 * z - 1.388731625493765e-3) * z + 4.166664568298827e-2)
    size = jnp.abs(turns)
    odd = size == 1.0
    far = size == 2.0
    sine = jnp.where(odd, c, s)
    cosine = jnp.where(odd, s, c)
    sine = jnp.where(far | (turns == -1.0), -sine, sine)
    cosine = jnp.where(far | (turns == 1.0), -cosine, cosine)
    return sine, cosine


def fused_kernel(dims, delays, phase_bins, assignment, voltages, phase_model, first_hbm, twist_hbm, second_hbm, out,
                 small, first, twist, second, rxu, series, windows, turned, planes, rows, phases, phase_rows, trig,
                 tx2, rx2, gs, tscr, tx3, rx3, sums, binned, tx4, rx4, landed, rx0, heard, tables, orders,
                 load_sems, s0, r0, s1, r1, s2, r2, s3, r3, s4, r4, own_sems, unit_sems):
    owners, pairs, frames, stations, slots = dims
    devices, layers, halves = owners * pairs, owners // 2, pairs // 2
    all_frames = owners * frames
    bins_here = BINS // owners
    piece = bins_here * 4
    sk = stations * RADIX_A
    depth = (frames + AHEAD) * UNIT + 8
    tm, pair = lax.axis_index("tm"), lax.axis_index("pair")
    u, h, m, c = tm // 2, tm % 2, pair // 2, pair % 2
    me = tm * pairs + pair
    mine = 2 * m + h
    e = h * halves + m
    top = u == layers - 1

    def place_of(device):
        return (device // pairs, device % pairs)

    def remote(src, dst, send_sem, recv_sem, where):
        return pltpu.make_async_remote_copy(
            src_ref=src, dst_ref=dst, send_sem=send_sem, recv_sem=recv_sem, device_id=where, device_id_type=MESH)

    loads = [
        pltpu.make_async_copy(first_hbm, first, load_sems.at[0]),
        pltpu.make_async_copy(twist_hbm, twist, load_sems.at[1]),
        pltpu.make_async_copy(second_hbm, second, load_sems.at[2]),
        pltpu.make_async_copy(
            phase_model.at[pl.ds(pl.multiple_of(mine * stations // 8 * 8, 8), 8)], phases, load_sems.at[3]),
    ]
    for copy in loads:
        copy.start()

    lane = lax.broadcasted_iota(I32, (1, LANES), 1)
    listed, marked = jnp.zeros((1, LANES), I32), jnp.zeros((1, LANES), I32)
    for i in range(stations * frames):
        listed = jnp.where(lane == i, delays[i // frames, i % frames], listed)
    for i in range(frames):
        listed = jnp.where(lane == stations * frames + i, phase_bins[i], listed)
        marked = jnp.where(lane == tm * frames + i, phase_bins[i] + 1, marked)
    for i in range(slots):
        listed = jnp.where(lane == (stations + 1) * frames + i, assignment[i], listed)
    small[0:1] = listed
    small[1:2] = marked

    barrier = pltpu.get_barrier_semaphore()

    def greet(step, carry):
        pl.semaphore_signal(barrier, inc=1, device_id=place_of((me + step) % devices), device_id_type=MESH)
        return carry

    lax.fori_loop(1, devices, greet, 0)
    pl.semaphore_wait(barrier, devices - 1)

    def small_copy(step, peer, slot):
        return remote(small, rx0.at[slot], s0.at[step], r0.at[slot], place_of(peer))

    def start_small(step, carry):
        small_copy(step, (me + step) % devices, me).start()
        return carry

    lax.fori_loop(1, devices, start_small, 0)
    own_small = pltpu.make_async_copy(small, rx0.at[me], own_sems.at[0])
    own_small.start()

    def at(layer, half, core):
        return (2 * layer + half, 2 * m + core)

    def sample_copy(index, src, where, slot):
        return remote(src, rxu.at[slot], s1.at[index], r1.at[slot], where)

    def own_unit(i):
        return voltages.at[:, :, pl.ds(i * NCHAN, NCHAN)]

    def arrived(slot):
        sample_copy(0, rxu.at[slot], at(u, h, c), slot).wait_recv()

    below = u > 0
    lower = jnp.maximum(u - 1, 0)
    is00, is10 = (h == 0) & (c == 0), (h == 1) & (c == 0)
    is01, is11 = (h == 0) & (c == 1), (h == 1) & (c == 1)
    start_00 = [(0, 0, (lower, 0, 0), 8), (1, 1, (lower, 0, 0), 9), (2, 2, (lower, 0, 1), 6), (3, 3, (lower, 0, 1), 7)]

    @pl.when(is10)
    def _():
        for i in range(4):
            sample_copy(i, own_unit(i), at(u, 0, 0), 4 + i).start()

    @pl.when(is01)
    def _():
        for i in range(4):
            sample_copy(i, own_unit(i), at(u, 1, 0), i).start()

    @pl.when(is11)
    def _():
        for i in range(4):
            sample_copy(i, own_unit(i), at(u, 1, 0), 4 + i).start()

        @pl.when(below)
        def _():
            for i in range(2):
                sample_copy(4 + i, own_unit(i), at(lower, 1, 1), 8 + i).start()

    @pl.when(c == h)
    def _():
        for i in range(4):
            pltpu.make_async_copy(own_unit(i), rxu.at[i], unit_sems.at[i]).start()

    @pl.when(is00 & below)
    def _():
        for index, i, where, slot in start_00:
            sample_copy(index, own_unit(i), at(*where), slot).start()

    for copy in loads:
        copy.wait()

    def spread(j, carry):
        phase_rows[pl.ds(j, 8, stride=UNIT), :] = phases[:, pl.ds(pl.multiple_of(j * LANES, LANES), LANES)]
        return carry

    lax.fori_loop(0, UNIT, spread, 0)
    skip = mine * stations % 8

    def one_phase(s, carry):
        held = phase_rows[pl.ds(pl.multiple_of((skip + s) * UNIT, UNIT), UNIT), :].T
        angles = jnp.concatenate([held[:CHAVG], held[CHAVG:]], 1)
        sine, cosine = sin_cos(angles)
        here = pl.ds(pl.multiple_of(s * RADIX_A, RADIX_A), RADIX_A)
        for g in range(QUADS):
            trig[0, g, here, :] = cosine[g * RADIX_A:(g + 1) * RADIX_A]
            trig[1, g, here, :] = sine[g * RADIX_A:(g + 1) * RADIX_A]
        return carry

    lax.fori_loop(0, stations, one_phase, 0)

    own_small.wait()

    def finish_small(step, carry):
        source = (me + devices - step) % devices
        small_copy(step, source, source).wait_recv()
        return carry

    lax.fori_loop(1, devices, finish_small, 0)
    hear = pltpu.make_async_copy(rx0, heard, own_sems.at[1])
    hear.start()
    hear.wait()
    delays_at = ((2 * u + c) * pairs + 2 * m + h)

    line = rx0[0, 1:2, :]
    for t in range(1, owners):
        line = line + rx0[t * pairs, 1:2, :]
    span = jnp.broadcast_to(line, (all_frames, LANES))
    across = lax.broadcasted_iota(I32, (all_frames, LANES), 1)
    down = lax.broadcasted_iota(I32, (all_frames, LANES), 0)
    column = jnp.max(jnp.where(across == down, span, 0), 1, keepdims=True)
    found = jnp.max(jnp.where((span == column) & (across < down), across, -1), 1, keepdims=True)
    tables[0:all_frames] = jnp.broadcast_to(jnp.where(found < 0, all_frames, found), (all_frames, LANES))
    down = lax.broadcasted_iota(I32, (BINS, LANES), 0)
    across = lax.broadcasted_iota(I32, (BINS, LANES), 1)
    found = jnp.max(jnp.where(jnp.broadcast_to(line, (BINS, LANES)) == down + 1, across, -1), 1, keepdims=True)
    tables[all_frames:] = jnp.broadcast_to(jnp.where(found < 0, all_frames, found), (BINS, LANES))
    tell = pltpu.make_async_copy(tables, orders, own_sems.at[5])
    tell.start()

    def widen(slot):
        def one(j, carry):
            for r in range(2):
                held = rxu[slot, r, :, pl.ds(pl.multiple_of(j * LANES, LANES), LANES)].astype(F32)
                series[pl.ds(r * stations * depth + slot * UNIT + j, stations, stride=depth), :] = held
            return carry
        lax.fori_loop(0, UNIT, one, 0, unroll=4)

    def blank(slot):
        def one(i, carry):
            series[pl.ds(pl.multiple_of(i * depth + slot * UNIT, 8), UNIT), :] = jnp.zeros((UNIT, LANES), F32)
            return carry
        lax.fori_loop(0, 2 * stations, one, 0)

    def clear_tail(i, carry):
        series[pl.ds(pl.multiple_of(i * depth + (frames + AHEAD) * UNIT, 8), 8), :] = jnp.zeros((8, LANES), F32)
        return carry

    lax.fori_loop(0, 2 * stations, clear_tail, 0)

    @pl.when(is00)
    def _():
        for slot in range(4):
            pltpu.make_async_copy(own_unit(slot), rxu.at[slot], unit_sems.at[slot]).wait()
            widen(slot)
        for slot in range(4, 8):
            arrived(slot)
            sample_copy(4 + slot, rxu.at[slot], at(u, 0, 1), slot - 4).start()
            if slot < 6:
                @pl.when(below)
                def _(slot=slot):
                    sample_copy(slot, rxu.at[slot], at(lower, 0, 1), slot + 4).start()

                @pl.when(jnp.logical_not(top))
                def _(slot=slot):
                    arrived(slot + 4)
                    sample_copy(slot + 8, rxu.at[slot + 4], at(u, 0, 1), slot).start()
                    widen(slot + 4)
            widen(slot)

    @pl.when(is10)
    def _():
        for slot in range(4):
            arrived(slot)

            @pl.when(below)
            def _(slot=slot):
                where = at(lower, 1, 0) if slot < 2 else at(lower, 1, 1)
                sample_copy(4 + slot, rxu.at[slot], where, 8 + slot if slot < 2 else 4 + slot).start()
            if slot >= 2:
                @pl.when(jnp.logical_not(top))
                def _(slot=slot):
                    arrived(slot + 6)
                    sample_copy(slot + 6, rxu.at[slot + 6], at(u, 1, 1), slot + 2).start()
                    widen(slot + 6)
            widen(slot)
        for slot in range(4, 8):
            arrived(slot)
            widen(slot)

    @pl.when(is01)
    def _():
        for slot in range(4):
            arrived(slot)
            widen(slot)

    @pl.when(is11)
    def _():
        for slot in range(4):
            pltpu.make_async_copy(own_unit(slot), rxu.at[slot], unit_sems.at[slot]).wait()
            widen(slot)

    @pl.when((c == 1) & jnp.logical_not(top))
    def _():
        for slot in range(4, 8):
            arrived(slot)
            widen(slot)

    @pl.when((c == 1) & top)
    def _():
        for slot in range(4, 8):
            blank(slot)

    @pl.when(top)
    def _():
        for slot in range(8, 10):
            blank(slot)

    lane16 = lax.broadcasted_iota(I32, (RADIX_A, LANES), 1)
    batch = 2

    def frame_copy(j):
        where = (2 * u + j // halves, 2 * (j % halves) + c)
        return remote(tx2.at[j], rx2.at[mine], s2.at[j], r2.at[mine], where)

    def own_frame():
        return pltpu.make_async_copy(tx2.at[e], rx2.at[mine], own_sems.at[2])

    def spectra(step, carry):
        @pl.when((step == 1) & (c == 1) & jnp.logical_not(top))
        def _():
            for slot in range(8, 10):
                arrived(slot)
                widen(slot)

        def one_frame(i, inner):
            f = step * batch + i
            for s in range(stations):
                offset = f * NCHAN + heard[delays_at, 0, s * frames + f]
                row, shift = offset // LANES, offset % LANES
                for r in range(2):
                    parts = [
                        pltpu.roll(
                            series[pl.ds((r * stations + s) * depth + row + q, RADIX_A, stride=QUADS), :],
                            (LANES - shift) % LANES, 1)
                        for q in range(QUADS + 1)
                    ]
                    for q in range(QUADS):
                        cut = jnp.where(lane16 < LANES - shift, parts[q], parts[q + 1])
                        windows[(2 * s + r) * RADIX_A:(2 * s + r + 1) * RADIX_A, q * LANES:(q + 1) * LANES] = cut.astype(BF16)
            passed = jnp.dot(first[...], windows[...], preferred_element_type=F32)
            real, imag = passed[:sk], passed[sk:]
            here = pl.ds(pl.multiple_of(i * sk, sk), sk)
            turned[here, 0:RADIX_B] = (real * twist[0] + imag * twist[1]).astype(BF16)
            turned[here, RADIX_B:] = (imag * twist[0] - real * twist[1]).astype(BF16)
            return inner

        lax.fori_loop(0, batch, one_frame, 0)
        for g in range(QUADS):
            channels = jnp.dot(turned[...], second[:, g * 2 * LANES:(g + 1) * 2 * LANES], preferred_element_type=F32)
            real = channels[:, :LANES].reshape(batch, sk, LANES)
            imag = channels[:, LANES:].reshape(batch, sk, LANES)
            cosine, sine = trig[0, g], trig[1, g]
            turned_re = (real * cosine - imag * sine).reshape(batch * stations, RADIX_A, LANES)
            turned_im = (real * sine + imag * cosine).reshape(batch * stations, RADIX_A, LANES)
            planes[:, g * RADIX_A:(g + 1) * RADIX_A, :] = turned_re
            planes[:, CHAVG + g * RADIX_A:CHAVG + (g + 1) * RADIX_A, :] = turned_im

        def one_out(i, inner):
            def flip(s, deep):
                rows[pl.ds(s, OUTCH, stride=stations), :] = planes[i * stations + s].T
                return deep

            lax.fori_loop(0, stations, flip, 0, unroll=4)
            j = step * batch + i
            tx2[j] = rows[...].astype(BF16).reshape(OUTCH, stations, LANES)

            @pl.when(j == e)
            def _():
                own_frame().start()

            @pl.when(j != e)
            def _():
                frame_copy(j).start()
            return inner

        lax.fori_loop(0, batch, one_out, 0)
        return carry

    lax.fori_loop(0, frames // batch, spectra, 0)

    lane32 = lax.broadcasted_iota(I32, (pairs * stations, LANES), 1)
    half = pairs * stations // 2

    @pl.when(e < frames)
    def _():
        own_frame().wait()

        def get(step, carry):
            g = (mine + step) % pairs
            remote(rx2.at[g], rx2.at[g], s2.at[0], r2.at[g], (tm, pair)).wait_recv()
            return carry

        lax.fori_loop(1, pairs, get, 0)

        def gram(o, carry):
            row = o % 2 * (OUTCH // 2) + o // 2
            left = jnp.concatenate([rx2[g, row].astype(F32) for g in range(pairs)], 0)
            swapped = pltpu.roll(left, CHAVG, 1)
            swapped = jnp.where(lane32 < CHAVG, -swapped, swapped)
            both = jnp.concatenate([left, swapped], 0).astype(BF16)
            right = jnp.concatenate([both, both], 0)
            made = lax.dot_general(left.astype(BF16), right, (((1,), (1,)), ((), ())), preferred_element_type=F32)
            gs[pl.ds(o, half, stride=OUTCH), :] = jnp.where(lane32[:half] < CHAVG, made[:half], made[half:])
            return carry

        lax.fori_loop(0, OUTCH, gram, 0, unroll=4)

        def turn(i, carry):
            block = gs[pl.ds(pl.multiple_of(i * OUTCH, OUTCH), OUTCH), :].T * (1.0 / CHAVG)
            for upper in range(2):
                row = i + half * upper
                a, p = row // GROUP_ST, row % GROUP_ST
                for ri in range(2):
                    for b in range(NGRP):
                        top_row = upper * CHAVG + ri * 32 + b * GROUP_ST
                        tscr[pl.ds(p * 256 + ri * 128 + a * NGRP + b, GROUP_ST, stride=NBLK), :] = block[top_row:top_row + GROUP_ST]
            return carry

        lax.fori_loop(0, half, turn, 0)

        def pack(i, carry):
            p, ri = i // 2, i % 2
            held = tscr[pl.ds(pl.multiple_of(i * 128, 128), 128), :].astype(BF16).reshape(GROUP_ST, NBLK, LANES)
            tx3[pl.ds(p % 4 * GROUP_ST, GROUP_ST), p // 4 * 2 + ri] = held
            return carry

        lax.fori_loop(0, 2 * GROUP_ST, pack, 0)
        frame = tm // 2 * 2 * frames + c * frames + e

        def send(step, carry):
            d = (me + step) % SLICES

            @pl.when(d != me)
            def _():
                remote(tx3.at[d], rx3.at[frame], s3.at[d], r3.at[frame], place_of(d)).start()

            @pl.when(d == me)
            def _():
                pltpu.make_async_copy(tx3.at[d], rx3.at[frame], own_sems.at[3]).start()
            return carry

        lax.fori_loop(0, SLICES, send, 0)

    tell.wait()

    @pl.when(me < SLICES)
    def _():
        def get(f, carry):
            layer, core, j = f // (2 * frames), f // frames % 2, f % frames
            source = (2 * layer + j // halves) * pairs + 2 * (j % halves) + core

            @pl.when(source != me)
            def _():
                remote(rx3.at[f], rx3.at[f], s3.at[0], r3.at[f], (tm, pair)).wait_recv()

            @pl.when(source == me)
            def _():
                pltpu.make_async_copy(tx3.at[0], rx3.at[f], own_sems.at[3]).wait()
            return carry

        lax.fori_loop(0, all_frames, get, 0)
        sums[all_frames] = jnp.zeros((4 * NBLK, LANES), F32)

        def add(f, carry):
            sums[f] = sums[orders[f, 0]] + rx3[f].reshape(4 * NBLK, LANES).astype(F32)
            return carry

        lax.fori_loop(0, all_frames, add, 0)

        def gather(b, carry):
            binned[pl.ds(pl.multiple_of(b * 4 * NBLK, 4 * NBLK), 4 * NBLK), :] = sums[orders[all_frames + b, 0]]
            return carry

        lax.fori_loop(0, BINS, gather, 0)

        def choose(i, carry):
            q, k = i // slots, i % slots
            block = heard[q, 0, (stations + 1) * frames + k]
            held = binned[pl.ds(block, BINS * 4, stride=NBLK), :]
            tx4[:, q, k] = held.astype(BF16).reshape(owners, piece, LANES)
            return carry

        lax.fori_loop(0, pairs * slots, choose, 0)

        def send(step, carry):
            d = (me + step) % devices
            remote(tx4.at[d // pairs, d % pairs], rx4.at[me], s4.at[d], r4.at[me], place_of(d)).start()
            return carry

        lax.fori_loop(1, devices, send, 0)
        pltpu.make_async_copy(tx4.at[tm, pair], rx4.at[me], own_sems.at[4]).start()

    @pl.when(me < SLICES)
    def _():
        pltpu.make_async_copy(tx4.at[tm, pair], rx4.at[me], own_sems.at[4]).wait()

    def collect(d, carry):
        @pl.when(d != me)
        def _():
            remote(rx4.at[d], rx4.at[d], s4.at[0], r4.at[d], (tm, pair)).wait_recv()
        return carry

    lax.fori_loop(0, SLICES, collect, 0)
    landed[...] = rx4[...].reshape(landed.shape).astype(F32)
    for b in range(bins_here):
        for k in range(slots):
            for part in range(2):
                for ri in range(2):
                    held = landed[pl.ds(k * piece + b * 4 + part * 2 + ri, SLICES, stride=slots * piece), :]
                    out[b, k, ri, part * SLICES:(part + 1) * SLICES, :] = held

    def small_sent(step, carry):
        small_copy(step, (me + step) % devices, me).wait_send()
        return carry

    lax.fori_loop(1, devices, small_sent, 0)

    def sent(index):
        sample_copy(index, rxu.at[0], at(u, h, c), 0).wait_send()

    @pl.when(is00)
    def _():
        for index in range(8, 12):
            sent(index)

        @pl.when(below)
        def _():
            for index in range(6):
                sent(index)

        @pl.when(jnp.logical_not(top))
        def _():
            for index in range(12, 14):
                sent(index)

    @pl.when(is10)
    def _():
        for index in range(4):
            sent(index)

        @pl.when(below)
        def _():
            for index in range(4, 8):
                sent(index)

        @pl.when(jnp.logical_not(top))
        def _():
            for index in range(8, 10):
                sent(index)

    @pl.when(c == 1)
    def _():
        for index in range(4):
            sent(index)

    @pl.when(is11 & below)
    def _():
        for index in range(4, 6):
            sent(index)

    def frame_sent(j, carry):
        @pl.when(j != e)
        def _():
            frame_copy(j).wait_send()
        return carry

    lax.fori_loop(0, frames, frame_sent, 0)

    @pl.when(e < frames)
    def _():
        def slice_sent(d, carry):
            @pl.when(d != me)
            def _():
                remote(tx3.at[d], rx3.at[0], s3.at[d], r3.at[0], place_of(d)).wait_send()
            return carry

        lax.fori_loop(0, SLICES, slice_sent, 0)

    @pl.when(me < SLICES)
    def _():
        def sum_sent(step, carry):
            d = (me + step) % devices
            remote(tx4.at[d // pairs, d % pairs], rx4.at[me], s4.at[d], r4.at[me], place_of(d)).wait_send()
            return carry

        lax.fori_loop(1, devices, sum_sent, 0)


VMEM = pl.BlockSpec(memory_space=pltpu.VMEM)
SMEM = pl.BlockSpec(memory_space=pltpu.SMEM)
ANY = pl.BlockSpec(memory_space=pl.ANY)


def body(voltages, delays, phase_model, phase_bins, assignment):
    owners, pairs = lax.axis_size("tm"), lax.axis_size("pair")
    devices = owners * pairs
    stations, samples = voltages.shape[1], voltages.shape[2]
    frames = samples // NCHAN
    slots = assignment.shape[0]
    all_frames = owners * frames
    bins_here = BINS // owners
    piece = bins_here * 4
    sk = stations * RADIX_A
    batch = 2

    first, twist, second = section_tables(stations)
    span = (frames + AHEAD) * UNIT
    scratch = [
        pltpu.VMEM((2, LANES), I32),
        pltpu.VMEM(first.shape, BF16),
        pltpu.VMEM(twist.shape, F32),
        pltpu.VMEM(second.shape, BF16),
        pltpu.VMEM((frames + AHEAD, 2, stations, NCHAN), BF16),
        pltpu.VMEM((2 * stations * (span + 8), LANES), F32),
        pltpu.VMEM((2 * sk, RADIX_B), BF16),
        pltpu.VMEM((batch * sk, 2 * RADIX_B), BF16),
        pltpu.VMEM((batch * stations, LANES, LANES), F32),
        pltpu.VMEM((OUTCH * stations, LANES), F32),
        pltpu.VMEM((8, NCHAN), F32),
        pltpu.VMEM((8 * UNIT, LANES), F32),
        pltpu.VMEM((2, QUADS, sk, LANES), F32),
        pltpu.VMEM((frames, OUTCH, stations, LANES), BF16),
        pltpu.VMEM((pairs, OUTCH, stations, LANES), BF16),
        pltpu.VMEM((pairs * stations // 2 * OUTCH, LANES), F32),
        pltpu.VMEM((2 * pairs * stations * pairs * stations, LANES), F32),
        pltpu.VMEM((SLICES, 4, NBLK, LANES), BF16),
        pltpu.VMEM((all_frames, 4, NBLK, LANES), BF16),
        pltpu.VMEM((all_frames + 1, 4 * NBLK, LANES), F32),
        pltpu.VMEM((BINS * 4 * NBLK, LANES), F32),
        pltpu.VMEM((owners, pairs, slots, piece, LANES), BF16),
        pltpu.VMEM((SLICES, slots, piece, LANES), BF16),
        pltpu.VMEM((SLICES * slots * piece, LANES), F32),
        pltpu.VMEM((devices, 2, LANES), I32),
        pltpu.SMEM((devices, 2, LANES), I32),
        pltpu.VMEM((all_frames + BINS, LANES), I32),
        pltpu.SMEM((all_frames + BINS, LANES), I32),
        pltpu.SemaphoreType.DMA((4,)),
        pltpu.SemaphoreType.DMA((devices,)),
        pltpu.SemaphoreType.DMA((devices,)),
        pltpu.SemaphoreType.DMA((14,)),
        pltpu.SemaphoreType.DMA((frames + AHEAD,)),
        pltpu.SemaphoreType.DMA((frames,)),
        pltpu.SemaphoreType.DMA((pairs,)),
        pltpu.SemaphoreType.DMA((SLICES,)),
        pltpu.SemaphoreType.DMA((all_frames,)),
        pltpu.SemaphoreType.DMA((devices,)),
        pltpu.SemaphoreType.DMA((SLICES,)),
        pltpu.SemaphoreType.DMA((6,)),
        pltpu.SemaphoreType.DMA((4,)),
    ]
    return pl.pallas_call(
        functools.partial(fused_kernel, (owners, pairs, frames, stations, slots)),
        out_shape=jax.ShapeDtypeStruct((bins_here, slots, 2, GROUP_ST * GROUP_ST, OUTCH), F32),
        in_specs=[SMEM, SMEM, SMEM, ANY, ANY, ANY, ANY, ANY],
        out_specs=VMEM,
        scratch_shapes=scratch,
        compiler_params=pltpu.CompilerParams(
            collective_id=0, has_side_effects=True, vmem_limit_bytes=56 * 1024 * 1024),
        name="correlate",
    )(delays, phase_bins, assignment, voltages, phase_model, first, twist, second)


def solution(mesh):
    in_specs = (P(None, "pair", "tm"), P("pair", "tm"), P(), P("tm"), P("pair"))
    out_specs = P("tm", "pair", None, None, None)
    return jax.shard_map(body, mesh=mesh, in_specs=in_specs, out_specs=out_specs, check_vma=False)
```

```python
import functools
import math

import jax
import jax.numpy as jnp
import numpy as np
from jax import lax
from jax.experimental import pallas as pl
from jax.experimental.pallas import tpu as pltpu
from jax.sharding import PartitionSpec as P

NCHAN = 8192
GROUP_ST = 8
RADIX_A = 16
CHAVG = 64
NGRP = 4
NBLK = 16
OUTCH = 128
BINS = 32
DELAY_MAX = 49152
LANES = 128
RADIX_B = NCHAN // RADIX_A
QUADS = RADIX_B // LANES
UNIT = NCHAN // LANES
AHEAD = DELAY_MAX // NCHAN
SLICES = GROUP_ST * GROUP_ST // 2
F32, BF16, I32 = jnp.float32, jnp.bfloat16, jnp.int32
MESH = pl.DeviceIdType.MESH


def section_tables(stations):
    a, b = np.arange(RADIX_A), np.arange(RADIX_B)
    angle = ((a[:, None] * a[None, :]) % RADIX_A).astype(np.float32) * np.float32(2.0 * math.pi / RADIX_A)
    cos_a = (np.cos(angle) * np.float32(1.0 / math.sqrt(RADIX_A))).astype(np.float32)
    sin_a = (np.sin(angle) * np.float32(1.0 / math.sqrt(RADIX_A))).astype(np.float32)
    small = np.stack([np.stack([cos_a, sin_a], 1), np.stack([-sin_a, cos_a], 1)], 0)
    first = np.einsum("st,pkrn->psktrn", np.eye(stations, dtype=np.float32), small)
    rows = 2 * stations * RADIX_A
    first = first.reshape(rows, rows)
    turn = (a[:, None] * b[None, :]).astype(np.float32) * np.float32(2.0 * math.pi / NCHAN)
    twist = np.stack([np.cos(turn), np.sin(turn)]).astype(np.float32)
    twist = np.tile(twist, (1, stations, 1))
    angle = ((b[:, None] * b[None, :]) % RADIX_B).astype(np.float32) * np.float32(2.0 * math.pi / RADIX_B)
    cos_b = (np.cos(angle) * np.float32(1.0 / math.sqrt(RADIX_B))).astype(np.float32)
    sin_b = (np.sin(angle) * np.float32(1.0 / math.sqrt(RADIX_B))).astype(np.float32)
    second = np.stack([np.stack([cos_b, -sin_b], 1), np.stack([sin_b, cos_b], 1)], 0)
    second = second.reshape(2, RADIX_B, 2, OUTCH // 2, 2, QUADS).transpose(0, 1, 5, 2, 4, 3)
    second = second.reshape(2 * RADIX_B, 2 * RADIX_B)
    return jnp.asarray(first, BF16), jnp.asarray(twist), jnp.asarray(second, BF16)


def sin_cos(x):
    turns = jnp.round(x * (2.0 / math.pi))
    r = x - turns * 1.5703125
    r = r - turns * 4.837512969970703125e-4
    r = r - turns * 7.54978995489188216e-8
    z = r * r
    s = r + r * z * ((-1.9515295891e-4 * z + 8.3321608736e-3) * z - 1.6666654611e-1)
    c = 1.0 - 0.5 * z + z * z * ((2.443315711809948e-5 * z - 1.388731625493765e-3) * z + 4.166664568298827e-2)
    size = jnp.abs(turns)
    odd = size == 1.0
    far = size == 2.0
    sine = jnp.where(odd, c, s)
    cosine = jnp.where(odd, s, c)
    sine = jnp.where(far | (turns == -1.0), -sine, sine)
    cosine = jnp.where(far | (turns == 1.0), -cosine, cosine)
    return sine, cosine


def fused_kernel(dims, delays, phase_bins, assignment, voltages, phase_model, first_hbm, twist_hbm, second_hbm, out,
                 small, first, twist, second, rxu, series, windows, turned, planes, rows, phases, phase_rows, trig,
                 tx2, rx2, gs, tscr, tx3, rx3, sums, tx4, rx4, landed, rxd, rxb, heard, tables, orders,
                 load_sems, s0, r0, s1, r1, s2, r2, s3, r3, s4, r4, s5, own_sems, unit_sems):
    owners, pairs, frames, stations, slots = dims
    devices, layers, halves = owners * pairs, owners // 2, pairs // 2
    all_frames = owners * frames
    bins_here = BINS // owners
    sk = stations * RADIX_A
    depth = (frames + AHEAD) * UNIT + 8
    tm, pair = lax.axis_index("tm"), lax.axis_index("pair")
    u, h, m, c = tm // 2, tm % 2, pair // 2, pair % 2
    me = tm * pairs + pair
    mine = 2 * m + h
    e = jnp.where(m < 2, (h + m) % 2 * 2 + m, frames)
    top = u == layers - 1

    def place_of(device):
        return (device // pairs, device % pairs)

    def remote(src, dst, send_sem, recv_sem, where):
        return pltpu.make_async_remote_copy(
            src_ref=src, dst_ref=dst, send_sem=send_sem, recv_sem=recv_sem, device_id=where, device_id_type=MESH)

    loads = [
        pltpu.make_async_copy(first_hbm, first, load_sems.at[0]),
        pltpu.make_async_copy(twist_hbm, twist, load_sems.at[1]),
        pltpu.make_async_copy(second_hbm, second, load_sems.at[2]),
        pltpu.make_async_copy(
            phase_model.at[pl.ds(pl.multiple_of(mine * stations // 8 * 8, 8), 8)], phases, load_sems.at[3]),
    ]
    for copy in loads:
        copy.start()

    lane = lax.broadcasted_iota(I32, (1, LANES), 1)
    listed, marked = jnp.zeros((1, LANES), I32), jnp.zeros((1, LANES), I32)
    for i in range(stations * frames):
        listed = jnp.where(lane == i, delays[i // stations, i % stations], listed)
    for i in range(frames):
        marked = jnp.where(lane == tm * frames + i, phase_bins[i] + 1, marked)
    small[0] = listed
    small[1] = marked

    barrier = pltpu.get_barrier_semaphore()

    def greet(step, carry):
        pl.semaphore_signal(barrier, inc=1, device_id=place_of((me + step) % devices), device_id_type=MESH)
        return carry

    lax.fori_loop(1, devices, greet, 0, unroll=True) if devices < 64 else lax.fori_loop(1, devices, greet, 0)
    pl.semaphore_wait(barrier, devices - 1)

    def delay_copy():
        return remote(small.at[0], rxd, s0.at[0], r0.at[0], (2 * u + c, 2 * m + h))

    def own_delays():
        return pltpu.make_async_copy(small.at[0], rxd, own_sems.at[0])

    @pl.when(c == h)
    def _():
        own_delays().start()

    @pl.when(c != h)
    def _():
        delay_copy().start()

    def start_bins(step, carry):
        remote(small.at[1], rxb.at[tm], s0.at[1], r0.at[1], ((tm + step) % owners, pair)).start()
        return carry

    lax.fori_loop(1, owners, start_bins, 0)
    own_bins = pltpu.make_async_copy(small.at[1], rxb.at[tm], own_sems.at[5])
    own_bins.start()

    def at(layer, half, core):
        return (2 * layer + half, 2 * m + core)

    def sample_copy(index, src, where, slot):
        return remote(src, rxu.at[slot], s1.at[index], r1.at[slot], where)

    def own_unit(i):
        return voltages.at[:, :, pl.ds(i * NCHAN, NCHAN)]

    def arrived(slot):
        sample_copy(0, rxu.at[slot], at(u, h, c), slot).wait_recv()

    below = u > 0
    lower = jnp.maximum(u - 1, 0)
    is00, is10 = (h == 0) & (c == 0), (h == 1) & (c == 0)
    is01, is11 = (h == 0) & (c == 1), (h == 1) & (c == 1)
    start_00 = [(0, 0, (lower, 0, 0), 8), (1, 1, (lower, 0, 0), 9), (2, 2, (lower, 0, 1), 6), (3, 3, (lower, 0, 1), 7)]

    @pl.when(is10)
    def _():
        for i in range(4):
            sample_copy(i, own_unit(i), at(u, 0, 0), 4 + i).start()

    @pl.when(is01)
    def _():
        for i in range(4):
            sample_copy(i, own_unit(i), at(u, 1, 0), i).start()

    @pl.when(is11)
    def _():
        for i in range(4):
            sample_copy(i, own_unit(i), at(u, 1, 0), 4 + i).start()

        @pl.when(below)
        def _():
            for i in range(2):
                sample_copy(4 + i, own_unit(i), at(lower, 1, 1), 8 + i).start()

    @pl.when(c == h)
    def _():
        for i in range(4):
            pltpu.make_async_copy(own_unit(i), rxu.at[i], unit_sems.at[i]).start()

    @pl.when(is00 & below)
    def _():
        for index, i, where, slot in start_00:
            sample_copy(index, own_unit(i), at(*where), slot).start()

    for copy in loads:
        copy.wait()

    def spread(j, carry):
        phase_rows[pl.ds(j, 8, stride=UNIT), :] = phases[:, pl.ds(pl.multiple_of(j * LANES, LANES), LANES)]
        return carry

    lax.fori_loop(0, UNIT, spread, 0)
    skip = mine * stations % 8

    def one_phase(s, carry):
        held = phase_rows[pl.ds(pl.multiple_of((skip + s) * UNIT, UNIT), UNIT), :].T
        angles = jnp.concatenate([held[:CHAVG], held[CHAVG:]], 1)
        sine, cosine = sin_cos(angles)
        here = pl.ds(pl.multiple_of(s * RADIX_A, RADIX_A), RADIX_A)
        for g in range(QUADS):
            trig[0, g, here, :] = cosine[g * RADIX_A:(g + 1) * RADIX_A]
            trig[1, g, here, :] = sine[g * RADIX_A:(g + 1) * RADIX_A]
        return carry

    lax.fori_loop(0, stations, one_phase, 0)

    @pl.when(c == h)
    def _():
        own_delays().wait()

    @pl.when(c != h)
    def _():
        delay_copy().wait_recv()

    hear = pltpu.make_async_copy(rxd, heard, own_sems.at[1])
    hear.start()
    hear.wait()

    def widen(slot):
        def one(j, carry):
            for r in range(2):
                held = rxu[slot, r, :, pl.ds(pl.multiple_of(j * LANES, LANES), LANES)].astype(F32)
                series[pl.ds(r * stations * depth + slot * UNIT + j, stations, stride=depth), :] = held
            return carry
        lax.fori_loop(0, UNIT, one, 0, unroll=8)

    def blank(slot):
        def one(i, carry):
            series[pl.ds(pl.multiple_of(i * depth + slot * UNIT, 8), UNIT), :] = jnp.zeros((UNIT, LANES), F32)
            return carry
        lax.fori_loop(0, 2 * stations, one, 0)

    def clear_tail(i, carry):
        series[pl.ds(pl.multiple_of(i * depth + (frames + AHEAD) * UNIT, 8), 8), :] = jnp.zeros((8, LANES), F32)
        return carry

    lax.fori_loop(0, 2 * stations, clear_tail, 0)

    @pl.when(is00)
    def _():
        for slot in range(4):
            pltpu.make_async_copy(own_unit(slot), rxu.at[slot], unit_sems.at[slot]).wait()
            widen(slot)
        for slot in range(4, 8):
            arrived(slot)
            sample_copy(4 + slot, rxu.at[slot], at(u, 0, 1), slot - 4).start()
            if slot < 6:
                @pl.when(below)
                def _(slot=slot):
                    sample_copy(slot, rxu.at[slot], at(lower, 0, 1), slot + 4).start()

                @pl.when(jnp.logical_not(top))
                def _(slot=slot):
                    arrived(slot + 4)
                    sample_copy(slot + 8, rxu.at[slot + 4], at(u, 0, 1), slot).start()
                    widen(slot + 4)
            widen(slot)

    @pl.when(is10)
    def _():
        for slot in range(4):
            arrived(slot)

            @pl.when(below)
            def _(slot=slot):
                where = at(lower, 1, 0) if slot < 2 else at(lower, 1, 1)
                sample_copy(4 + slot, rxu.at[slot], where, 8 + slot if slot < 2 else 4 + slot).start()
            if slot >= 2:
                @pl.when(jnp.logical_not(top))
                def _(slot=slot):
                    arrived(slot + 6)
                    sample_copy(slot + 6, rxu.at[slot + 6], at(u, 1, 1), slot + 2).start()
                    widen(slot + 6)
            widen(slot)
        for slot in range(4, 8):
            arrived(slot)
            widen(slot)

    @pl.when(is01)
    def _():
        for slot in range(4):
            arrived(slot)
            widen(slot)

    @pl.when(is11)
    def _():
        for slot in range(4):
            pltpu.make_async_copy(own_unit(slot), rxu.at[slot], unit_sems.at[slot]).wait()
            widen(slot)

    @pl.when((c == 1) & jnp.logical_not(top))
    def _():
        for slot in range(4, 8):
            arrived(slot)
            widen(slot)

    @pl.when((c == 1) & top)
    def _():
        for slot in range(4, 8):
            blank(slot)

    @pl.when(top)
    def _():
        for slot in range(8, 10):
            blank(slot)

    lane16 = lax.broadcasted_iota(I32, (RADIX_A, LANES), 1)
    batch = 2

    def frame_copy(j):
        return remote(tx2.at[j], rx2.at[mine], s2.at[0], r2.at[0], (2 * u + (j + 1) // 2 % 2, j % 2 * 2 + c))

    def own_frame():
        return pltpu.make_async_copy(tx2.at[e], rx2.at[mine], own_sems.at[6])

    def spectra(step, carry):
        @pl.when((step == 1) & (c == 1) & jnp.logical_not(top))
        def _():
            for slot in range(8, 10):
                arrived(slot)
                widen(slot)

        def one_frame(i, inner):
            f = step * batch + i
            for s in range(stations):
                offset = f * NCHAN + heard[0, f * stations + s]
                row, shift = offset // LANES, offset % LANES
                for r in range(2):
                    parts = [
                        pltpu.roll(
                            series[pl.ds((r * stations + s) * depth + row + q, RADIX_A, stride=QUADS), :],
                            (LANES - shift) % LANES, 1)
                        for q in range(QUADS + 1)
                    ]
                    for q in range(QUADS):
                        cut = jnp.where(lane16 < LANES - shift, parts[q], parts[q + 1])
                        windows[(2 * s + r) * RADIX_A:(2 * s + r + 1) * RADIX_A, q * LANES:(q + 1) * LANES] = cut.astype(BF16)
            passed = jnp.dot(first[...], windows[...], preferred_element_type=F32)
            real, imag = passed[:sk], passed[sk:]
            here = pl.ds(pl.multiple_of(i * sk, sk), sk)
            turned[here, 0:RADIX_B] = (real * twist[0] + imag * twist[1]).astype(BF16)
            turned[here, RADIX_B:] = (imag * twist[0] - real * twist[1]).astype(BF16)
            return inner

        lax.fori_loop(0, batch, one_frame, 0)
        for g in range(QUADS):
            channels = jnp.dot(turned[...], second[:, g * 2 * LANES:(g + 1) * 2 * LANES], preferred_element_type=F32)
            real = channels[:, :LANES].reshape(batch, sk, LANES)
            imag = channels[:, LANES:].reshape(batch, sk, LANES)
            cosine, sine = trig[0, g], trig[1, g]
            turned_re = (real * cosine - imag * sine).reshape(batch * stations, RADIX_A, LANES)
            turned_im = (real * sine + imag * cosine).reshape(batch * stations, RADIX_A, LANES)
            planes[:, g * RADIX_A:(g + 1) * RADIX_A, :] = turned_re
            planes[:, CHAVG + g * RADIX_A:CHAVG + (g + 1) * RADIX_A, :] = turned_im

        def one_out(i, inner):
            def flip(s, deep):
                rows[pl.ds(s, OUTCH, stride=stations), :] = planes[i * stations + s].T
                return deep

            lax.fori_loop(0, stations, flip, 0, unroll=4)
            j = step * batch + i
            tx2[j] = rows[...].astype(BF16).reshape(OUTCH, stations, LANES)

            @pl.when(j == e)
            def _():
                own_frame().start()

            @pl.when(j != e)
            def _():
                frame_copy(j).start()
            return inner

        lax.fori_loop(0, batch, one_out, 0)
        return carry

    lax.fori_loop(0, frames // batch, spectra, 0)

    own_bins.wait()
    rest = rxb.at[pl.ds(0, owners - 1)]
    remote(rest, rest, s0.at[1], r0.at[1], (tm, pair)).wait_recv()
    line = rxb[0]
    for t in range(1, owners):
        line = line + rxb[t]
    span = jnp.broadcast_to(line, (all_frames, LANES))
    across = lax.broadcasted_iota(I32, (all_frames, LANES), 1)
    down = lax.broadcasted_iota(I32, (all_frames, LANES), 0)
    column = jnp.max(jnp.where(across == down, span, 0), 1, keepdims=True)
    found = jnp.max(jnp.where((span == column) & (across < down), across, -1), 1, keepdims=True)
    tables[0:all_frames] = jnp.broadcast_to(jnp.where(found < 0, all_frames, found), (all_frames, LANES))
    down = lax.broadcasted_iota(I32, (BINS, LANES), 0)
    across = lax.broadcasted_iota(I32, (BINS, LANES), 1)
    found = jnp.max(jnp.where(jnp.broadcast_to(line, (BINS, LANES)) == down + 1, across, -1), 1, keepdims=True)
    tables[all_frames:] = jnp.broadcast_to(jnp.where(found < 0, all_frames, found), (BINS, LANES))
    tell = pltpu.make_async_copy(tables, orders, own_sems.at[2])
    tell.start()

    lane32 = lax.broadcasted_iota(I32, (pairs * stations, LANES), 1)
    half = pairs * stations // 2

    @pl.when(e < frames)
    def _():
        own_frame().wait()

        rest = rx2.at[pl.ds(0, pairs - 1)]
        remote(rest, rest, s2.at[0], r2.at[0], (tm, pair)).wait_recv()

        def gram(o, carry):
            row = o % 2 * (OUTCH // 2) + o // 2
            left = jnp.concatenate([rx2[g, row].astype(F32) for g in range(pairs)], 0)
            swapped = pltpu.roll(left, CHAVG, 1)
            swapped = jnp.where(lane32 < CHAVG, -swapped, swapped)
            both = jnp.concatenate([left, swapped], 0).astype(BF16)
            right = jnp.concatenate([both, both], 0)
            made = lax.dot_general(left.astype(BF16), right, (((1,), (1,)), ((), ())), preferred_element_type=F32)
            gs[pl.ds(o, half, stride=OUTCH), :] = jnp.where(lane32[:half] < CHAVG, made[:half], made[half:])
            return carry

        lax.fori_loop(0, OUTCH, gram, 0, unroll=16)

        def turn(i, carry):
            block = gs[pl.ds(pl.multiple_of(i * OUTCH, OUTCH), OUTCH), :].T * (1.0 / CHAVG)
            for upper in range(2):
                row = i + half * upper
                a, p = row // GROUP_ST, row % GROUP_ST
                for ri in range(2):
                    for b in range(NGRP):
                        top_row = upper * CHAVG + ri * 32 + b * GROUP_ST
                        tscr[pl.ds(p * 256 + ri * 128 + a * NGRP + b, GROUP_ST, stride=NBLK), :] = block[top_row:top_row + GROUP_ST]
            return carry

        lax.fori_loop(0, half, turn, 0, unroll=4)

        def pack(p, carry):
            real = tscr[pl.ds(pl.multiple_of(p * 256, 256), 128), :].reshape(GROUP_ST, NBLK, LANES)
            imag = tscr[pl.ds(pl.multiple_of(p * 256 + 128, 128), 128), :].reshape(GROUP_ST, NBLK, LANES)
            q = lax.broadcasted_iota(I32, (GROUP_ST, NBLK, LANES), 0)
            ab = lax.broadcasted_iota(I32, (GROUP_ST, NBLK, LANES), 1)
            a, b = ab // NGRP, ab % NGRP
            upper = (a < b) | ((a == b) & (p <= q))
            tx3[pl.ds(p % 4 * GROUP_ST, GROUP_ST), p // 4] = jnp.where(upper, real, imag).astype(BF16)
            return carry

        lax.fori_loop(0, GROUP_ST, pack, 0, unroll=2)
        frame = tm // 2 * 2 * frames + c * frames + e

        def send(step, carry):
            d = (me + step) % SLICES

            @pl.when(d != me)
            def _():
                remote(tx3.at[d], rx3.at[frame], s3.at[0], r3.at[0], place_of(d)).start()

            @pl.when(d == me)
            def _():
                pltpu.make_async_copy(tx3.at[d], rx3.at[frame], own_sems.at[3]).start()
            return carry

        lax.fori_loop(0, SLICES, send, 0, unroll=4)

    tell.wait()

    @pl.when(me < SLICES)
    def _():
        @pl.when(e < frames)
        def _():
            pltpu.make_async_copy(tx3.at[0], rx3.at[0], own_sems.at[3]).wait()
            rest = rx3.at[pl.ds(0, all_frames - 1)]
            remote(rest, rest, s3.at[0], r3.at[0], (tm, pair)).wait_recv()

        @pl.when(e >= frames)
        def _():
            remote(rx3, rx3, s3.at[0], r3.at[0], (tm, pair)).wait_recv()

        sums[all_frames] = jnp.zeros((2 * NBLK, LANES), F32)

        def add(f, carry):
            sums[f] = sums[orders[f, 0]] + rx3[f].reshape(2 * NBLK, LANES).astype(F32)
            return carry

        lax.fori_loop(0, all_frames, add, 0)

        def gather(b, carry):
            held = sums[orders[all_frames + b, 0]].astype(BF16)
            tx4[b // bins_here, pl.ds(pl.multiple_of(b % bins_here * 2 * NBLK, 2 * NBLK), 2 * NBLK), :] = held
            return carry

        lax.fori_loop(0, BINS, gather, 0, unroll=8)

        def send(step, carry):
            t = (tm + step) % owners
            remote(tx4.at[t], rx4.at[me], s4.at[0], r4.at[me], (t, pair)).start()
            return carry

        lax.fori_loop(1, owners, send, 0)
        pltpu.make_async_copy(tx4.at[tm], rx4.at[me], own_sems.at[4]).start()

    sources = SLICES // pairs

    def pass_on(d, other):
        return remote(rx4.at[d], rx4.at[d], s5.at[0], r4.at[d], (tm, other))

    def landing(d):
        def one(i, carry):
            held = rx4[d, pl.ds(pl.multiple_of(i * NBLK, NBLK), NBLK), :].astype(F32)
            landed[pl.ds(i // 2 * NBLK * 2 * SLICES + i % 2 * SLICES + d, NBLK, stride=2 * SLICES), :] = held
            return carry

        lax.fori_loop(0, 2 * bins_here, one, 0, unroll=2 * bins_here)

    def nearest(step):
        if sources != 8:
            return (tm + step) % sources
        return (tm + step) % 2 + (tm // 2 + step // 2) % 2 * 2 + (tm // 4 + step // 4) % 2 * 4

    def first_hop(step, carry):
        i = nearest(step)
        d = i * pairs + pair

        @pl.when(d == me)
        def _():
            pltpu.make_async_copy(tx4.at[tm], rx4.at[d], own_sems.at[4]).wait()

        @pl.when(d != me)
        def _():
            remote(rx4.at[d], rx4.at[d], s4.at[0], r4.at[d], (tm, pair)).wait_recv()

        for n in range(1, halves):
            pass_on(d, (pair + 2 * n) % pairs).start()
        pass_on(d, pair + 1 - 2 * c).start()
        landing(d)
        return carry

    lax.fori_loop(0, sources, first_hop, 0)

    def second_hop(step, carry):
        i = nearest(step)
        for n in range(1, halves):
            d = i * pairs + (pair + 2 * n) % pairs
            remote(rx4.at[d], rx4.at[d], s4.at[0], r4.at[d], (tm, pair)).wait_recv()
            pass_on(d, pair + 1 - 2 * c).start()
            landing(d)
        return carry

    lax.fori_loop(0, sources, second_hop, 0)

    def third_hop(step, carry):
        i = nearest(step)
        for n in range(halves):
            d = i * pairs + (pair + 1 - 2 * c + 2 * n) % pairs
            remote(rx4.at[d], rx4.at[d], s4.at[0], r4.at[d], (tm, pair)).wait_recv()
            landing(d)
        return carry

    lax.fori_loop(0, sources, third_hop, 0)

    place = lax.broadcasted_iota(I32, (GROUP_ST, LANES), 0)
    none = jnp.zeros((GROUP_ST, LANES), I32)
    span = 2 * SLICES

    def one_bin(b, carry):
        for k in range(slots):
            block = assignment[k]
            a, bb = block // NGRP, block % NGRP
            row, column = none + a, none + bb
            ahead, within = row < column, row == column
            here = (b * NBLK + block) * span
            there = (b * NBLK + bb * NGRP + a) * span
            for p in range(GROUP_ST):
                straight = landed[pl.ds(here + p * GROUP_ST, GROUP_ST), :]
                mirrored = landed[pl.ds(there + p, GROUP_ST, stride=GROUP_ST), :]
                upper = ahead | (within & (place >= p))
                real = jnp.where(upper, straight, mirrored)
                imag = jnp.where(upper, -mirrored, straight)
                imag = jnp.where(within & (place == p), 0.0, imag)
                out[b, k, 0, p * GROUP_ST:(p + 1) * GROUP_ST, :] = real.astype(BF16)
                out[b, k, 1, p * GROUP_ST:(p + 1) * GROUP_ST, :] = imag.astype(BF16)
        return carry

    lax.fori_loop(0, bins_here, one_bin, 0)

    rest = rxb.at[pl.ds(0, owners - 1)]
    remote(rest, rest, s0.at[1], r0.at[1], (tm, pair)).wait_send()

    @pl.when(c != h)
    def _():
        delay_copy().wait_send()

    def sent(index):
        sample_copy(index, rxu.at[0], at(u, h, c), 0).wait_send()

    @pl.when(is00)
    def _():
        for index in range(8, 12):
            sent(index)

        @pl.when(below)
        def _():
            for index in range(6):
                sent(index)

        @pl.when(jnp.logical_not(top))
        def _():
            for index in range(12, 14):
                sent(index)

    @pl.when(is10)
    def _():
        for index in range(4):
            sent(index)

        @pl.when(below)
        def _():
            for index in range(4, 8):
                sent(index)

        @pl.when(jnp.logical_not(top))
        def _():
            for index in range(8, 10):
                sent(index)

    @pl.when(c == 1)
    def _():
        for index in range(4):
            sent(index)

    @pl.when(is11 & below)
    def _():
        for index in range(4, 6):
            sent(index)

    def all_sent(ref, count, sem):
        rest = ref.at[pl.ds(0, count)]
        remote(rest, rest, sem, r4.at[0], (tm, pair)).wait_send()

    @pl.when(e < frames)
    def _():
        all_sent(tx2, frames - 1, s2.at[0])

        @pl.when(me < SLICES)
        def _():
            all_sent(tx3, SLICES - 1, s3.at[0])

        @pl.when(me >= SLICES)
        def _():
            all_sent(tx3, SLICES, s3.at[0])

    @pl.when(e >= frames)
    def _():
        all_sent(tx2, frames, s2.at[0])

    @pl.when(me < SLICES)
    def _():
        all_sent(tx4, owners - 1, s4.at[0])

    all_sent(rx4, sources * (2 * halves - 1), s5.at[0])


VMEM = pl.BlockSpec(memory_space=pltpu.VMEM)
SMEM = pl.BlockSpec(memory_space=pltpu.SMEM)
ANY = pl.BlockSpec(memory_space=pl.ANY)


def body(voltages, delays, phase_model, phase_bins, assignment):
    owners, pairs = lax.axis_size("tm"), lax.axis_size("pair")
    devices = owners * pairs
    stations, samples = voltages.shape[1], voltages.shape[2]
    frames = samples // NCHAN
    slots = assignment.shape[0]
    all_frames = owners * frames
    bins_here = BINS // owners
    sk = stations * RADIX_A
    batch = 2

    first, twist, second = section_tables(stations)
    span = (frames + AHEAD) * UNIT
    scratch = [
        pltpu.VMEM((2, 1, LANES), I32),
        pltpu.VMEM(first.shape, BF16),
        pltpu.VMEM(twist.shape, F32),
        pltpu.VMEM(second.shape, BF16),
        pltpu.VMEM((frames + AHEAD, 2, stations, NCHAN), BF16),
        pltpu.VMEM((2 * stations * (span + 8), LANES), F32),
        pltpu.VMEM((2 * sk, RADIX_B), BF16),
        pltpu.VMEM((batch * sk, 2 * RADIX_B), BF16),
        pltpu.VMEM((batch * stations, LANES, LANES), F32),
        pltpu.VMEM((OUTCH * stations, LANES), F32),
        pltpu.VMEM((8, NCHAN), F32),
        pltpu.VMEM((8 * UNIT, LANES), F32),
        pltpu.VMEM((2, QUADS, sk, LANES), F32),
        pltpu.VMEM((frames, OUTCH, stations, LANES), BF16),
        pltpu.VMEM((pairs, OUTCH, stations, LANES), BF16),
        pltpu.VMEM((pairs * stations // 2 * OUTCH, LANES), F32),
        pltpu.VMEM((2 * pairs * stations * pairs * stations, LANES), F32),
        pltpu.VMEM((SLICES, 2, NBLK, LANES), BF16),
        pltpu.VMEM((all_frames, 2, NBLK, LANES), BF16),
        pltpu.VMEM((all_frames + 1, 2 * NBLK, LANES), F32),
        pltpu.VMEM((owners, bins_here * 2 * NBLK, LANES), BF16),
        pltpu.VMEM((SLICES, bins_here * 2 * NBLK, LANES), BF16),
        pltpu.VMEM((bins_here * NBLK * 2 * SLICES, LANES), F32),
        pltpu.VMEM((1, LANES), I32),
        pltpu.VMEM((owners, 1, LANES), I32),
        pltpu.SMEM((1, LANES), I32),
        pltpu.VMEM((all_frames + BINS, LANES), I32),
        pltpu.SMEM((all_frames + BINS, LANES), I32),
        pltpu.SemaphoreType.DMA((4,)),
        pltpu.SemaphoreType.DMA((2,)),
        pltpu.SemaphoreType.DMA((2,)),
        pltpu.SemaphoreType.DMA((14,)),
        pltpu.SemaphoreType.DMA((frames + AHEAD,)),
        pltpu.SemaphoreType.DMA((1,)),
        pltpu.SemaphoreType.DMA((1,)),
        pltpu.SemaphoreType.DMA((1,)),
        pltpu.SemaphoreType.DMA((1,)),
        pltpu.SemaphoreType.DMA((1,)),
        pltpu.SemaphoreType.DMA((SLICES,)),
        pltpu.SemaphoreType.DMA((1,)),
        pltpu.SemaphoreType.DMA((7,)),
        pltpu.SemaphoreType.DMA((4,)),
    ]
    result = pl.pallas_call(
        functools.partial(fused_kernel, (owners, pairs, frames, stations, slots)),
        out_shape=pltpu.VMEM((bins_here, slots, 2, GROUP_ST * GROUP_ST, OUTCH), BF16),
        in_specs=[SMEM, SMEM, SMEM, ANY, ANY, ANY, ANY, ANY],
        out_specs=VMEM,
        scratch_shapes=scratch,
        compiler_params=pltpu.CompilerParams(
            collective_id=0, has_side_effects=True, vmem_limit_bytes=56 * 1024 * 1024),
        name="correlate",
    )(delays.T, phase_bins, assignment, voltages, phase_model, first, twist, second)
    return result.astype(F32)


def solution(mesh):
    in_specs = (P(None, "pair", "tm"), P("pair", "tm"), P(), P("tm"), P("pair"))
    out_specs = P("tm", "pair", None, None, None)
    return jax.shard_map(body, mesh=mesh, in_specs=in_specs, out_specs=out_specs, check_vma=False)
```

```python
import functools
import math

import jax
import jax.numpy as jnp
import numpy as np
from jax import lax
from jax.experimental import pallas as pl
from jax.experimental.pallas import tpu as pltpu
from jax.sharding import PartitionSpec as P

NCHAN = 8192
GROUP_ST = 8
RADIX_A = 16
CHAVG = 64
NGRP = 4
NBLK = 16
OUTCH = 128
BINS = 32
DELAY_MAX = 49152
LANES = 128
RADIX_B = NCHAN // RADIX_A
QUADS = RADIX_B // LANES
UNIT = NCHAN // LANES
AHEAD = DELAY_MAX // NCHAN
SLICES = GROUP_ST * GROUP_ST // 2
PART = 32
F32, BF16, I32 = jnp.float32, jnp.bfloat16, jnp.int32
MESH = pl.DeviceIdType.MESH


def section_tables(stations):
    a, b = np.arange(RADIX_A), np.arange(RADIX_B)
    angle = ((a[:, None] * a[None, :]) % RADIX_A).astype(np.float32) * np.float32(2.0 * math.pi / RADIX_A)
    cos_a = (np.cos(angle) * np.float32(1.0 / math.sqrt(RADIX_A))).astype(np.float32)
    sin_a = (np.sin(angle) * np.float32(1.0 / math.sqrt(RADIX_A))).astype(np.float32)
    small = np.stack([np.stack([cos_a, sin_a], 1), np.stack([-sin_a, cos_a], 1)], 0)
    first = np.einsum("st,pkrn->psktrn", np.eye(stations, dtype=np.float32), small)
    rows = 2 * stations * RADIX_A
    first = first.reshape(rows, rows)
    turn = (a[:, None] * b[None, :]).astype(np.float32) * np.float32(2.0 * math.pi / NCHAN)
    twist = np.stack([np.cos(turn), np.sin(turn)]).astype(np.float32)
    twist = np.tile(twist, (1, stations, 1))
    angle = ((b[:, None] * b[None, :]) % RADIX_B).astype(np.float32) * np.float32(2.0 * math.pi / RADIX_B)
    cos_b = (np.cos(angle) * np.float32(1.0 / math.sqrt(RADIX_B))).astype(np.float32)
    sin_b = (np.sin(angle) * np.float32(1.0 / math.sqrt(RADIX_B))).astype(np.float32)
    second = np.stack([np.stack([cos_b, -sin_b], 1), np.stack([sin_b, cos_b], 1)], 0)
    second = second.reshape(2, RADIX_B, 2, OUTCH // 2, 2, QUADS).transpose(0, 1, 5, 2, 4, 3)
    second = second.reshape(2 * RADIX_B, 2 * RADIX_B)
    return jnp.asarray(first, BF16), jnp.asarray(twist), jnp.asarray(second, BF16)


def sin_cos(x):
    turns = jnp.round(x * (2.0 / math.pi))
    r = x - turns * 1.5703125
    r = r - turns * 4.837512969970703125e-4
    r = r - turns * 7.54978995489188216e-8
    z = r * r
    s = r + r * z * ((-1.9515295891e-4 * z + 8.3321608736e-3) * z - 1.6666654611e-1)
    c = 1.0 - 0.5 * z + z * z * ((2.443315711809948e-5 * z - 1.388731625493765e-3) * z + 4.166664568298827e-2)
    size = jnp.abs(turns)
    odd = size == 1.0
    far = size == 2.0
    sine = jnp.where(odd, c, s)
    cosine = jnp.where(odd, s, c)
    sine = jnp.where(far | (turns == -1.0), -sine, sine)
    cosine = jnp.where(far | (turns == 1.0), -cosine, cosine)
    return sine, cosine


def fused_kernel(dims, delays, phase_bins, assignment, voltages, phase_model, first_hbm, twist_hbm, second_hbm, out,
                 small, first, twist, second, rxu, series, windows, turned, planes, rows, phases, phase_rows, trig,
                 tx2, rx2, gs, tscr, tx3, rx3, sums, tx4, rx4, landed, rxd, rxb, heard, tables, orders,
                 load_sems, s0, r0, s1, r1, s2, r2, s3, r3, s4, r4, s5, own_sems, unit_sems, crossed):
    owners, pairs, frames, stations, slots = dims
    devices, layers, halves = owners * pairs, owners // 2, pairs // 2
    all_frames = owners * frames
    bins_here = BINS // owners
    sk = stations * RADIX_A
    depth = (frames + AHEAD) * UNIT + 8
    tm, pair = lax.axis_index("tm"), lax.axis_index("pair")
    u, h, m, c = tm // 2, tm % 2, pair // 2, pair % 2
    me = tm * pairs + pair
    mine = 2 * m + h
    e = jnp.where(m < 2, (h + m) % 2 * 2 + m, frames)
    top = u == layers - 1

    def place_of(device):
        return (device // pairs, device % pairs)

    def remote(src, dst, send_sem, recv_sem, where):
        return pltpu.make_async_remote_copy(
            src_ref=src, dst_ref=dst, send_sem=send_sem, recv_sem=recv_sem, device_id=where, device_id_type=MESH)

    loads = [
        pltpu.make_async_copy(first_hbm, first, load_sems.at[0]),
        pltpu.make_async_copy(twist_hbm, twist, load_sems.at[1]),
        pltpu.make_async_copy(second_hbm, second, load_sems.at[2]),
        pltpu.make_async_copy(
            phase_model.at[pl.ds(pl.multiple_of(mine * stations // 8 * 8, 8), 8)], phases, load_sems.at[3]),
    ]
    for copy in loads:
        copy.start()

    lane = lax.broadcasted_iota(I32, (1, LANES), 1)
    listed, marked = jnp.zeros((1, LANES), I32), jnp.zeros((1, LANES), I32)
    for i in range(stations * frames):
        listed = jnp.where(lane == i, delays[i // stations, i % stations], listed)
    for i in range(frames):
        marked = jnp.where(lane == tm * frames + i, phase_bins[i] + 1, marked)
    small[0] = listed
    small[1] = marked

    barrier = pltpu.get_barrier_semaphore()

    def greet(step, carry):
        pl.semaphore_signal(barrier, inc=1, device_id=place_of((me + step) % devices), device_id_type=MESH)
        return carry

    lax.fori_loop(1, devices, greet, 0, unroll=True) if devices < 64 else lax.fori_loop(1, devices, greet, 0)
    pl.semaphore_wait(barrier, devices - 1)

    def delay_copy():
        return remote(small.at[0], rxd, s0.at[0], r0.at[0], (2 * u + c, 2 * m + h))

    def own_delays():
        return pltpu.make_async_copy(small.at[0], rxd, own_sems.at[0])

    @pl.when(c == h)
    def _():
        own_delays().start()

    @pl.when(c != h)
    def _():
        delay_copy().start()

    def start_bins(step, carry):
        remote(small.at[1], rxb.at[tm], s0.at[1], r0.at[1], ((tm + step) % owners, pair)).start()
        return carry

    lax.fori_loop(1, owners, start_bins, 0)
    own_bins = pltpu.make_async_copy(small.at[1], rxb.at[tm], own_sems.at[5])
    own_bins.start()

    def at(layer, half, core):
        return (2 * layer + half, 2 * m + core)

    def sample_copy(group, src, where, slot, r):
        return remote(src, rxu.at[slot, r], s1.at[group], r1.at[slot, r], where)

    def own_unit(i, r):
        return voltages.at[r, :, pl.ds(i * NCHAN, NCHAN)]

    def own_copy(i, r):
        return pltpu.make_async_copy(own_unit(i, r), rxu.at[i, r], unit_sems.at[i, r])

    def arrived(slot, r):
        sample_copy(0, rxu.at[slot, r], at(u, h, c), slot, r).wait_recv()

    below = u > 0
    lower = jnp.maximum(u - 1, 0)
    is00, is10 = (h == 0) & (c == 0), (h == 1) & (c == 0)
    is01, is11 = (h == 0) & (c == 1), (h == 1) & (c == 1)
    both = [(i, r) for i in range(4) for r in range(2)]

    @pl.when(is10)
    def _():
        for i, r in both:
            sample_copy(0, own_unit(i, r), at(u, 0, 0), 4 + i, r).start()

    @pl.when(is01)
    def _():
        for i, r in both:
            sample_copy(0, own_unit(i, r), at(u, 1, 0), i, r).start()

    @pl.when(is11)
    def _():
        for i, r in both:
            sample_copy(0, own_unit(i, r), at(u, 1, 0), 4 + i, r).start()

        @pl.when(below)
        def _():
            for i, r in both[:4]:
                sample_copy(1, own_unit(i, r), at(lower, 1, 1), 8 + i, r).start()

    @pl.when(c == h)
    def _():
        for i, r in both:
            own_copy(i, r).start()

    @pl.when(is00 & below)
    def _():
        for i, r in both:
            where, slot = (at(lower, 0, 0), 8 + i) if i < 2 else (at(lower, 0, 1), 4 + i)
            sample_copy(1, own_unit(i, r), where, slot, r).start()

    for copy in loads:
        copy.wait()

    def spread(j, carry):
        phase_rows[pl.ds(j, 8, stride=UNIT), :] = phases[:, pl.ds(pl.multiple_of(j * LANES, LANES), LANES)]
        return carry

    lax.fori_loop(0, UNIT, spread, 0)
    skip = mine * stations % 8

    def one_phase(s, carry):
        held = phase_rows[pl.ds(pl.multiple_of((skip + s) * UNIT, UNIT), UNIT), :].T
        angles = jnp.concatenate([held[:CHAVG], held[CHAVG:]], 1)
        sine, cosine = sin_cos(angles)
        here = pl.ds(pl.multiple_of(s * RADIX_A, RADIX_A), RADIX_A)
        for g in range(QUADS):
            trig[0, g, here, :] = cosine[g * RADIX_A:(g + 1) * RADIX_A]
            trig[1, g, here, :] = sine[g * RADIX_A:(g + 1) * RADIX_A]
        return carry

    lax.fori_loop(0, stations, one_phase, 0)

    @pl.when(c == h)
    def _():
        own_delays().wait()

    @pl.when(c != h)
    def _():
        delay_copy().wait_recv()

    hear = pltpu.make_async_copy(rxd, heard, own_sems.at[1])
    hear.start()
    hear.wait()

    def widen(slot, r):
        def one(j, carry):
            held = rxu[slot, r, :, pl.ds(pl.multiple_of(j * LANES, LANES), LANES)].astype(F32)
            series[pl.ds(r * stations * depth + slot * UNIT + j, stations, stride=depth), :] = held
            return carry
        lax.fori_loop(0, UNIT, one, 0, unroll=16)

    def take(slot):
        for r in range(2):
            arrived(slot, r)
            widen(slot, r)

    def blank(slot):
        def one(i, carry):
            series[pl.ds(pl.multiple_of(i * depth + slot * UNIT, 8), UNIT), :] = jnp.zeros((UNIT, LANES), F32)
            return carry
        lax.fori_loop(0, 2 * stations, one, 0)

    def clear_tail(i, carry):
        series[pl.ds(pl.multiple_of(i * depth + (frames + AHEAD) * UNIT, 8), 8), :] = jnp.zeros((8, LANES), F32)
        return carry

    lax.fori_loop(0, 2 * stations, clear_tail, 0)

    def cross(slot):
        for r in range(2):
            arrived(slot, r)
            sample_copy(0, rxu.at[slot, r], at(u, 0, 1), slot - 4, r).start()
            if slot < 6:
                @pl.when(below)
                def _(slot=slot, r=r):
                    sample_copy(1, rxu.at[slot, r], at(lower, 0, 1), slot + 4, r).start()

                @pl.when(jnp.logical_not(top))
                def _(slot=slot, r=r):
                    arrived(slot + 4, r)
                    sample_copy(2, rxu.at[slot + 4, r], at(u, 0, 1), slot, r).start()
                    widen(slot + 4, r)
            widen(slot, r)

    @pl.when(c == h)
    def _():
        for i, r in both:
            own_copy(i, r).wait()
            widen(i, r)

    @pl.when(is00)
    def _():
        for slot in range(4, 7):
            cross(slot)

    @pl.when(is10)
    def _():
        for slot in range(4):
            for r in range(2):
                arrived(slot, r)

                @pl.when(below)
                def _(slot=slot, r=r):
                    where, into = (at(lower, 1, 0), 8 + slot) if slot < 2 else (at(lower, 1, 1), 4 + slot)
                    sample_copy(1, rxu.at[slot, r], where, into, r).start()
                if slot >= 2:
                    @pl.when(jnp.logical_not(top))
                    def _(slot=slot, r=r):
                        arrived(slot + 6, r)
                        sample_copy(2, rxu.at[slot + 6, r], at(u, 1, 1), slot + 2, r).start()
                        widen(slot + 6, r)
                widen(slot, r)
        for slot in range(4, 8):
            take(slot)

        @pl.when(top)
        def _():
            pl.semaphore_signal(crossed, inc=1, device_id=at(u, 1, 1), device_id_type=MESH)

    @pl.when(is01)
    def _():
        for slot in range(4):
            take(slot)

    @pl.when((c == 1) & jnp.logical_not(top))
    def _():
        for slot in range(4, 7):
            take(slot)

    @pl.when((c == 1) & top)
    def _():
        for slot in range(4, 8):
            blank(slot)

    @pl.when(top)
    def _():
        for slot in range(8, 10):
            blank(slot)

    @pl.when(is11 & top)
    def _():
        pl.semaphore_wait(crossed, 1)

    lane16 = lax.broadcasted_iota(I32, (RADIX_A, LANES), 1)

    def frame_copy(j, part):
        rows_of = pl.ds(part * PART, PART)
        where = (2 * u + (j + 1) // 2 % 2, j % 2 * 2 + c)
        return remote(tx2.at[j, rows_of], rx2.at[mine, rows_of], s2.at[0], r2.at[part], where)

    def own_frame():
        return pltpu.make_async_copy(tx2.at[e], rx2.at[mine], own_sems.at[6])

    def spectra(f, carry):
        @pl.when((f == 1) & is00)
        def _():
            cross(7)

        for slot in range(7, 10):
            @pl.when((f == slot - 6) & (c == 1) & jnp.logical_not(top))
            def _(slot=slot):
                take(slot)

        for s in range(stations):
            offset = f * NCHAN + heard[0, f * stations + s]
            row, shift = offset // LANES, offset % LANES
            for r in range(2):
                parts = [
                    pltpu.roll(
                        series[pl.ds((r * stations + s) * depth + row + q, RADIX_A, stride=QUADS), :],
                        (LANES - shift) % LANES, 1)
                    for q in range(QUADS + 1)
                ]
                for q in range(QUADS):
                    cut = jnp.where(lane16 < LANES - shift, parts[q], parts[q + 1])
                    windows[(2 * s + r) * RADIX_A:(2 * s + r + 1) * RADIX_A, q * LANES:(q + 1) * LANES] = cut.astype(BF16)
        passed = jnp.dot(first[...], windows[...], preferred_element_type=F32)
        real, imag = passed[:sk], passed[sk:]
        turned[:, 0:RADIX_B] = (real * twist[0] + imag * twist[1]).astype(BF16)
        turned[:, RADIX_B:] = (imag * twist[0] - real * twist[1]).astype(BF16)
        for g in range(QUADS):
            channels = jnp.dot(turned[...], second[:, g * 2 * LANES:(g + 1) * 2 * LANES], preferred_element_type=F32)
            real, imag = channels[:, :LANES], channels[:, LANES:]
            cosine, sine = trig[0, g], trig[1, g]
            turned_re = (real * cosine - imag * sine).reshape(stations, RADIX_A, LANES)
            turned_im = (real * sine + imag * cosine).reshape(stations, RADIX_A, LANES)
            planes[:, g * RADIX_A:(g + 1) * RADIX_A, :] = turned_re
            planes[:, CHAVG + g * RADIX_A:CHAVG + (g + 1) * RADIX_A, :] = turned_im
        for s in range(stations):
            rows[pl.ds(s, OUTCH, stride=stations), :] = planes[s].T
        tx2[f] = rows[...].astype(BF16).reshape(OUTCH, stations, LANES)

        @pl.when(f == e)
        def _():
            own_frame().start()

        @pl.when(f != e)
        def _():
            for part in range(OUTCH // PART):
                frame_copy(f, part).start()
        return carry

    lax.fori_loop(0, frames, spectra, 0)

    own_bins.wait()
    rest = rxb.at[pl.ds(0, owners - 1)]
    remote(rest, rest, s0.at[1], r0.at[1], (tm, pair)).wait_recv()
    line = rxb[0]
    for t in range(1, owners):
        line = line + rxb[t]
    span = jnp.broadcast_to(line, (all_frames, LANES))
    across = lax.broadcasted_iota(I32, (all_frames, LANES), 1)
    down = lax.broadcasted_iota(I32, (all_frames, LANES), 0)
    column = jnp.max(jnp.where(across == down, span, 0), 1, keepdims=True)
    found = jnp.max(jnp.where((span == column) & (across < down), across, -1), 1, keepdims=True)
    tables[0:all_frames] = jnp.broadcast_to(jnp.where(found < 0, all_frames, found), (all_frames, LANES))
    down = lax.broadcasted_iota(I32, (BINS, LANES), 0)
    across = lax.broadcasted_iota(I32, (BINS, LANES), 1)
    found = jnp.max(jnp.where(jnp.broadcast_to(line, (BINS, LANES)) == down + 1, across, -1), 1, keepdims=True)
    tables[all_frames:] = jnp.broadcast_to(jnp.where(found < 0, all_frames, found), (BINS, LANES))
    tell = pltpu.make_async_copy(tables, orders, own_sems.at[2])
    tell.start()

    lane32 = lax.broadcasted_iota(I32, (pairs * stations, LANES), 1)
    half = pairs * stations // 2

    @pl.when(e < frames)
    def _():
        own_frame().wait()

        def gram(row, carry):
            o = row % (OUTCH // 2) * 2 + row // (OUTCH // 2)
            left = jnp.concatenate([rx2[g, row].astype(F32) for g in range(pairs)], 0)
            swapped = pltpu.roll(left, CHAVG, 1)
            swapped = jnp.where(lane32 < CHAVG, -swapped, swapped)
            both = jnp.concatenate([left, swapped], 0).astype(BF16)
            right = jnp.concatenate([both, both], 0)
            made = lax.dot_general(left.astype(BF16), right, (((1,), (1,)), ((), ())), preferred_element_type=F32)
            gs[pl.ds(o, half, stride=OUTCH), :] = jnp.where(lane32[:half] < CHAVG, made[:half], made[half:])
            return carry

        def one_part(part, carry):
            rest = rx2.at[pl.ds(0, pairs - 1), pl.ds(0, PART)]
            remote(rest, rest, s2.at[0], r2.at[part], (tm, pair)).wait_recv()
            lax.fori_loop(0, PART, lambda i, inner: gram(part * PART + i, inner), 0, unroll=16)
            return carry

        lax.fori_loop(0, OUTCH // PART, one_part, 0)
        def turn(i, carry):
            block = gs[pl.ds(pl.multiple_of(i * OUTCH, OUTCH), OUTCH), :].T * (1.0 / CHAVG)
            for upper in range(2):
                row = i + half * upper
                a, p = row // GROUP_ST, row % GROUP_ST
                for ri in range(2):
                    for b in range(NGRP):
                        top_row = upper * CHAVG + ri * 32 + b * GROUP_ST
                        tscr[pl.ds(p * 256 + ri * 128 + a * NGRP + b, GROUP_ST, stride=NBLK), :] = block[top_row:top_row + GROUP_ST]
            return carry

        lax.fori_loop(0, half, turn, 0, unroll=4)

        def pack(p, carry):
            real = tscr[pl.ds(pl.multiple_of(p * 256, 256), 128), :].reshape(GROUP_ST, NBLK, LANES)
            imag = tscr[pl.ds(pl.multiple_of(p * 256 + 128, 128), 128), :].reshape(GROUP_ST, NBLK, LANES)
            q = lax.broadcasted_iota(I32, (GROUP_ST, NBLK, LANES), 0)
            ab = lax.broadcasted_iota(I32, (GROUP_ST, NBLK, LANES), 1)
            a, b = ab // NGRP, ab % NGRP
            upper = (a < b) | ((a == b) & (p <= q))
            tx3[pl.ds(p % 4 * GROUP_ST, GROUP_ST), p // 4] = jnp.where(upper, real, imag).astype(BF16)
            return carry

        lax.fori_loop(0, GROUP_ST, pack, 0, unroll=2)
        frame = tm // 2 * 2 * frames + c * frames + e

        def send(step, carry):
            d = (me + SLICES // 2 + step) % SLICES

            @pl.when(d != me)
            def _():
                remote(tx3.at[d], rx3.at[frame], s3.at[0], r3.at[0], place_of(d)).start()

            @pl.when(d == me)
            def _():
                pltpu.make_async_copy(tx3.at[d], rx3.at[frame], own_sems.at[3]).start()
            return carry

        lax.fori_loop(0, SLICES, send, 0, unroll=4)

    tell.wait()

    @pl.when(me < SLICES)
    def _():
        @pl.when(e < frames)
        def _():
            pltpu.make_async_copy(tx3.at[0], rx3.at[0], own_sems.at[3]).wait()
            rest = rx3.at[pl.ds(0, all_frames - 1)]
            remote(rest, rest, s3.at[0], r3.at[0], (tm, pair)).wait_recv()

        @pl.when(e >= frames)
        def _():
            remote(rx3, rx3, s3.at[0], r3.at[0], (tm, pair)).wait_recv()

        sums[all_frames] = jnp.zeros((2 * NBLK, LANES), F32)

        def add(f, carry):
            sums[f] = sums[orders[f, 0]] + rx3[f].reshape(2 * NBLK, LANES).astype(F32)
            return carry

        lax.fori_loop(0, all_frames, add, 0)

        def gather(b, carry):
            held = sums[orders[all_frames + b, 0]].astype(BF16)
            tx4[b // bins_here, pl.ds(pl.multiple_of(b % bins_here * 2 * NBLK, 2 * NBLK), 2 * NBLK), :] = held
            return carry

        lax.fori_loop(0, BINS, gather, 0, unroll=8)

        def send(step, carry):
            t = (tm + step) % owners
            remote(tx4.at[t], rx4.at[me], s4.at[0], r4.at[me], (t, pair)).start()
            return carry

        lax.fori_loop(1, owners, send, 0)
        pltpu.make_async_copy(tx4.at[tm], rx4.at[me], own_sems.at[4]).start()

    sources = SLICES // pairs

    def pass_on(d, other):
        return remote(rx4.at[d], rx4.at[d], s5.at[0], r4.at[d], (tm, other))

    def landing(d):
        def one(i, carry):
            held = rx4[d, pl.ds(pl.multiple_of(i * NBLK, NBLK), NBLK), :].astype(F32)
            landed[pl.ds(i // 2 * NBLK * 2 * SLICES + i % 2 * SLICES + d, NBLK, stride=2 * SLICES), :] = held
            return carry

        lax.fori_loop(0, 2 * bins_here, one, 0, unroll=2 * bins_here)

    def nearest(step):
        if sources != 8:
            return (tm + step) % sources
        return (tm + step) % 2 + (tm // 2 + step // 2) % 2 * 2 + (tm // 4 + step // 4) % 2 * 4

    def first_hop(step, carry):
        i = nearest(step)
        d = i * pairs + pair

        @pl.when(d == me)
        def _():
            pltpu.make_async_copy(tx4.at[tm], rx4.at[d], own_sems.at[4]).wait()

        @pl.when(d != me)
        def _():
            remote(rx4.at[d], rx4.at[d], s4.at[0], r4.at[d], (tm, pair)).wait_recv()

        for n in range(1, halves):
            pass_on(d, (pair + 2 * n) % pairs).start()
        pass_on(d, pair + 1 - 2 * c).start()
        landing(d)
        return carry

    lax.fori_loop(0, sources, first_hop, 0)

    def second_hop(step, carry):
        i = nearest(step)
        for n in range(1, halves):
            d = i * pairs + (pair + 2 * n) % pairs
            remote(rx4.at[d], rx4.at[d], s4.at[0], r4.at[d], (tm, pair)).wait_recv()
            pass_on(d, pair + 1 - 2 * c).start()
            landing(d)
        return carry

    lax.fori_loop(0, sources, second_hop, 0)

    def third_hop(step, carry):
        i = nearest(step)
        for n in range(halves):
            d = i * pairs + (pair + 1 - 2 * c + 2 * n) % pairs
            remote(rx4.at[d], rx4.at[d], s4.at[0], r4.at[d], (tm, pair)).wait_recv()
            landing(d)
        return carry

    lax.fori_loop(0, sources, third_hop, 0)

    place = lax.broadcasted_iota(I32, (GROUP_ST, LANES), 0)
    none = jnp.zeros((GROUP_ST, LANES), I32)
    span = 2 * SLICES

    def one_bin(b, carry):
        for k in range(slots):
            block = assignment[k]
            a, bb = block // NGRP, block % NGRP
            row, column = none + a, none + bb
            ahead, within = row < column, row == column
            here = (b * NBLK + block) * span
            there = (b * NBLK + bb * NGRP + a) * span
            for p in range(GROUP_ST):
                straight = landed[pl.ds(here + p * GROUP_ST, GROUP_ST), :]
                mirrored = landed[pl.ds(there + p, GROUP_ST, stride=GROUP_ST), :]
                upper = ahead | (within & (place >= p))
                real = jnp.where(upper, straight, mirrored)
                imag = jnp.where(upper, -mirrored, straight)
                imag = jnp.where(within & (place == p), 0.0, imag)
                out[b, k, 0, p * GROUP_ST:(p + 1) * GROUP_ST, :] = real.astype(BF16)
                out[b, k, 1, p * GROUP_ST:(p + 1) * GROUP_ST, :] = imag.astype(BF16)
        return carry

    lax.fori_loop(0, bins_here, one_bin, 0)

    rest = rxb.at[pl.ds(0, owners - 1)]
    remote(rest, rest, s0.at[1], r0.at[1], (tm, pair)).wait_send()

    @pl.when(c != h)
    def _():
        delay_copy().wait_send()

    def all_sent(ref, count, sem):
        rest = ref.at[pl.ds(0, count)]
        remote(rest, rest, sem, r4.at[0], (tm, pair)).wait_send()

    @pl.when(is00)
    def _():
        all_sent(rxu, 4, s1.at[0])

        @pl.when(below)
        def _():
            all_sent(rxu, 6, s1.at[1])

        @pl.when(jnp.logical_not(top))
        def _():
            all_sent(rxu, 2, s1.at[2])

    @pl.when(is10)
    def _():
        all_sent(rxu, 4, s1.at[0])

        @pl.when(below)
        def _():
            all_sent(rxu, 4, s1.at[1])

        @pl.when(jnp.logical_not(top))
        def _():
            all_sent(rxu, 2, s1.at[2])

    @pl.when(c == 1)
    def _():
        all_sent(rxu, 4, s1.at[0])

    @pl.when(is11 & below)
    def _():
        all_sent(rxu, 2, s1.at[1])

    @pl.when(e < frames)
    def _():
        all_sent(tx2, frames - 1, s2.at[0])

        @pl.when(me < SLICES)
        def _():
            all_sent(tx3, SLICES - 1, s3.at[0])

        @pl.when(me >= SLICES)
        def _():
            all_sent(tx3, SLICES, s3.at[0])

    @pl.when(e >= frames)
    def _():
        all_sent(tx2, frames, s2.at[0])

    @pl.when(me < SLICES)
    def _():
        all_sent(tx4, owners - 1, s4.at[0])

    all_sent(rx4, sources * (2 * halves - 1), s5.at[0])


VMEM = pl.BlockSpec(memory_space=pltpu.VMEM)
SMEM = pl.BlockSpec(memory_space=pltpu.SMEM)
ANY = pl.BlockSpec(memory_space=pl.ANY)


def body(voltages, delays, phase_model, phase_bins, assignment):
    owners, pairs = lax.axis_size("tm"), lax.axis_size("pair")
    devices = owners * pairs
    stations, samples = voltages.shape[1], voltages.shape[2]
    frames = samples // NCHAN
    slots = assignment.shape[0]
    all_frames = owners * frames
    bins_here = BINS // owners
    sk = stations * RADIX_A

    first, twist, second = section_tables(stations)
    span = (frames + AHEAD) * UNIT
    scratch = [
        pltpu.VMEM((2, 1, LANES), I32),
        pltpu.VMEM(first.shape, BF16),
        pltpu.VMEM(twist.shape, F32),
        pltpu.VMEM(second.shape, BF16),
        pltpu.VMEM((frames + AHEAD, 2, stations, NCHAN), BF16),
        pltpu.VMEM((2 * stations * (span + 8), LANES), F32),
        pltpu.VMEM((2 * sk, RADIX_B), BF16),
        pltpu.VMEM((sk, 2 * RADIX_B), BF16),
        pltpu.VMEM((stations, LANES, LANES), F32),
        pltpu.VMEM((OUTCH * stations, LANES), F32),
        pltpu.VMEM((8, NCHAN), F32),
        pltpu.VMEM((8 * UNIT, LANES), F32),
        pltpu.VMEM((2, QUADS, sk, LANES), F32),
        pltpu.VMEM((frames, OUTCH, stations, LANES), BF16),
        pltpu.VMEM((pairs, OUTCH, stations, LANES), BF16),
        pltpu.VMEM((pairs * stations // 2 * OUTCH, LANES), F32),
        pltpu.VMEM((2 * pairs * stations * pairs * stations, LANES), F32),
        pltpu.VMEM((SLICES, 2, NBLK, LANES), BF16),
        pltpu.VMEM((all_frames, 2, NBLK, LANES), BF16),
        pltpu.VMEM((all_frames + 1, 2 * NBLK, LANES), F32),
        pltpu.VMEM((owners, bins_here * 2 * NBLK, LANES), BF16),
        pltpu.VMEM((SLICES, bins_here * 2 * NBLK, LANES), BF16),
        pltpu.VMEM((bins_here * NBLK * 2 * SLICES, LANES), F32),
        pltpu.VMEM((1, LANES), I32),
        pltpu.VMEM((owners, 1, LANES), I32),
        pltpu.SMEM((1, LANES), I32),
        pltpu.VMEM((all_frames + BINS, LANES), I32),
        pltpu.SMEM((all_frames + BINS, LANES), I32),
        pltpu.SemaphoreType.DMA((4,)),
        pltpu.SemaphoreType.DMA((2,)),
        pltpu.SemaphoreType.DMA((2,)),
        pltpu.SemaphoreType.DMA((3,)),
        pltpu.SemaphoreType.DMA((frames + AHEAD, 2)),
        pltpu.SemaphoreType.DMA((1,)),
        pltpu.SemaphoreType.DMA((OUTCH // PART,)),
        pltpu.SemaphoreType.DMA((1,)),
        pltpu.SemaphoreType.DMA((1,)),
        pltpu.SemaphoreType.DMA((1,)),
        pltpu.SemaphoreType.DMA((SLICES,)),
        pltpu.SemaphoreType.DMA((1,)),
        pltpu.SemaphoreType.DMA((7,)),
        pltpu.SemaphoreType.DMA((4, 2)),
        pltpu.SemaphoreType.REGULAR,
    ]
    result = pl.pallas_call(
        functools.partial(fused_kernel, (owners, pairs, frames, stations, slots)),
        out_shape=pltpu.VMEM((bins_here, slots, 2, GROUP_ST * GROUP_ST, OUTCH), BF16),
        in_specs=[SMEM, SMEM, SMEM, ANY, ANY, ANY, ANY, ANY],
        out_specs=VMEM,
        scratch_shapes=scratch,
        compiler_params=pltpu.CompilerParams(
            collective_id=0, has_side_effects=True, vmem_limit_bytes=56 * 1024 * 1024),
        name="correlate",
    )(delays.T, phase_bins, assignment, voltages, phase_model, first, twist, second)
    return result.astype(F32)


def solution(mesh):
    in_specs = (P(None, "pair", "tm"), P("pair", "tm"), P(), P("tm"), P("pair"))
    out_specs = P("tm", "pair", None, None, None)
    return jax.shard_map(body, mesh=mesh, in_specs=in_specs, out_specs=out_specs, check_vma=False)
```

```python
import functools
import math

import jax
import jax.numpy as jnp
import numpy as np
from jax import lax
from jax.experimental import pallas as pl
from jax.experimental.pallas import tpu as pltpu
from jax.sharding import PartitionSpec as P

NCHAN = 8192
GROUP_ST = 8
RADIX_A = 16
CHAVG = 64
NGRP = 4
NBLK = 16
OUTCH = 128
BINS = 32
DELAY_MAX = 49152
LANES = 128
RADIX_B = NCHAN // RADIX_A
QUADS = RADIX_B // LANES
UNIT = NCHAN // LANES
AHEAD = DELAY_MAX // NCHAN
SLICES = GROUP_ST * GROUP_ST // 2
PART = 32
F32, BF16, I32 = jnp.float32, jnp.bfloat16, jnp.int32
MESH = pl.DeviceIdType.MESH


def section_tables(stations):
    a, b = np.arange(RADIX_A), np.arange(RADIX_B)
    angle = ((a[:, None] * a[None, :]) % RADIX_A).astype(np.float32) * np.float32(2.0 * math.pi / RADIX_A)
    cos_a = (np.cos(angle) * np.float32(1.0 / math.sqrt(RADIX_A))).astype(np.float32)
    sin_a = (np.sin(angle) * np.float32(1.0 / math.sqrt(RADIX_A))).astype(np.float32)
    small = np.stack([np.stack([cos_a, sin_a], 1), np.stack([-sin_a, cos_a], 1)], 0)
    first = np.einsum("st,pkrn->psktrn", np.eye(stations, dtype=np.float32), small)
    rows = 2 * stations * RADIX_A
    first = first.reshape(rows, rows)
    turn = (a[:, None] * b[None, :]).astype(np.float32) * np.float32(2.0 * math.pi / NCHAN)
    twist = np.stack([np.cos(turn), np.sin(turn)]).astype(np.float32)
    twist = np.tile(twist, (1, stations, 1))
    angle = ((b[:, None] * b[None, :]) % RADIX_B).astype(np.float32) * np.float32(2.0 * math.pi / RADIX_B)
    cos_b = (np.cos(angle) * np.float32(1.0 / math.sqrt(RADIX_B))).astype(np.float32)
    sin_b = (np.sin(angle) * np.float32(1.0 / math.sqrt(RADIX_B))).astype(np.float32)
    second = np.stack([np.stack([cos_b, -sin_b], 1), np.stack([sin_b, cos_b], 1)], 0)
    second = second.reshape(2, RADIX_B, 2, OUTCH // 2, 2, QUADS).transpose(0, 1, 5, 2, 4, 3)
    second = second.reshape(2 * RADIX_B, 2 * RADIX_B)
    return jnp.asarray(first, BF16), jnp.asarray(twist), jnp.asarray(second, BF16)


def sin_cos(x):
    turns = jnp.round(x * (2.0 / math.pi))
    r = x - turns * 1.5703125
    r = r - turns * 4.837512969970703125e-4
    r = r - turns * 7.54978995489188216e-8
    z = r * r
    s = r + r * z * ((-1.9515295891e-4 * z + 8.3321608736e-3) * z - 1.6666654611e-1)
    c = 1.0 - 0.5 * z + z * z * ((2.443315711809948e-5 * z - 1.388731625493765e-3) * z + 4.166664568298827e-2)
    size = jnp.abs(turns)
    odd = size == 1.0
    far = size == 2.0
    sine = jnp.where(odd, c, s)
    cosine = jnp.where(odd, s, c)
    sine = jnp.where(far | (turns == -1.0), -sine, sine)
    cosine = jnp.where(far | (turns == 1.0), -cosine, cosine)
    return sine, cosine


def fused_kernel(dims, delays, phase_bins, assignment, voltages, phase_model, first_hbm, twist_hbm, second_hbm, out,
                 small, first, twist, second, rxu, series, windows, turned, planes, rows, phases, phase_rows, trig,
                 tx2, rx2, gs, tscr, tx3, rx3, sums, tx4, rx4, landed, rxd, rxb, heard, tables, orders,
                 load_sems, s0, r0, s1, r1, s2, r2, s3, r3, s4, r4, s5, own_sems, unit_sems, crossed):
    owners, pairs, frames, stations, slots = dims
    devices, layers, halves = owners * pairs, owners // 2, pairs // 2
    all_frames = owners * frames
    bins_here = BINS // owners
    sk = stations * RADIX_A
    depth = (frames + AHEAD) * UNIT + 8
    tm, pair = lax.axis_index("tm"), lax.axis_index("pair")
    u, h, m, c = tm // 2, tm % 2, pair // 2, pair % 2
    me = tm * pairs + pair
    mine = 2 * m + h
    e = jnp.where(m < 2, (h + m) % 2 * 2 + m, frames)
    top = u == layers - 1

    def place_of(device):
        return (device // pairs, device % pairs)

    def remote(src, dst, send_sem, recv_sem, where):
        return pltpu.make_async_remote_copy(
            src_ref=src, dst_ref=dst, send_sem=send_sem, recv_sem=recv_sem, device_id=where, device_id_type=MESH)

    loads = [
        pltpu.make_async_copy(first_hbm, first, load_sems.at[0]),
        pltpu.make_async_copy(twist_hbm, twist, load_sems.at[1]),
        pltpu.make_async_copy(second_hbm, second, load_sems.at[2]),
        pltpu.make_async_copy(
            phase_model.at[pl.ds(pl.multiple_of(mine * stations // 8 * 8, 8), 8)], phases, load_sems.at[3]),
    ]
    for copy in loads:
        copy.start()

    lane = lax.broadcasted_iota(I32, (1, LANES), 1)
    listed, marked = jnp.zeros((1, LANES), I32), jnp.zeros((1, LANES), I32)
    for i in range(stations * frames):
        listed = jnp.where(lane == i, delays[i // stations, i % stations], listed)
    for i in range(frames):
        marked = jnp.where(lane == tm * frames + i, phase_bins[i] + 1, marked)
    small[0] = listed
    small[1] = marked

    barrier = pltpu.get_barrier_semaphore()

    def greet(step, carry):
        pl.semaphore_signal(barrier, inc=1, device_id=place_of((me + step) % devices), device_id_type=MESH)
        return carry

    lax.fori_loop(1, devices, greet, 0, unroll=True) if devices < 64 else lax.fori_loop(1, devices, greet, 0)
    pl.semaphore_wait(barrier, devices - 1)

    def delay_copy():
        return remote(small.at[0], rxd, s0.at[0], r0.at[0], (2 * u + c, 2 * m + h))

    def own_delays():
        return pltpu.make_async_copy(small.at[0], rxd, own_sems.at[0])

    @pl.when(c == h)
    def _():
        own_delays().start()

    @pl.when(c != h)
    def _():
        delay_copy().start()

    def start_bins(step, carry):
        remote(small.at[1], rxb.at[tm], s0.at[1], r0.at[1], ((tm + step) % owners, pair)).start()
        return carry

    lax.fori_loop(1, owners, start_bins, 0)
    own_bins = pltpu.make_async_copy(small.at[1], rxb.at[tm], own_sems.at[5])
    own_bins.start()

    def at(layer, half, core):
        return (2 * layer + half, 2 * m + core)

    def sample_copy(group, src, where, slot, r):
        return remote(src, rxu.at[slot, r], s1.at[group], r1.at[slot, r], where)

    def own_unit(i, r):
        return voltages.at[r, :, pl.ds(i * NCHAN, NCHAN)]

    def own_copy(i, r):
        return pltpu.make_async_copy(own_unit(i, r), rxu.at[i, r], unit_sems.at[i, r])

    def arrived(slot, r):
        sample_copy(0, rxu.at[slot, r], at(u, h, c), slot, r).wait_recv()

    below = u > 0
    lower = jnp.maximum(u - 1, 0)
    is00, is10 = (h == 0) & (c == 0), (h == 1) & (c == 0)
    is01, is11 = (h == 0) & (c == 1), (h == 1) & (c == 1)
    both = [(i, r) for i in range(4) for r in range(2)]

    @pl.when(is10)
    def _():
        for i, r in both:
            sample_copy(0, own_unit(i, r), at(u, 0, 0), 4 + i, r).start()

    @pl.when(is01)
    def _():
        for i, r in both:
            sample_copy(0, own_unit(i, r), at(u, 1, 0), i, r).start()

    @pl.when(is11)
    def _():
        for i, r in both:
            sample_copy(0, own_unit(i, r), at(u, 1, 0), 4 + i, r).start()

        @pl.when(below)
        def _():
            for i, r in both[:4]:
                sample_copy(1, own_unit(i, r), at(lower, 1, 1), 8 + i, r).start()

    @pl.when(c == h)
    def _():
        for i, r in both:
            own_copy(i, r).start()

    @pl.when(is00 & below)
    def _():
        for i, r in both:
            where, slot = (at(lower, 0, 0), 8 + i) if i < 2 else (at(lower, 0, 1), 4 + i)
            sample_copy(1, own_unit(i, r), where, slot, r).start()

    for copy in loads:
        copy.wait()

    def spread(j, carry):
        phase_rows[pl.ds(j, 8, stride=UNIT), :] = phases[:, pl.ds(pl.multiple_of(j * LANES, LANES), LANES)]
        return carry

    lax.fori_loop(0, UNIT, spread, 0)
    skip = mine * stations % 8

    def one_phase(s, carry):
        held = phase_rows[pl.ds(pl.multiple_of((skip + s) * UNIT, UNIT), UNIT), :].T
        angles = jnp.concatenate([held[:CHAVG], held[CHAVG:]], 1)
        sine, cosine = sin_cos(angles)
        here = pl.ds(pl.multiple_of(s * RADIX_A, RADIX_A), RADIX_A)
        for g in range(QUADS):
            trig[0, g, here, :] = cosine[g * RADIX_A:(g + 1) * RADIX_A]
            trig[1, g, here, :] = sine[g * RADIX_A:(g + 1) * RADIX_A]
        return carry

    lax.fori_loop(0, stations, one_phase, 0)

    @pl.when(c == h)
    def _():
        own_delays().wait()

    @pl.when(c != h)
    def _():
        delay_copy().wait_recv()

    hear = pltpu.make_async_copy(rxd, heard, own_sems.at[1])
    hear.start()
    hear.wait()

    def widen(slot, r):
        def one(j, carry):
            held = rxu[slot, r, :, pl.ds(pl.multiple_of(j * LANES, LANES), LANES)].astype(F32)
            series[pl.ds(r * stations * depth + slot * UNIT + j, stations, stride=depth), :] = held
            return carry
        lax.fori_loop(0, UNIT, one, 0, unroll=16)

    def take(slot):
        for r in range(2):
            arrived(slot, r)
            widen(slot, r)

    def blank(slot):
        def one(i, carry):
            series[pl.ds(pl.multiple_of(i * depth + slot * UNIT, 8), UNIT), :] = jnp.zeros((UNIT, LANES), F32)
            return carry
        lax.fori_loop(0, 2 * stations, one, 0)

    def clear_tail(i, carry):
        series[pl.ds(pl.multiple_of(i * depth + (frames + AHEAD) * UNIT, 8), 8), :] = jnp.zeros((8, LANES), F32)
        return carry

    lax.fori_loop(0, 2 * stations, clear_tail, 0)

    def cross(slot):
        for r in range(2):
            arrived(slot, r)
            sample_copy(0, rxu.at[slot, r], at(u, 0, 1), slot - 4, r).start()
            if slot < 6:
                @pl.when(below)
                def _(slot=slot, r=r):
                    sample_copy(1, rxu.at[slot, r], at(lower, 0, 1), slot + 4, r).start()

                @pl.when(jnp.logical_not(top))
                def _(slot=slot, r=r):
                    arrived(slot + 4, r)
                    sample_copy(2, rxu.at[slot + 4, r], at(u, 0, 1), slot, r).start()
                    widen(slot + 4, r)
            widen(slot, r)

    @pl.when(c == h)
    def _():
        for i, r in both:
            own_copy(i, r).wait()
            widen(i, r)

    @pl.when(is00)
    def _():
        for slot in range(4, 8):
            cross(slot)

    @pl.when(is10)
    def _():
        for slot in range(4):
            for r in range(2):
                arrived(slot, r)

                @pl.when(below)
                def _(slot=slot, r=r):
                    where, into = (at(lower, 1, 0), 8 + slot) if slot < 2 else (at(lower, 1, 1), 4 + slot)
                    sample_copy(1, rxu.at[slot, r], where, into, r).start()
                if slot >= 2:
                    @pl.when(jnp.logical_not(top))
                    def _(slot=slot, r=r):
                        arrived(slot + 6, r)
                        sample_copy(2, rxu.at[slot + 6, r], at(u, 1, 1), slot + 2, r).start()
                        widen(slot + 6, r)
                widen(slot, r)
        for slot in range(4, 8):
            take(slot)

        @pl.when(top)
        def _():
            pl.semaphore_signal(crossed, inc=1, device_id=at(u, 1, 1), device_id_type=MESH)

    @pl.when(is01)
    def _():
        for slot in range(4):
            take(slot)

    @pl.when((c == 1) & jnp.logical_not(top))
    def _():
        for slot in range(4, 7):
            take(slot)

    @pl.when((c == 1) & top)
    def _():
        for slot in range(4, 8):
            blank(slot)

    @pl.when(top)
    def _():
        for slot in range(8, 10):
            blank(slot)

    @pl.when(is11 & top)
    def _():
        pl.semaphore_wait(crossed, 1)

    lane16 = lax.broadcasted_iota(I32, (RADIX_A, LANES), 1)

    def frame_copy(j, part):
        rows_of = pl.ds(part * PART, PART)
        where = (2 * u + (j + 1) // 2 % 2, j % 2 * 2 + c)
        return remote(tx2.at[j, rows_of], rx2.at[mine, rows_of], s2.at[0], r2.at[part], where)

    def own_frame():
        return pltpu.make_async_copy(tx2.at[e], rx2.at[mine], own_sems.at[6])

    def dispatch(f):
        @pl.when(f == e)
        def _():
            own_frame().start()

        @pl.when(f != e)
        def _():
            for part in range(OUTCH // PART):
                frame_copy(f, part).start()

    def spectra(step, carry):
        there_h = jnp.where(step == 1, h, jnp.where(step == 3, h, 1 - h))
        there_m = jnp.where((step == 1) | (step == 2), (m + 1) % 2, m)
        f = jnp.where((c == 0) & (m < 2), (there_h + there_m) % 2 * 2 + there_m, step)

        for slot in range(7, 10):
            @pl.when((step == slot - 6) & (c == 1) & jnp.logical_not(top))
            def _(slot=slot):
                take(slot)

        for s in range(stations):
            offset = f * NCHAN + heard[0, f * stations + s]
            row, shift = offset // LANES, offset % LANES
            for r in range(2):
                parts = [
                    pltpu.roll(
                        series[pl.ds((r * stations + s) * depth + row + q, RADIX_A, stride=QUADS), :],
                        (LANES - shift) % LANES, 1)
                    for q in range(QUADS + 1)
                ]
                for q in range(QUADS):
                    cut = jnp.where(lane16 < LANES - shift, parts[q], parts[q + 1])
                    windows[(2 * s + r) * RADIX_A:(2 * s + r + 1) * RADIX_A, q * LANES:(q + 1) * LANES] = cut.astype(BF16)
        passed = jnp.dot(first[...], windows[...], preferred_element_type=F32)
        real, imag = passed[:sk], passed[sk:]
        turned[:, 0:RADIX_B] = (real * twist[0] + imag * twist[1]).astype(BF16)
        turned[:, RADIX_B:] = (imag * twist[0] - real * twist[1]).astype(BF16)
        for g in range(QUADS):
            channels = jnp.dot(turned[...], second[:, g * 2 * LANES:(g + 1) * 2 * LANES], preferred_element_type=F32)
            real, imag = channels[:, :LANES], channels[:, LANES:]
            cosine, sine = trig[0, g], trig[1, g]
            turned_re = (real * cosine - imag * sine).reshape(stations, RADIX_A, LANES)
            turned_im = (real * sine + imag * cosine).reshape(stations, RADIX_A, LANES)
            planes[:, g * RADIX_A:(g + 1) * RADIX_A, :] = turned_re
            planes[:, CHAVG + g * RADIX_A:CHAVG + (g + 1) * RADIX_A, :] = turned_im
        for s in range(stations):
            rows[pl.ds(s, OUTCH, stride=stations), :] = planes[s].T
        tx2[f] = rows[...].astype(BF16).reshape(OUTCH, stations, LANES)

        @pl.when(c == 0)
        def _():
            dispatch(f)

        @pl.when((c == 1) & (step >= 1))
        def _():
            dispatch(step - 1)

        return carry


    lax.fori_loop(0, frames, spectra, 0)

    @pl.when(c == 1)
    def _():
        for j in range(frames - 1, frames):
            dispatch(j)

    own_bins.wait()
    rest = rxb.at[pl.ds(0, owners - 1)]
    remote(rest, rest, s0.at[1], r0.at[1], (tm, pair)).wait_recv()
    line = rxb[0]
    for t in range(1, owners):
        line = line + rxb[t]
    span = jnp.broadcast_to(line, (all_frames, LANES))
    across = lax.broadcasted_iota(I32, (all_frames, LANES), 1)
    down = lax.broadcasted_iota(I32, (all_frames, LANES), 0)
    column = jnp.max(jnp.where(across == down, span, 0), 1, keepdims=True)
    found = jnp.max(jnp.where((span == column) & (across < down), across, -1), 1, keepdims=True)
    tables[0:all_frames] = jnp.broadcast_to(jnp.where(found < 0, all_frames, found), (all_frames, LANES))
    down = lax.broadcasted_iota(I32, (BINS, LANES), 0)
    across = lax.broadcasted_iota(I32, (BINS, LANES), 1)
    found = jnp.max(jnp.where(jnp.broadcast_to(line, (BINS, LANES)) == down + 1, across, -1), 1, keepdims=True)
    tables[all_frames:] = jnp.broadcast_to(jnp.where(found < 0, all_frames, found), (BINS, LANES))
    tell = pltpu.make_async_copy(tables, orders, own_sems.at[2])
    tell.start()

    lane32 = lax.broadcasted_iota(I32, (pairs * stations, LANES), 1)
    half = pairs * stations // 2

    @pl.when(e < frames)
    def _():
        own_frame().wait()

        def gram(row, carry):
            o = row % (OUTCH // 2) * 2 + row // (OUTCH // 2)
            left = jnp.concatenate([rx2[g, row].astype(F32) for g in range(pairs)], 0)
            swapped = pltpu.roll(left, CHAVG, 1)
            swapped = jnp.where(lane32 < CHAVG, -swapped, swapped)
            both = jnp.concatenate([left, swapped], 0).astype(BF16)
            right = jnp.concatenate([both, both], 0)
            made = lax.dot_general(left.astype(BF16), right, (((1,), (1,)), ((), ())), preferred_element_type=F32)
            gs[pl.ds(o, half, stride=OUTCH), :] = jnp.where(lane32[:half] < CHAVG, made[:half], made[half:])
            return carry

        def one_part(part, carry):
            rest = rx2.at[pl.ds(0, pairs - 1), pl.ds(0, PART)]
            remote(rest, rest, s2.at[0], r2.at[part], (tm, pair)).wait_recv()
            lax.fori_loop(0, PART, lambda i, inner: gram(part * PART + i, inner), 0, unroll=16)
            return carry

        lax.fori_loop(0, OUTCH // PART, one_part, 0)
        def turn(i, carry):
            block = gs[pl.ds(pl.multiple_of(i * OUTCH, OUTCH), OUTCH), :].T * (1.0 / CHAVG)
            for upper in range(2):
                row = i + half * upper
                a, p = row // GROUP_ST, row % GROUP_ST
                for ri in range(2):
                    for b in range(NGRP):
                        top_row = upper * CHAVG + ri * 32 + b * GROUP_ST
                        tscr[pl.ds(p * 256 + ri * 128 + a * NGRP + b, GROUP_ST, stride=NBLK), :] = block[top_row:top_row + GROUP_ST]
            return carry

        lax.fori_loop(0, half, turn, 0, unroll=4)

        def pack(p, carry):
            real = tscr[pl.ds(pl.multiple_of(p * 256, 256), 128), :].reshape(GROUP_ST, NBLK, LANES)
            imag = tscr[pl.ds(pl.multiple_of(p * 256 + 128, 128), 128), :].reshape(GROUP_ST, NBLK, LANES)
            q = lax.broadcasted_iota(I32, (GROUP_ST, NBLK, LANES), 0)
            ab = lax.broadcasted_iota(I32, (GROUP_ST, NBLK, LANES), 1)
            a, b = ab // NGRP, ab % NGRP
            upper = (a < b) | ((a == b) & (p <= q))
            tx3[pl.ds(p % 4 * GROUP_ST, GROUP_ST), p // 4] = jnp.where(upper, real, imag).astype(BF16)
            return carry

        lax.fori_loop(0, GROUP_ST, pack, 0, unroll=2)
        frame = tm // 2 * 2 * frames + c * frames + e

        def send(step, carry):
            d = (me + SLICES // 2 + step) % SLICES

            @pl.when(d != me)
            def _():
                remote(tx3.at[d], rx3.at[frame], s3.at[0], r3.at[0], place_of(d)).start()

            @pl.when(d == me)
            def _():
                pltpu.make_async_copy(tx3.at[d], rx3.at[frame], own_sems.at[3]).start()
            return carry

        lax.fori_loop(0, SLICES, send, 0, unroll=4)

    tell.wait()

    @pl.when(me < SLICES)
    def _():
        @pl.when(e < frames)
        def _():
            pltpu.make_async_copy(tx3.at[0], rx3.at[0], own_sems.at[3]).wait()
            rest = rx3.at[pl.ds(0, all_frames - 1)]
            remote(rest, rest, s3.at[0], r3.at[0], (tm, pair)).wait_recv()

        @pl.when(e >= frames)
        def _():
            remote(rx3, rx3, s3.at[0], r3.at[0], (tm, pair)).wait_recv()

        sums[all_frames] = jnp.zeros((2 * NBLK, LANES), F32)

        def add(f, carry):
            sums[f] = sums[orders[f, 0]] + rx3[f].reshape(2 * NBLK, LANES).astype(F32)
            return carry

        lax.fori_loop(0, all_frames, add, 0, unroll=4)

        def gather(b, carry):
            held = sums[orders[all_frames + b, 0]].astype(BF16)
            tx4[b // bins_here, pl.ds(pl.multiple_of(b % bins_here * 2 * NBLK, 2 * NBLK), 2 * NBLK), :] = held
            return carry

        lax.fori_loop(0, BINS, gather, 0, unroll=8)

        def send(step, carry):
            t = (tm + step) % owners
            remote(tx4.at[t], rx4.at[me], s4.at[0], r4.at[me], (t, pair)).start()
            return carry

        lax.fori_loop(1, owners, send, 0)
        pltpu.make_async_copy(tx4.at[tm], rx4.at[me], own_sems.at[4]).start()

    sources = SLICES // pairs

    def pass_on(d, other):
        return remote(rx4.at[d], rx4.at[d], s5.at[0], r4.at[d], (tm, other))

    def landing(d):
        def one(i, carry):
            held = rx4[d, pl.ds(pl.multiple_of(i * NBLK, NBLK), NBLK), :].astype(F32)
            landed[pl.ds(i // 2 * NBLK * 2 * SLICES + i % 2 * SLICES + d, NBLK, stride=2 * SLICES), :] = held
            return carry

        lax.fori_loop(0, 2 * bins_here, one, 0, unroll=2 * bins_here)

    def nearest(step):
        if sources != 8:
            return (tm + step) % sources
        return (tm + step) % 2 + (tm // 2 + step // 2) % 2 * 2 + (tm // 4 + step // 4) % 2 * 4

    def first_hop(step, carry):
        i = nearest(step)
        d = i * pairs + pair

        @pl.when(d == me)
        def _():
            pltpu.make_async_copy(tx4.at[tm], rx4.at[d], own_sems.at[4]).wait()

        @pl.when(d != me)
        def _():
            remote(rx4.at[d], rx4.at[d], s4.at[0], r4.at[d], (tm, pair)).wait_recv()

        for n in range(1, halves):
            pass_on(d, (pair + 2 * n) % pairs).start()
        pass_on(d, pair + 1 - 2 * c).start()
        landing(d)
        return carry

    lax.fori_loop(0, sources, first_hop, 0)

    def second_hop(step, carry):
        i = nearest(step)
        for n in range(1, halves):
            d = i * pairs + (pair + 2 * n) % pairs
            remote(rx4.at[d], rx4.at[d], s4.at[0], r4.at[d], (tm, pair)).wait_recv()
            pass_on(d, pair + 1 - 2 * c).start()
            landing(d)
        return carry

    lax.fori_loop(0, sources, second_hop, 0)

    def third_hop(step, carry):
        i = nearest(step)
        for n in range(halves):
            d = i * pairs + (pair + 1 - 2 * c + 2 * n) % pairs
            remote(rx4.at[d], rx4.at[d], s4.at[0], r4.at[d], (tm, pair)).wait_recv()
            landing(d)
        return carry

    lax.fori_loop(0, sources, third_hop, 0)

    place = lax.broadcasted_iota(I32, (GROUP_ST, LANES), 0)
    none = jnp.zeros((GROUP_ST, LANES), I32)
    span = 2 * SLICES

    def one_bin(b, carry):
        for k in range(slots):
            block = assignment[k]
            a, bb = block // NGRP, block % NGRP
            row, column = none + a, none + bb
            ahead, within = row < column, row == column
            here = (b * NBLK + block) * span
            there = (b * NBLK + bb * NGRP + a) * span
            for p in range(GROUP_ST):
                straight = landed[pl.ds(here + p * GROUP_ST, GROUP_ST), :]
                mirrored = landed[pl.ds(there + p, GROUP_ST, stride=GROUP_ST), :]
                upper = ahead | (within & (place >= p))
                real = jnp.where(upper, straight, mirrored)
                imag = jnp.where(upper, -mirrored, straight)
                imag = jnp.where(within & (place == p), 0.0, imag)
                out[b, k, 0, p * GROUP_ST:(p + 1) * GROUP_ST, :] = real.astype(BF16)
                out[b, k, 1, p * GROUP_ST:(p + 1) * GROUP_ST, :] = imag.astype(BF16)
        return carry

    lax.fori_loop(0, bins_here, one_bin, 0)

    rest = rxb.at[pl.ds(0, owners - 1)]
    remote(rest, rest, s0.at[1], r0.at[1], (tm, pair)).wait_send()

    @pl.when(c != h)
    def _():
        delay_copy().wait_send()

    def all_sent(ref, count, sem):
        rest = ref.at[pl.ds(0, count)]
        remote(rest, rest, sem, r4.at[0], (tm, pair)).wait_send()

    @pl.when(is00)
    def _():
        all_sent(rxu, 4, s1.at[0])

        @pl.when(below)
        def _():
            all_sent(rxu, 6, s1.at[1])

        @pl.when(jnp.logical_not(top))
        def _():
            all_sent(rxu, 2, s1.at[2])

    @pl.when(is10)
    def _():
        all_sent(rxu, 4, s1.at[0])

        @pl.when(below)
        def _():
            all_sent(rxu, 4, s1.at[1])

        @pl.when(jnp.logical_not(top))
        def _():
            all_sent(rxu, 2, s1.at[2])

    @pl.when(c == 1)
    def _():
        all_sent(rxu, 4, s1.at[0])

    @pl.when(is11 & below)
    def _():
        all_sent(rxu, 2, s1.at[1])

    @pl.when(e < frames)
    def _():
        all_sent(tx2, frames - 1, s2.at[0])

        @pl.when(me < SLICES)
        def _():
            all_sent(tx3, SLICES - 1, s3.at[0])

        @pl.when(me >= SLICES)
        def _():
            all_sent(tx3, SLICES, s3.at[0])

    @pl.when(e >= frames)
    def _():
        all_sent(tx2, frames, s2.at[0])

    @pl.when(me < SLICES)
    def _():
        all_sent(tx4, owners - 1, s4.at[0])

    all_sent(rx4, sources * (2 * halves - 1), s5.at[0])


VMEM = pl.BlockSpec(memory_space=pltpu.VMEM)
SMEM = pl.BlockSpec(memory_space=pltpu.SMEM)
ANY = pl.BlockSpec(memory_space=pl.ANY)


def body(voltages, delays, phase_model, phase_bins, assignment):
    owners, pairs = lax.axis_size("tm"), lax.axis_size("pair")
    devices = owners * pairs
    stations, samples = voltages.shape[1], voltages.shape[2]
    frames = samples // NCHAN
    slots = assignment.shape[0]
    all_frames = owners * frames
    bins_here = BINS // owners
    sk = stations * RADIX_A

    first, twist, second = section_tables(stations)
    span = (frames + AHEAD) * UNIT
    scratch = [
        pltpu.VMEM((2, 1, LANES), I32),
        pltpu.VMEM(first.shape, BF16),
        pltpu.VMEM(twist.shape, F32),
        pltpu.VMEM(second.shape, BF16),
        pltpu.VMEM((frames + AHEAD, 2, stations, NCHAN), BF16),
        pltpu.VMEM((2 * stations * (span + 8), LANES), F32),
        pltpu.VMEM((2 * sk, RADIX_B), BF16),
        pltpu.VMEM((sk, 2 * RADIX_B), BF16),
        pltpu.VMEM((stations, LANES, LANES), F32),
        pltpu.VMEM((OUTCH * stations, LANES), F32),
        pltpu.VMEM((8, NCHAN), F32),
        pltpu.VMEM((8 * UNIT, LANES), F32),
        pltpu.VMEM((2, QUADS, sk, LANES), F32),
        pltpu.VMEM((frames, OUTCH, stations, LANES), BF16),
        pltpu.VMEM((pairs, OUTCH, stations, LANES), BF16),
        pltpu.VMEM((pairs * stations // 2 * OUTCH, LANES), F32),
        pltpu.VMEM((2 * pairs * stations * pairs * stations, LANES), F32),
        pltpu.VMEM((SLICES, 2, NBLK, LANES), BF16),
        pltpu.VMEM((all_frames, 2, NBLK, LANES), BF16),
        pltpu.VMEM((all_frames + 1, 2 * NBLK, LANES), F32),
        pltpu.VMEM((owners, bins_here * 2 * NBLK, LANES), BF16),
        pltpu.VMEM((SLICES, bins_here * 2 * NBLK, LANES), BF16),
        pltpu.VMEM((bins_here * NBLK * 2 * SLICES, LANES), F32),
        pltpu.VMEM((1, LANES), I32),
        pltpu.VMEM((owners, 1, LANES), I32),
        pltpu.SMEM((1, LANES), I32),
        pltpu.VMEM((all_frames + BINS, LANES), I32),
        pltpu.SMEM((all_frames + BINS, LANES), I32),
        pltpu.SemaphoreType.DMA((4,)),
        pltpu.SemaphoreType.DMA((2,)),
        pltpu.SemaphoreType.DMA((2,)),
        pltpu.SemaphoreType.DMA((3,)),
        pltpu.SemaphoreType.DMA((frames + AHEAD, 2)),
        pltpu.SemaphoreType.DMA((1,)),
        pltpu.SemaphoreType.DMA((OUTCH // PART,)),
        pltpu.SemaphoreType.DMA((1,)),
        pltpu.SemaphoreType.DMA((1,)),
        pltpu.SemaphoreType.DMA((1,)),
        pltpu.SemaphoreType.DMA((SLICES,)),
        pltpu.SemaphoreType.DMA((1,)),
        pltpu.SemaphoreType.DMA((7,)),
        pltpu.SemaphoreType.DMA((4, 2)),
        pltpu.SemaphoreType.REGULAR,
    ]
    result = pl.pallas_call(
        functools.partial(fused_kernel, (owners, pairs, frames, stations, slots)),
        out_shape=pltpu.VMEM((bins_here, slots, 2, GROUP_ST * GROUP_ST, OUTCH), BF16),
        in_specs=[SMEM, SMEM, SMEM, ANY, ANY, ANY, ANY, ANY],
        out_specs=VMEM,
        scratch_shapes=scratch,
        compiler_params=pltpu.CompilerParams(
            collective_id=0, has_side_effects=True, vmem_limit_bytes=56 * 1024 * 1024),
        name="correlate",
    )(delays.T, phase_bins, assignment, voltages, phase_model, first, twist, second)
    return result.astype(F32)


def solution(mesh):
    in_specs = (P(None, "pair", "tm"), P("pair", "tm"), P(), P("tm"), P("pair"))
    out_specs = P("tm", "pair", None, None, None)
    return jax.shard_map(body, mesh=mesh, in_specs=in_specs, out_specs=out_specs, check_vma=False)
```

```python
import functools
import math

import jax
import jax.numpy as jnp
import numpy as np
from jax import lax
from jax.experimental import pallas as pl
from jax.experimental.pallas import tpu as pltpu
from jax.sharding import PartitionSpec as P

NCHAN = 8192
GROUP_ST = 8
RADIX_A = 16
CHAVG = 64
NGRP = 4
NBLK = 16
OUTCH = 128
BINS = 32
DELAY_MAX = 49152
LANES = 128
RADIX_B = NCHAN // RADIX_A
QUADS = RADIX_B // LANES
UNIT = NCHAN // LANES
AHEAD = DELAY_MAX // NCHAN
SLICES = GROUP_ST * GROUP_ST // 2
PART = 16
F32, BF16, I32 = jnp.float32, jnp.bfloat16, jnp.int32
MESH = pl.DeviceIdType.MESH


def section_tables(stations):
    a, b = np.arange(RADIX_A), np.arange(RADIX_B)
    angle = ((a[:, None] * a[None, :]) % RADIX_A).astype(np.float32) * np.float32(2.0 * math.pi / RADIX_A)
    cos_a = (np.cos(angle) * np.float32(1.0 / math.sqrt(RADIX_A))).astype(np.float32)
    sin_a = (np.sin(angle) * np.float32(1.0 / math.sqrt(RADIX_A))).astype(np.float32)
    small = np.stack([np.stack([cos_a, sin_a], 1), np.stack([-sin_a, cos_a], 1)], 0)
    first = np.einsum("st,pkrn->psktrn", np.eye(stations, dtype=np.float32), small)
    rows = 2 * stations * RADIX_A
    first = first.reshape(rows, rows)
    turn = (a[:, None] * b[None, :]).astype(np.float32) * np.float32(2.0 * math.pi / NCHAN)
    twist = np.stack([np.cos(turn), np.sin(turn)]).astype(np.float32)
    twist = np.tile(twist, (1, stations, 1))
    angle = ((b[:, None] * b[None, :]) % RADIX_B).astype(np.float32) * np.float32(2.0 * math.pi / RADIX_B)
    cos_b = (np.cos(angle) * np.float32(1.0 / math.sqrt(RADIX_B))).astype(np.float32)
    sin_b = (np.sin(angle) * np.float32(1.0 / math.sqrt(RADIX_B))).astype(np.float32)
    second = np.stack([np.stack([cos_b, -sin_b], 1), np.stack([sin_b, cos_b], 1)], 0)
    second = second.reshape(2, RADIX_B, 2, OUTCH // 2, 2, QUADS).transpose(0, 1, 5, 2, 4, 3)
    second = second.reshape(2 * RADIX_B, 2 * RADIX_B)
    return jnp.asarray(first, BF16), jnp.asarray(twist), jnp.asarray(second, BF16)


def sin_cos(x):
    turns = jnp.round(x * (2.0 / math.pi))
    r = x - turns * 1.5703125
    r = r - turns * 4.837512969970703125e-4
    r = r - turns * 7.54978995489188216e-8
    z = r * r
    s = r + r * z * ((-1.9515295891e-4 * z + 8.3321608736e-3) * z - 1.6666654611e-1)
    c = 1.0 - 0.5 * z + z * z * ((2.443315711809948e-5 * z - 1.388731625493765e-3) * z + 4.166664568298827e-2)
    size = jnp.abs(turns)
    odd = size == 1.0
    far = size == 2.0
    sine = jnp.where(odd, c, s)
    cosine = jnp.where(odd, s, c)
    sine = jnp.where(far | (turns == -1.0), -sine, sine)
    cosine = jnp.where(far | (turns == 1.0), -cosine, cosine)
    return sine, cosine


def fused_kernel(dims, delays, phase_bins, assignment, voltages, phase_model, first_hbm, twist_hbm, second_hbm, out,
                 small, first, twist, second, rxu, series, windows, turned, planes, rows, phases, phase_rows, trig,
                 tx2, rx2, gs, tscr, tx3, rx3, sums, tx4, rx4, landed, rxd, rxb, heard, tables, orders,
                 load_sems, s0, r0, s1, r1, s2, r2, s3, r3, s4, r4, s5, own_sems, unit_sems, crossed):
    owners, pairs, frames, stations, slots = dims
    devices, layers, halves = owners * pairs, owners // 2, pairs // 2
    all_frames = owners * frames
    bins_here = BINS // owners
    sk = stations * RADIX_A
    depth = (frames + AHEAD) * UNIT + 8
    tm, pair = lax.axis_index("tm"), lax.axis_index("pair")
    u, h, m, c = tm // 2, tm % 2, pair // 2, pair % 2
    me = tm * pairs + pair
    mine = 2 * m + h
    e = jnp.where(m < 2, (h + m) % 2 * 2 + m, frames)
    top = u == layers - 1

    def place_of(device):
        return (device // pairs, device % pairs)

    def remote(src, dst, send_sem, recv_sem, where):
        return pltpu.make_async_remote_copy(
            src_ref=src, dst_ref=dst, send_sem=send_sem, recv_sem=recv_sem, device_id=where, device_id_type=MESH)

    loads = [
        pltpu.make_async_copy(first_hbm, first, load_sems.at[0]),
        pltpu.make_async_copy(twist_hbm, twist, load_sems.at[1]),
        pltpu.make_async_copy(second_hbm, second, load_sems.at[2]),
        pltpu.make_async_copy(
            phase_model.at[pl.ds(pl.multiple_of(mine * stations // 8 * 8, 8), 8)], phases, load_sems.at[3]),
    ]
    for copy in loads:
        copy.start()

    lane = lax.broadcasted_iota(I32, (1, LANES), 1)
    listed, marked = jnp.zeros((1, LANES), I32), jnp.zeros((1, LANES), I32)
    for i in range(stations * frames):
        listed = jnp.where(lane == i, delays[i // stations, i % stations], listed)
    for i in range(frames):
        marked = jnp.where(lane == tm * frames + i, phase_bins[i] + 1, marked)
    small[0] = listed
    small[1] = marked

    barrier = pltpu.get_barrier_semaphore()

    def greet(step, carry):
        pl.semaphore_signal(barrier, inc=1, device_id=place_of((me + step) % devices), device_id_type=MESH)
        return carry

    lax.fori_loop(1, devices, greet, 0, unroll=True) if devices < 64 else lax.fori_loop(1, devices, greet, 0)
    pl.semaphore_wait(barrier, devices - 1)

    def delay_copy():
        return remote(small.at[0], rxd, s0.at[0], r0.at[0], (2 * u + c, 2 * m + h))

    def own_delays():
        return pltpu.make_async_copy(small.at[0], rxd, own_sems.at[0])

    @pl.when(c == h)
    def _():
        own_delays().start()

    @pl.when(c != h)
    def _():
        delay_copy().start()

    def start_bins(step, carry):
        remote(small.at[1], rxb.at[tm], s0.at[1], r0.at[1], ((tm + step) % owners, pair)).start()
        return carry

    lax.fori_loop(1, owners, start_bins, 0)
    own_bins = pltpu.make_async_copy(small.at[1], rxb.at[tm], own_sems.at[5])
    own_bins.start()

    def at(layer, half, core):
        return (2 * layer + half, 2 * m + core)

    def sample_copy(group, src, where, slot, r):
        return remote(src, rxu.at[slot, r], s1.at[group], r1.at[slot, r], where)

    def own_unit(i, r):
        return voltages.at[r, :, pl.ds(i * NCHAN, NCHAN)]

    def own_copy(i, r):
        return pltpu.make_async_copy(own_unit(i, r), rxu.at[i, r], unit_sems.at[i, r])

    def arrived(slot, r):
        sample_copy(0, rxu.at[slot, r], at(u, h, c), slot, r).wait_recv()

    below = u > 0
    lower = jnp.maximum(u - 1, 0)
    is00, is10 = (h == 0) & (c == 0), (h == 1) & (c == 0)
    is01, is11 = (h == 0) & (c == 1), (h == 1) & (c == 1)
    both = [(i, r) for i in range(4) for r in range(2)]

    @pl.when(is10)
    def _():
        for i, r in both:
            sample_copy(0, own_unit(i, r), at(u, 0, 0), 4 + i, r).start()

    @pl.when(is01)
    def _():
        for i, r in both:
            sample_copy(0, own_unit(i, r), at(u, 1, 0), i, r).start()

    @pl.when(is11)
    def _():
        for i, r in both:
            sample_copy(0, own_unit(i, r), at(u, 1, 0), 4 + i, r).start()

        @pl.when(below)
        def _():
            for i, r in both[:4]:
                sample_copy(1, own_unit(i, r), at(lower, 1, 1), 8 + i, r).start()

    @pl.when(c == h)
    def _():
        for i, r in both:
            own_copy(i, r).start()

    @pl.when(is00 & below)
    def _():
        for i, r in both:
            where, slot = (at(lower, 0, 0), 8 + i) if i < 2 else (at(lower, 0, 1), 4 + i)
            sample_copy(1, own_unit(i, r), where, slot, r).start()

    for copy in loads:
        copy.wait()

    def spread(j, carry):
        phase_rows[pl.ds(j, 8, stride=UNIT), :] = phases[:, pl.ds(pl.multiple_of(j * LANES, LANES), LANES)]
        return carry

    lax.fori_loop(0, UNIT, spread, 0, unroll=8)
    skip = mine * stations % 8

    def one_phase(s, carry):
        held = phase_rows[pl.ds(pl.multiple_of((skip + s) * UNIT, UNIT), UNIT), :].T
        angles = jnp.concatenate([held[:CHAVG], held[CHAVG:]], 1)
        sine, cosine = sin_cos(angles)
        here = pl.ds(pl.multiple_of(s * RADIX_A, RADIX_A), RADIX_A)
        for g in range(QUADS):
            trig[0, g, here, :] = cosine[g * RADIX_A:(g + 1) * RADIX_A]
            trig[1, g, here, :] = sine[g * RADIX_A:(g + 1) * RADIX_A]
        return carry

    lax.fori_loop(0, stations, one_phase, 0, unroll=2)

    @pl.when(c == h)
    def _():
        own_delays().wait()

    @pl.when(c != h)
    def _():
        delay_copy().wait_recv()

    hear = pltpu.make_async_copy(rxd, heard, own_sems.at[1])
    hear.start()
    hear.wait()

    def widen(slot, r):
        def one(j, carry):
            held = rxu[slot, r, :, pl.ds(pl.multiple_of(j * LANES, LANES), LANES)].astype(F32)
            series[pl.ds(r * stations * depth + slot * UNIT + j, stations, stride=depth), :] = held
            return carry
        lax.fori_loop(0, UNIT, one, 0, unroll=16)

    def take(slot):
        for r in range(2):
            arrived(slot, r)
            widen(slot, r)

    def blank(slot):
        def one(i, carry):
            series[pl.ds(pl.multiple_of(i * depth + slot * UNIT, 8), UNIT), :] = jnp.zeros((UNIT, LANES), F32)
            return carry
        lax.fori_loop(0, 2 * stations, one, 0)

    def clear_tail(i, carry):
        series[pl.ds(pl.multiple_of(i * depth + (frames + AHEAD) * UNIT, 8), 8), :] = jnp.zeros((8, LANES), F32)
        return carry

    lax.fori_loop(0, 2 * stations, clear_tail, 0)

    def cross(slot):
        for r in range(2):
            arrived(slot, r)
            sample_copy(0, rxu.at[slot, r], at(u, 0, 1), slot - 4, r).start()
            if slot < 6:
                @pl.when(below)
                def _(slot=slot, r=r):
                    sample_copy(1, rxu.at[slot, r], at(lower, 0, 1), slot + 4, r).start()

                @pl.when(jnp.logical_not(top))
                def _(slot=slot, r=r):
                    arrived(slot + 4, r)
                    sample_copy(2, rxu.at[slot + 4, r], at(u, 0, 1), slot, r).start()
                    widen(slot + 4, r)
            widen(slot, r)

    @pl.when(c == h)
    def _():
        for i, r in both:
            own_copy(i, r).wait()
            widen(i, r)

    @pl.when(is00)
    def _():
        for slot in range(4, 8):
            cross(slot)

    @pl.when(is10)
    def _():
        for slot in range(4):
            for r in range(2):
                arrived(slot, r)

                @pl.when(below)
                def _(slot=slot, r=r):
                    where, into = (at(lower, 1, 0), 8 + slot) if slot < 2 else (at(lower, 1, 1), 4 + slot)
                    sample_copy(1, rxu.at[slot, r], where, into, r).start()
                if slot >= 2:
                    @pl.when(jnp.logical_not(top))
                    def _(slot=slot, r=r):
                        arrived(slot + 6, r)
                        sample_copy(2, rxu.at[slot + 6, r], at(u, 1, 1), slot + 2, r).start()
                        widen(slot + 6, r)
                widen(slot, r)
        for slot in range(4, 8):
            take(slot)

        @pl.when(top)
        def _():
            pl.semaphore_signal(crossed, inc=1, device_id=at(u, 1, 1), device_id_type=MESH)

    @pl.when(is01)
    def _():
        for slot in range(4):
            take(slot)

    @pl.when((c == 1) & jnp.logical_not(top))
    def _():
        for slot in range(4, 7):
            take(slot)

    @pl.when((c == 1) & top)
    def _():
        for slot in range(4, 8):
            blank(slot)

    @pl.when(top)
    def _():
        for slot in range(8, 10):
            blank(slot)

    @pl.when(is11 & top)
    def _():
        pl.semaphore_wait(crossed, 1)

    lane16 = lax.broadcasted_iota(I32, (RADIX_A, LANES), 1)

    def frame_copy(j, part):
        rows_of = pl.ds(part * PART, PART)
        where = (2 * u + (j + 1) // 2 % 2, j % 2 * 2 + c)
        return remote(tx2.at[j, rows_of], rx2.at[mine, rows_of], s2.at[0], r2.at[part], where)

    def own_frame():
        return pltpu.make_async_copy(tx2.at[e], rx2.at[mine], own_sems.at[6])

    def dispatch(f):
        @pl.when(f == e)
        def _():
            own_frame().start()

        @pl.when(f != e)
        def _():
            for part in range(OUTCH // PART):
                frame_copy(f, part).start()

    def spectra(step, carry):
        there_h = jnp.where(step == 1, h, jnp.where(step == 3, h, 1 - h))
        there_m = jnp.where((step == 1) | (step == 2), (m + 1) % 2, m)
        f = jnp.where((c == 0) & (m < 2), (there_h + there_m) % 2 * 2 + there_m, step)

        for slot in range(7, 10):
            @pl.when((step == slot - 6) & (c == 1) & jnp.logical_not(top))
            def _(slot=slot):
                take(slot)

        for s in range(stations):
            offset = f * NCHAN + heard[0, f * stations + s]
            row, shift = offset // LANES, offset % LANES
            for r in range(2):
                parts = [
                    pltpu.roll(
                        series[pl.ds((r * stations + s) * depth + row + q, RADIX_A, stride=QUADS), :],
                        (LANES - shift) % LANES, 1)
                    for q in range(QUADS + 1)
                ]
                for q in range(QUADS):
                    cut = jnp.where(lane16 < LANES - shift, parts[q], parts[q + 1])
                    windows[(2 * s + r) * RADIX_A:(2 * s + r + 1) * RADIX_A, q * LANES:(q + 1) * LANES] = cut.astype(BF16)
        passed = jnp.dot(first[...], windows[...], preferred_element_type=F32)
        real, imag = passed[:sk], passed[sk:]
        turned[:, 0:RADIX_B] = (real * twist[0] + imag * twist[1]).astype(BF16)
        turned[:, RADIX_B:] = (imag * twist[0] - real * twist[1]).astype(BF16)
        for g in range(QUADS):
            channels = jnp.dot(turned[...], second[:, g * 2 * LANES:(g + 1) * 2 * LANES], preferred_element_type=F32)
            real, imag = channels[:, :LANES], channels[:, LANES:]
            cosine, sine = trig[0, g], trig[1, g]
            turned_re = (real * cosine - imag * sine).reshape(stations, RADIX_A, LANES)
            turned_im = (real * sine + imag * cosine).reshape(stations, RADIX_A, LANES)
            planes[:, g * RADIX_A:(g + 1) * RADIX_A, :] = turned_re
            planes[:, CHAVG + g * RADIX_A:CHAVG + (g + 1) * RADIX_A, :] = turned_im
        for s in range(stations):
            rows[pl.ds(s, OUTCH, stride=stations), :] = planes[s].T
        tx2[f] = rows[...].astype(BF16).reshape(OUTCH, stations, LANES)

        @pl.when(c == 0)
        def _():
            dispatch(f)

        @pl.when((c == 1) & (step >= 1))
        def _():
            dispatch(step - 1)

        return carry


    lax.fori_loop(0, frames, spectra, 0)

    @pl.when(c == 1)
    def _():
        for j in range(frames - 1, frames):
            dispatch(j)

    own_bins.wait()
    rest = rxb.at[pl.ds(0, owners - 1)]
    remote(rest, rest, s0.at[1], r0.at[1], (tm, pair)).wait_recv()
    line = rxb[0]
    for t in range(1, owners):
        line = line + rxb[t]
    span = jnp.broadcast_to(line, (all_frames, LANES))
    across = lax.broadcasted_iota(I32, (all_frames, LANES), 1)
    down = lax.broadcasted_iota(I32, (all_frames, LANES), 0)
    column = jnp.max(jnp.where(across == down, span, 0), 1, keepdims=True)
    found = jnp.max(jnp.where((span == column) & (across < down), across, -1), 1, keepdims=True)
    tables[0:all_frames] = jnp.broadcast_to(jnp.where(found < 0, all_frames, found), (all_frames, LANES))
    down = lax.broadcasted_iota(I32, (BINS, LANES), 0)
    across = lax.broadcasted_iota(I32, (BINS, LANES), 1)
    found = jnp.max(jnp.where(jnp.broadcast_to(line, (BINS, LANES)) == down + 1, across, -1), 1, keepdims=True)
    tables[all_frames:] = jnp.broadcast_to(jnp.where(found < 0, all_frames, found), (BINS, LANES))
    tell = pltpu.make_async_copy(tables, orders, own_sems.at[2])
    tell.start()

    lane32 = lax.broadcasted_iota(I32, (pairs * stations, LANES), 1)
    half = pairs * stations // 2

    @pl.when(e < frames)
    def _():
        own_frame().wait()

        def gram(row, carry):
            o = row % (OUTCH // 2) * 2 + row // (OUTCH // 2)
            left = jnp.concatenate([rx2[g, row].astype(F32) for g in range(pairs)], 0)
            swapped = pltpu.roll(left, CHAVG, 1)
            swapped = jnp.where(lane32 < CHAVG, -swapped, swapped)
            both = jnp.concatenate([left, swapped], 0).astype(BF16)
            right = jnp.concatenate([both, both], 0)
            made = lax.dot_general(left.astype(BF16), right, (((1,), (1,)), ((), ())), preferred_element_type=F32)
            gs[pl.ds(o, half, stride=OUTCH), :] = jnp.where(lane32[:half] < CHAVG, made[:half], made[half:])
            return carry

        def one_part(part, carry):
            rest = rx2.at[pl.ds(0, pairs - 1), pl.ds(0, PART)]
            remote(rest, rest, s2.at[0], r2.at[part], (tm, pair)).wait_recv()
            lax.fori_loop(0, PART, lambda i, inner: gram(part * PART + i, inner), 0, unroll=16)
            return carry

        lax.fori_loop(0, OUTCH // PART, one_part, 0)
        def turn(i, carry):
            block = gs[pl.ds(pl.multiple_of(i * OUTCH, OUTCH), OUTCH), :].T * (1.0 / CHAVG)
            for upper in range(2):
                row = i + half * upper
                a, p = row // GROUP_ST, row % GROUP_ST
                for ri in range(2):
                    for b in range(NGRP):
                        top_row = upper * CHAVG + ri * 32 + b * GROUP_ST
                        tscr[pl.ds(p * 256 + ri * 128 + a * NGRP + b, GROUP_ST, stride=NBLK), :] = block[top_row:top_row + GROUP_ST]
            return carry

        lax.fori_loop(0, half, turn, 0, unroll=8)

        def pack(p, carry):
            real = tscr[pl.ds(pl.multiple_of(p * 256, 256), 128), :].reshape(GROUP_ST, NBLK, LANES)
            imag = tscr[pl.ds(pl.multiple_of(p * 256 + 128, 128), 128), :].reshape(GROUP_ST, NBLK, LANES)
            q = lax.broadcasted_iota(I32, (GROUP_ST, NBLK, LANES), 0)
            ab = lax.broadcasted_iota(I32, (GROUP_ST, NBLK, LANES), 1)
            a, b = ab // NGRP, ab % NGRP
            upper = (a < b) | ((a == b) & (p <= q))
            tx3[pl.ds(p % 4 * GROUP_ST, GROUP_ST), p // 4] = jnp.where(upper, real, imag).astype(BF16)
            return carry

        lax.fori_loop(0, GROUP_ST, pack, 0, unroll=2)
        frame = tm // 2 * 2 * frames + c * frames + e

        def send(step, carry):
            d = (me + SLICES // 2 + step) % SLICES

            @pl.when(d != me)
            def _():
                remote(tx3.at[d], rx3.at[frame], s3.at[0], r3.at[0], place_of(d)).start()

            @pl.when(d == me)
            def _():
                pltpu.make_async_copy(tx3.at[d], rx3.at[frame], own_sems.at[3]).start()
            return carry

        lax.fori_loop(0, SLICES, send, 0, unroll=16)

    tell.wait()

    def picked(step, order):
        value = order[0]
        for i in range(1, len(order)):
            value = jnp.where(step == i, order[i], value)
        return value

    def across(k):
        return (tm + k) % 2 + (tm // 2 + k // 2) % 2 * 2 + (tm // 4 + k // 4) % 2 * 4

    @pl.when(me < SLICES)
    def _():
        @pl.when(e < frames)
        def _():
            pltpu.make_async_copy(tx3.at[0], rx3.at[0], own_sems.at[3]).wait()
            rest = rx3.at[pl.ds(0, all_frames - 1)]
            remote(rest, rest, s3.at[0], r3.at[0], (tm, pair)).wait_recv()

        @pl.when(e >= frames)
        def _():
            remote(rx3, rx3, s3.at[0], r3.at[0], (tm, pair)).wait_recv()

        sums[all_frames] = jnp.zeros((2 * NBLK, LANES), F32)

        def add(f, carry):
            sums[f] = sums[orders[f, 0]] + rx3[f].reshape(2 * NBLK, LANES).astype(F32)
            return carry

        lax.fori_loop(0, all_frames, add, 0, unroll=4)

        def give(step, carry):
            t = (tm + step) % owners
            for i in range(bins_here):
                held = sums[orders[all_frames + t * bins_here + i, 0]].astype(BF16)
                tx4[t, i * 2 * NBLK:(i + 1) * 2 * NBLK, :] = held

            @pl.when(t != tm)
            def _():
                remote(tx4.at[t], rx4.at[me], s4.at[0], r4.at[me], (t, pair)).start()
            return carry

        lax.fori_loop(1, owners + 1, give, 0, unroll=2)
        pltpu.make_async_copy(tx4.at[tm], rx4.at[me], own_sems.at[4]).start()

    sources = SLICES // pairs

    def pass_on(d, other):
        return remote(rx4.at[d], rx4.at[d], s5.at[0], r4.at[d], (tm, other))

    def landing(d):
        def one(i, carry):
            held = rx4[d, pl.ds(pl.multiple_of(i * NBLK, NBLK), NBLK), :].astype(F32)
            landed[pl.ds(i // 2 * NBLK * 2 * SLICES + i % 2 * SLICES + d, NBLK, stride=2 * SLICES), :] = held
            return carry

        lax.fori_loop(0, 2 * bins_here, one, 0, unroll=2 * bins_here)

    def nearest(step):
        if owners != 8:
            return (tm + step) % sources
        return across(picked(step, (0, 1, 2, 3, 4, 5, 6, 7)))

    def first_hop(step, carry):
        i = nearest(step)
        d = i * pairs + pair

        @pl.when(d == me)
        def _():
            pltpu.make_async_copy(tx4.at[tm], rx4.at[d], own_sems.at[4]).wait()

        @pl.when(d != me)
        def _():
            remote(rx4.at[d], rx4.at[d], s4.at[0], r4.at[d], (tm, pair)).wait_recv()

        for n in range(1, halves):
            pass_on(d, (pair + 2 * n) % pairs).start()
        pass_on(d, pair + 1 - 2 * c).start()
        landing(d)
        return carry

    lax.fori_loop(0, sources, first_hop, 0)

    def second_hop(step, carry):
        i = nearest(step)
        for n in range(1, halves):
            d = i * pairs + (pair + 2 * n) % pairs
            remote(rx4.at[d], rx4.at[d], s4.at[0], r4.at[d], (tm, pair)).wait_recv()
            pass_on(d, pair + 1 - 2 * c).start()
            landing(d)
        return carry

    lax.fori_loop(0, sources, second_hop, 0)

    def third_hop(step, carry):
        i = nearest(step)
        for n in range(halves):
            d = i * pairs + (pair + 1 - 2 * c + 2 * n) % pairs
            remote(rx4.at[d], rx4.at[d], s4.at[0], r4.at[d], (tm, pair)).wait_recv()
            landing(d)
        return carry

    lax.fori_loop(0, sources, third_hop, 0)

    place = lax.broadcasted_iota(I32, (GROUP_ST, LANES), 0)
    none = jnp.zeros((GROUP_ST, LANES), I32)
    span = 2 * SLICES

    def one_bin(b, carry):
        for k in range(slots):
            block = assignment[k]
            a, bb = block // NGRP, block % NGRP
            row, column = none + a, none + bb
            ahead, within = row < column, row == column
            here = (b * NBLK + block) * span
            there = (b * NBLK + bb * NGRP + a) * span
            for p in range(GROUP_ST):
                straight = landed[pl.ds(here + p * GROUP_ST, GROUP_ST), :]
                mirrored = landed[pl.ds(there + p, GROUP_ST, stride=GROUP_ST), :]
                upper = ahead | (within & (place >= p))
                real = jnp.where(upper, straight, mirrored)
                imag = jnp.where(upper, -mirrored, straight)
                imag = jnp.where(within & (place == p), 0.0, imag)
                out[b, k, 0, p * GROUP_ST:(p + 1) * GROUP_ST, :] = real.astype(BF16)
                out[b, k, 1, p * GROUP_ST:(p + 1) * GROUP_ST, :] = imag.astype(BF16)
        return carry

    lax.fori_loop(0, bins_here, one_bin, 0)

    rest = rxb.at[pl.ds(0, owners - 1)]
    remote(rest, rest, s0.at[1], r0.at[1], (tm, pair)).wait_send()

    @pl.when(c != h)
    def _():
        delay_copy().wait_send()

    def all_sent(ref, count, sem):
        rest = ref.at[pl.ds(0, count)]
        remote(rest, rest, sem, r4.at[0], (tm, pair)).wait_send()

    @pl.when(is00)
    def _():
        all_sent(rxu, 4, s1.at[0])

        @pl.when(below)
        def _():
            all_sent(rxu, 6, s1.at[1])

        @pl.when(jnp.logical_not(top))
        def _():
            all_sent(rxu, 2, s1.at[2])

    @pl.when(is10)
    def _():
        all_sent(rxu, 4, s1.at[0])

        @pl.when(below)
        def _():
            all_sent(rxu, 4, s1.at[1])

        @pl.when(jnp.logical_not(top))
        def _():
            all_sent(rxu, 2, s1.at[2])

    @pl.when(c == 1)
    def _():
        all_sent(rxu, 4, s1.at[0])

    @pl.when(is11 & below)
    def _():
        all_sent(rxu, 2, s1.at[1])

    @pl.when(e < frames)
    def _():
        all_sent(tx2, frames - 1, s2.at[0])

        @pl.when(me < SLICES)
        def _():
            all_sent(tx3, SLICES - 1, s3.at[0])

        @pl.when(me >= SLICES)
        def _():
            all_sent(tx3, SLICES, s3.at[0])

    @pl.when(e >= frames)
    def _():
        all_sent(tx2, frames, s2.at[0])

    @pl.when(me < SLICES)
    def _():
        all_sent(tx4, owners - 1, s4.at[0])

    all_sent(rx4, sources * (2 * halves - 1), s5.at[0])


VMEM = pl.BlockSpec(memory_space=pltpu.VMEM)
SMEM = pl.BlockSpec(memory_space=pltpu.SMEM)
ANY = pl.BlockSpec(memory_space=pl.ANY)


def body(voltages, delays, phase_model, phase_bins, assignment):
    owners, pairs = lax.axis_size("tm"), lax.axis_size("pair")
    devices = owners * pairs
    stations, samples = voltages.shape[1], voltages.shape[2]
    frames = samples // NCHAN
    slots = assignment.shape[0]
    all_frames = owners * frames
    bins_here = BINS // owners
    sk = stations * RADIX_A

    first, twist, second = section_tables(stations)
    span = (frames + AHEAD) * UNIT
    scratch = [
        pltpu.VMEM((2, 1, LANES), I32),
        pltpu.VMEM(first.shape, BF16),
        pltpu.VMEM(twist.shape, F32),
        pltpu.VMEM(second.shape, BF16),
        pltpu.VMEM((frames + AHEAD, 2, stations, NCHAN), BF16),
        pltpu.VMEM((2 * stations * (span + 8), LANES), F32),
        pltpu.VMEM((2 * sk, RADIX_B), BF16),
        pltpu.VMEM((sk, 2 * RADIX_B), BF16),
        pltpu.VMEM((stations, LANES, LANES), F32),
        pltpu.VMEM((OUTCH * stations, LANES), F32),
        pltpu.VMEM((8, NCHAN), F32),
        pltpu.VMEM((8 * UNIT, LANES), F32),
        pltpu.VMEM((2, QUADS, sk, LANES), F32),
        pltpu.VMEM((frames, OUTCH, stations, LANES), BF16),
        pltpu.VMEM((pairs, OUTCH, stations, LANES), BF16),
        pltpu.VMEM((pairs * stations // 2 * OUTCH, LANES), F32),
        pltpu.VMEM((2 * pairs * stations * pairs * stations, LANES), F32),
        pltpu.VMEM((SLICES, 2, NBLK, LANES), BF16),
        pltpu.VMEM((all_frames, 2, NBLK, LANES), BF16),
        pltpu.VMEM((all_frames + 1, 2 * NBLK, LANES), F32),
        pltpu.VMEM((owners, bins_here * 2 * NBLK, LANES), BF16),
        pltpu.VMEM((SLICES, bins_here * 2 * NBLK, LANES), BF16),
        pltpu.VMEM((bins_here * NBLK * 2 * SLICES, LANES), F32),
        pltpu.VMEM((1, LANES), I32),
        pltpu.VMEM((owners, 1, LANES), I32),
        pltpu.SMEM((1, LANES), I32),
        pltpu.VMEM((all_frames + BINS, LANES), I32),
        pltpu.SMEM((all_frames + BINS, LANES), I32),
        pltpu.SemaphoreType.DMA((4,)),
        pltpu.SemaphoreType.DMA((2,)),
        pltpu.SemaphoreType.DMA((2,)),
        pltpu.SemaphoreType.DMA((3,)),
        pltpu.SemaphoreType.DMA((frames + AHEAD, 2)),
        pltpu.SemaphoreType.DMA((1,)),
        pltpu.SemaphoreType.DMA((OUTCH // PART,)),
        pltpu.SemaphoreType.DMA((1,)),
        pltpu.SemaphoreType.DMA((1,)),
        pltpu.SemaphoreType.DMA((1,)),
        pltpu.SemaphoreType.DMA((SLICES,)),
        pltpu.SemaphoreType.DMA((1,)),
        pltpu.SemaphoreType.DMA((7,)),
        pltpu.SemaphoreType.DMA((4, 2)),
        pltpu.SemaphoreType.REGULAR,
    ]
    result = pl.pallas_call(
        functools.partial(fused_kernel, (owners, pairs, frames, stations, slots)),
        out_shape=pltpu.VMEM((bins_here, slots, 2, GROUP_ST * GROUP_ST, OUTCH), BF16),
        in_specs=[SMEM, SMEM, SMEM, ANY, ANY, ANY, ANY, ANY],
        out_specs=VMEM,
        scratch_shapes=scratch,
        compiler_params=pltpu.CompilerParams(
            collective_id=0, has_side_effects=True, vmem_limit_bytes=56 * 1024 * 1024),
        name="correlate",
    )(delays.T, phase_bins, assignment, voltages, phase_model, first, twist, second)
    return result.astype(F32)


def solution(mesh):
    in_specs = (P(None, "pair", "tm"), P("pair", "tm"), P(), P("tm"), P("pair"))
    out_specs = P("tm", "pair", None, None, None)
    return jax.shard_map(body, mesh=mesh, in_specs=in_specs, out_specs=out_specs, check_vma=False)
```

```python
import functools
import math

import jax
import jax.numpy as jnp
import numpy as np
from jax import lax
from jax.experimental import pallas as pl
from jax.experimental.pallas import tpu as pltpu
from jax.sharding import PartitionSpec as P

NCHAN = 8192
GROUP_ST = 8
RADIX_A = 16
CHAVG = 64
NGRP = 4
NBLK = 16
OUTCH = 128
BINS = 32
DELAY_MAX = 49152
LANES = 128
RADIX_B = NCHAN // RADIX_A
QUADS = RADIX_B // LANES
UNIT = NCHAN // LANES
AHEAD = DELAY_MAX // NCHAN
SLICES = GROUP_ST * GROUP_ST // 2
PART = 16
F32, BF16, I32 = jnp.float32, jnp.bfloat16, jnp.int32
MESH = pl.DeviceIdType.MESH


def section_tables(stations):
    a, b = np.arange(RADIX_A), np.arange(RADIX_B)
    angle = ((a[:, None] * a[None, :]) % RADIX_A).astype(np.float32) * np.float32(2.0 * math.pi / RADIX_A)
    cos_a = (np.cos(angle) * np.float32(1.0 / math.sqrt(RADIX_A))).astype(np.float32)
    sin_a = (np.sin(angle) * np.float32(1.0 / math.sqrt(RADIX_A))).astype(np.float32)
    small = np.stack([np.stack([cos_a, sin_a], 1), np.stack([-sin_a, cos_a], 1)], 0)
    first = np.einsum("st,pkrn->psktrn", np.eye(stations, dtype=np.float32), small)
    rows = 2 * stations * RADIX_A
    first = first.reshape(rows, rows)
    turn = (a[:, None] * b[None, :]).astype(np.float32) * np.float32(2.0 * math.pi / NCHAN)
    twist = np.stack([np.cos(turn), np.sin(turn)]).astype(np.float32)
    twist = np.tile(twist, (1, stations, 1))
    angle = ((b[:, None] * b[None, :]) % RADIX_B).astype(np.float32) * np.float32(2.0 * math.pi / RADIX_B)
    cos_b = (np.cos(angle) * np.float32(1.0 / math.sqrt(RADIX_B))).astype(np.float32)
    sin_b = (np.sin(angle) * np.float32(1.0 / math.sqrt(RADIX_B))).astype(np.float32)
    second = np.stack([np.stack([cos_b, -sin_b], 1), np.stack([sin_b, cos_b], 1)], 0)
    second = second.reshape(2, RADIX_B, 2, OUTCH // 2, 2, QUADS).transpose(0, 1, 5, 2, 4, 3)
    second = second.reshape(2 * RADIX_B, 2 * RADIX_B)
    return jnp.asarray(first, BF16), jnp.asarray(twist), jnp.asarray(second, BF16)


def sin_cos(x):
    turns = jnp.round(x * (2.0 / math.pi))
    r = x - turns * 1.5703125
    r = r - turns * 4.837512969970703125e-4
    r = r - turns * 7.54978995489188216e-8
    z = r * r
    s = r + r * z * ((-1.9515295891e-4 * z + 8.3321608736e-3) * z - 1.6666654611e-1)
    c = 1.0 - 0.5 * z + z * z * ((2.443315711809948e-5 * z - 1.388731625493765e-3) * z + 4.166664568298827e-2)
    size = jnp.abs(turns)
    odd = size == 1.0
    far = size == 2.0
    sine = jnp.where(odd, c, s)
    cosine = jnp.where(odd, s, c)
    sine = jnp.where(far | (turns == -1.0), -sine, sine)
    cosine = jnp.where(far | (turns == 1.0), -cosine, cosine)
    return sine, cosine


def fused_kernel(dims, delays, phase_bins, assignment, voltages, phase_model, first_hbm, twist_hbm, second_hbm, out,
                 small, first, twist, second, rxu, series, windows, turned, planes, rows, phases, phase_rows, trig,
                 tx2, rx2, gs, tscr, tx3, rx3, sums, tx4, rx4, landed, rxd, rxb, heard, tables, orders,
                 load_sems, s0, r0, s1, r1, s2, r2, s3, r3, s4, r4, s5, own_sems, unit_sems, crossed):
    owners, pairs, frames, stations, slots = dims
    devices, layers, halves = owners * pairs, owners // 2, pairs // 2
    all_frames = owners * frames
    bins_here = BINS // owners
    sk = stations * RADIX_A
    depth = (frames + AHEAD) * UNIT + 8
    tm, pair = lax.axis_index("tm"), lax.axis_index("pair")
    u, h, m, c = tm // 2, tm % 2, pair // 2, pair % 2
    me = tm * pairs + pair
    mine = 2 * m + h
    e = jnp.where(m < 2, (h + m) % 2 * 2 + m, frames)
    top = u == layers - 1

    def place_of(device):
        return (device // pairs, device % pairs)

    def remote(src, dst, send_sem, recv_sem, where):
        return pltpu.make_async_remote_copy(
            src_ref=src, dst_ref=dst, send_sem=send_sem, recv_sem=recv_sem, device_id=where, device_id_type=MESH)

    loads = [
        pltpu.make_async_copy(first_hbm, first, load_sems.at[0]),
        pltpu.make_async_copy(twist_hbm, twist, load_sems.at[1]),
        pltpu.make_async_copy(second_hbm, second, load_sems.at[2]),
        pltpu.make_async_copy(
            phase_model.at[pl.ds(pl.multiple_of(mine * stations // 8 * 8, 8), 8)], phases, load_sems.at[3]),
    ]
    for copy in loads:
        copy.start()

    lane = lax.broadcasted_iota(I32, (1, LANES), 1)
    listed, marked = jnp.zeros((1, LANES), I32), jnp.zeros((1, LANES), I32)
    for i in range(stations * frames):
        listed = jnp.where(lane == i, delays[i // stations, i % stations], listed)
    for i in range(frames):
        marked = jnp.where(lane == tm * frames + i, phase_bins[i] + 1, marked)
    small[0] = listed
    small[1] = marked

    barrier = pltpu.get_barrier_semaphore()

    def greet(step, carry):
        pl.semaphore_signal(barrier, inc=1, device_id=place_of((me + step) % devices), device_id_type=MESH)
        return carry

    lax.fori_loop(1, devices, greet, 0, unroll=True) if devices < 64 else lax.fori_loop(1, devices, greet, 0)
    pl.semaphore_wait(barrier, devices - 1)

    def delay_copy():
        return remote(small.at[0], rxd, s0.at[0], r0.at[0], (2 * u + c, 2 * m + h))

    def own_delays():
        return pltpu.make_async_copy(small.at[0], rxd, own_sems.at[0])

    @pl.when(c == h)
    def _():
        own_delays().start()

    @pl.when(c != h)
    def _():
        delay_copy().start()

    def start_bins(step, carry):
        remote(small.at[1], rxb.at[tm], s0.at[1], r0.at[1], ((tm + step) % owners, pair)).start()
        return carry

    lax.fori_loop(1, owners, start_bins, 0)
    own_bins = pltpu.make_async_copy(small.at[1], rxb.at[tm], own_sems.at[5])
    own_bins.start()

    def at(layer, half, core):
        return (2 * layer + half, 2 * m + core)

    def sample_copy(group, src, where, slot, r):
        return remote(src, rxu.at[slot, r], s1.at[group], r1.at[slot, r], where)

    def own_unit(i, r):
        return voltages.at[r, :, pl.ds(i * NCHAN, NCHAN)]

    def own_copy(i, r):
        return pltpu.make_async_copy(own_unit(i, r), rxu.at[i, r], unit_sems.at[i, r])

    def arrived(slot, r):
        sample_copy(0, rxu.at[slot, r], at(u, h, c), slot, r).wait_recv()

    below = u > 0
    lower = jnp.maximum(u - 1, 0)
    is00, is10 = (h == 0) & (c == 0), (h == 1) & (c == 0)
    is01, is11 = (h == 0) & (c == 1), (h == 1) & (c == 1)
    both = [(i, r) for i in range(4) for r in range(2)]

    @pl.when(is10)
    def _():
        for i, r in both:
            sample_copy(0, own_unit(i, r), at(u, 0, 0), 4 + i, r).start()

    @pl.when(is01)
    def _():
        for i, r in both:
            sample_copy(0, own_unit(i, r), at(u, 1, 0), i, r).start()

    @pl.when(is11)
    def _():
        for i, r in both:
            sample_copy(0, own_unit(i, r), at(u, 1, 0), 4 + i, r).start()

        @pl.when(below)
        def _():
            for i, r in both[:4]:
                sample_copy(1, own_unit(i, r), at(lower, 1, 1), 8 + i, r).start()

    @pl.when(c == h)
    def _():
        for i, r in both:
            own_copy(i, r).start()

    @pl.when(is00 & below)
    def _():
        for i, r in both:
            where, slot = (at(lower, 0, 0), 8 + i) if i < 2 else (at(lower, 0, 1), 4 + i)
            sample_copy(1, own_unit(i, r), where, slot, r).start()

    for copy in loads:
        copy.wait()

    def spread(j, carry):
        phase_rows[pl.ds(j, 8, stride=UNIT), :] = phases[:, pl.ds(pl.multiple_of(j * LANES, LANES), LANES)]
        return carry

    lax.fori_loop(0, UNIT, spread, 0, unroll=8)
    skip = mine * stations % 8

    def one_phase(s, carry):
        held = phase_rows[pl.ds(pl.multiple_of((skip + s) * UNIT, UNIT), UNIT), :].T
        angles = jnp.concatenate([held[:CHAVG], held[CHAVG:]], 1)
        sine, cosine = sin_cos(angles)
        here = pl.ds(pl.multiple_of(s * RADIX_A, RADIX_A), RADIX_A)
        for g in range(QUADS):
            trig[0, g, here, :] = cosine[g * RADIX_A:(g + 1) * RADIX_A]
            trig[1, g, here, :] = sine[g * RADIX_A:(g + 1) * RADIX_A]
        return carry

    lax.fori_loop(0, stations, one_phase, 0, unroll=2)

    @pl.when(c == h)
    def _():
        own_delays().wait()

    @pl.when(c != h)
    def _():
        delay_copy().wait_recv()

    hear = pltpu.make_async_copy(rxd, heard, own_sems.at[1])
    hear.start()
    hear.wait()

    def widen(slot, r):
        def one(j, carry):
            held = rxu[slot, r, :, pl.ds(pl.multiple_of(j * LANES, LANES), LANES)].astype(F32)
            series[pl.ds(r * stations * depth + slot * UNIT + j, stations, stride=depth), :] = held
            return carry
        lax.fori_loop(0, UNIT, one, 0, unroll=16)

    def take(slot):
        for r in range(2):
            arrived(slot, r)
            widen(slot, r)

    def blank(slot):
        def one(i, carry):
            series[pl.ds(pl.multiple_of(i * depth + slot * UNIT, 8), UNIT), :] = jnp.zeros((UNIT, LANES), F32)
            return carry
        lax.fori_loop(0, 2 * stations, one, 0)

    def clear_tail(i, carry):
        series[pl.ds(pl.multiple_of(i * depth + (frames + AHEAD) * UNIT, 8), 8), :] = jnp.zeros((8, LANES), F32)
        return carry

    lax.fori_loop(0, 2 * stations, clear_tail, 0)

    def cross(slot):
        for r in range(2):
            arrived(slot, r)
            sample_copy(0, rxu.at[slot, r], at(u, 0, 1), slot - 4, r).start()
            if slot < 6:
                @pl.when(below)
                def _(slot=slot, r=r):
                    sample_copy(1, rxu.at[slot, r], at(lower, 0, 1), slot + 4, r).start()

                @pl.when(jnp.logical_not(top))
                def _(slot=slot, r=r):
                    arrived(slot + 4, r)
                    sample_copy(2, rxu.at[slot + 4, r], at(u, 0, 1), slot, r).start()
                    widen(slot + 4, r)
            widen(slot, r)

    @pl.when(c == h)
    def _():
        for i, r in both:
            own_copy(i, r).wait()
            widen(i, r)

    @pl.when(is00)
    def _():
        for slot in range(4, 8):
            cross(slot)

    @pl.when(is10)
    def _():
        for slot in range(4):
            for r in range(2):
                arrived(slot, r)

                @pl.when(below)
                def _(slot=slot, r=r):
                    where, into = (at(lower, 1, 0), 8 + slot) if slot < 2 else (at(lower, 1, 1), 4 + slot)
                    sample_copy(1, rxu.at[slot, r], where, into, r).start()
                if slot >= 2:
                    @pl.when(jnp.logical_not(top))
                    def _(slot=slot, r=r):
                        arrived(slot + 6, r)
                        sample_copy(2, rxu.at[slot + 6, r], at(u, 1, 1), slot + 2, r).start()
                        widen(slot + 6, r)
                widen(slot, r)
        for slot in range(4, 8):
            take(slot)

        @pl.when(top)
        def _():
            pl.semaphore_signal(crossed, inc=1, device_id=at(u, 1, 1), device_id_type=MESH)

    @pl.when(is01)
    def _():
        for slot in range(4):
            take(slot)

    @pl.when((c == 1) & jnp.logical_not(top))
    def _():
        for slot in range(4, 7):
            take(slot)

    @pl.when((c == 1) & top)
    def _():
        for slot in range(4, 8):
            blank(slot)

    @pl.when(top)
    def _():
        for slot in range(8, 10):
            blank(slot)

    @pl.when(is11 & top)
    def _():
        pl.semaphore_wait(crossed, 1)

    lane16 = lax.broadcasted_iota(I32, (RADIX_A, LANES), 1)

    def frame_copy(j, part):
        rows_of = pl.ds(part * PART, PART)
        where = (2 * u + (j + 1) // 2 % 2, j % 2 * 2 + c)
        return remote(tx2.at[j, rows_of], rx2.at[mine, rows_of], s2.at[0], r2.at[part], where)

    def own_frame():
        return pltpu.make_async_copy(tx2.at[e], rx2.at[mine], own_sems.at[6])

    def dispatch(f):
        @pl.when(f == e)
        def _():
            own_frame().start()

        @pl.when(f != e)
        def _():
            for part in range(OUTCH // PART):
                frame_copy(f, part).start()

    def spectra(step, carry):
        there_h = jnp.where(step == 1, h, jnp.where(step == 3, h, 1 - h))
        there_m = jnp.where((step == 1) | (step == 2), (m + 1) % 2, m)
        f = jnp.where((c == 0) & (m < 2), (there_h + there_m) % 2 * 2 + there_m, step)

        for slot in range(7, 10):
            @pl.when((step == slot - 6) & (c == 1) & jnp.logical_not(top))
            def _(slot=slot):
                take(slot)

        for s in range(stations):
            offset = f * NCHAN + heard[0, f * stations + s]
            row, shift = offset // LANES, offset % LANES
            for r in range(2):
                parts = [
                    pltpu.roll(
                        series[pl.ds((r * stations + s) * depth + row + q, RADIX_A, stride=QUADS), :],
                        (LANES - shift) % LANES, 1)
                    for q in range(QUADS + 1)
                ]
                for q in range(QUADS):
                    cut = jnp.where(lane16 < LANES - shift, parts[q], parts[q + 1])
                    windows[(2 * s + r) * RADIX_A:(2 * s + r + 1) * RADIX_A, q * LANES:(q + 1) * LANES] = cut.astype(BF16)
        passed = jnp.dot(first[...], windows[...], preferred_element_type=F32)
        real, imag = passed[:sk], passed[sk:]
        turned[:, 0:RADIX_B] = (real * twist[0] + imag * twist[1]).astype(BF16)
        turned[:, RADIX_B:] = (imag * twist[0] - real * twist[1]).astype(BF16)
        for g in range(QUADS):
            channels = jnp.dot(turned[...], second[:, g * 2 * LANES:(g + 1) * 2 * LANES], preferred_element_type=F32)
            real, imag = channels[:, :LANES], channels[:, LANES:]
            cosine, sine = trig[0, g], trig[1, g]
            turned_re = (real * cosine - imag * sine).reshape(stations, RADIX_A, LANES)
            turned_im = (real * sine + imag * cosine).reshape(stations, RADIX_A, LANES)
            planes[:, g * RADIX_A:(g + 1) * RADIX_A, :] = turned_re
            planes[:, CHAVG + g * RADIX_A:CHAVG + (g + 1) * RADIX_A, :] = turned_im
        for s in range(stations):
            rows[pl.ds(s, OUTCH, stride=stations), :] = planes[s].T
        tx2[f] = rows[...].astype(BF16).reshape(OUTCH, stations, LANES)

        @pl.when(c == 0)
        def _():
            dispatch(f)

        @pl.when((c == 1) & (step >= 1))
        def _():
            dispatch(step - 1)

        return carry


    lax.fori_loop(0, frames, spectra, 0)

    @pl.when(c == 1)
    def _():
        for j in range(frames - 1, frames):
            dispatch(j)

    own_bins.wait()
    rest = rxb.at[pl.ds(0, owners - 1)]
    remote(rest, rest, s0.at[1], r0.at[1], (tm, pair)).wait_recv()
    line = rxb[0]
    for t in range(1, owners):
        line = line + rxb[t]
    span = jnp.broadcast_to(line, (all_frames, LANES))
    across = lax.broadcasted_iota(I32, (all_frames, LANES), 1)
    down = lax.broadcasted_iota(I32, (all_frames, LANES), 0)
    column = jnp.max(jnp.where(across == down, span, 0), 1, keepdims=True)
    found = jnp.max(jnp.where((span == column) & (across < down), across, -1), 1, keepdims=True)
    tables[0:all_frames] = jnp.broadcast_to(jnp.where(found < 0, all_frames, found), (all_frames, LANES))
    down = lax.broadcasted_iota(I32, (BINS, LANES), 0)
    across = lax.broadcasted_iota(I32, (BINS, LANES), 1)
    found = jnp.max(jnp.where(jnp.broadcast_to(line, (BINS, LANES)) == down + 1, across, -1), 1, keepdims=True)
    tables[all_frames:] = jnp.broadcast_to(jnp.where(found < 0, all_frames, found), (BINS, LANES))
    tell = pltpu.make_async_copy(tables, orders, own_sems.at[2])
    tell.start()

    lane32 = lax.broadcasted_iota(I32, (pairs * stations, LANES), 1)
    half = pairs * stations // 2

    @pl.when(e < frames)
    def _():
        own_frame().wait()

        def gram(row, carry):
            o = row % (OUTCH // 2) * 2 + row // (OUTCH // 2)
            left = jnp.concatenate([rx2[g, row].astype(F32) for g in range(pairs)], 0)
            swapped = pltpu.roll(left, CHAVG, 1)
            swapped = jnp.where(lane32 < CHAVG, -swapped, swapped)
            both = jnp.concatenate([left, swapped], 0).astype(BF16)
            right = jnp.concatenate([both, both], 0)
            made = lax.dot_general(left.astype(BF16), right, (((1,), (1,)), ((), ())), preferred_element_type=F32)
            gs[pl.ds(o, half, stride=OUTCH), :] = jnp.where(lane32[:half] < CHAVG, made[:half], made[half:])
            return carry

        def one_part(part, carry):
            rest = rx2.at[pl.ds(0, pairs - 1), pl.ds(0, PART)]
            remote(rest, rest, s2.at[0], r2.at[part], (tm, pair)).wait_recv()
            lax.fori_loop(0, PART, lambda i, inner: gram(part * PART + i, inner), 0, unroll=16)
            return carry

        lax.fori_loop(0, OUTCH // PART, one_part, 0)
        def turn(i, carry):
            block = gs[pl.ds(pl.multiple_of(i * OUTCH, OUTCH), OUTCH), :].T * (1.0 / CHAVG)
            for upper in range(2):
                row = i + half * upper
                a, p = row // GROUP_ST, row % GROUP_ST
                for ri in range(2):
                    for b in range(NGRP):
                        top_row = upper * CHAVG + ri * 32 + b * GROUP_ST
                        tscr[pl.ds(p * 256 + ri * 128 + a * NGRP + b, GROUP_ST, stride=NBLK), :] = block[top_row:top_row + GROUP_ST]
            return carry

        lax.fori_loop(0, half, turn, 0, unroll=8)

        def pack(p, carry):
            real = tscr[pl.ds(pl.multiple_of(p * 256, 256), 128), :].reshape(GROUP_ST, NBLK, LANES)
            imag = tscr[pl.ds(pl.multiple_of(p * 256 + 128, 128), 128), :].reshape(GROUP_ST, NBLK, LANES)
            q = lax.broadcasted_iota(I32, (GROUP_ST, NBLK, LANES), 0)
            ab = lax.broadcasted_iota(I32, (GROUP_ST, NBLK, LANES), 1)
            a, b = ab // NGRP, ab % NGRP
            upper = (a < b) | ((a == b) & (p <= q))
            tx3[pl.ds(p % 4 * GROUP_ST, GROUP_ST), p // 4] = jnp.where(upper, real, imag).astype(BF16)
            return carry

        lax.fori_loop(0, GROUP_ST, pack, 0, unroll=2)
        frame = tm // 2 * 2 * frames + c * frames + e

        def send(step, carry):
            d = (me + SLICES // 2 + step) % SLICES

            @pl.when(d != me)
            def _():
                remote(tx3.at[d], rx3.at[frame], s3.at[0], r3.at[0], place_of(d)).start()

            @pl.when(d == me)
            def _():
                pltpu.make_async_copy(tx3.at[d], rx3.at[frame], own_sems.at[3]).start()
            return carry

        lax.fori_loop(0, SLICES, send, 0, unroll=16)

    tell.wait()

    def picked(step, order):
        value = order[0]
        for i in range(1, len(order)):
            value = jnp.where(step == i, order[i], value)
        return value

    def across(k):
        return (tm + k) % 2 + (tm // 2 + k // 2) % 2 * 2 + (tm // 4 + k // 4) % 2 * 4

    @pl.when(me < SLICES)
    def _():
        @pl.when(e < frames)
        def _():
            pltpu.make_async_copy(tx3.at[0], rx3.at[0], own_sems.at[3]).wait()
            rest = rx3.at[pl.ds(0, all_frames - 1)]
            remote(rest, rest, s3.at[0], r3.at[0], (tm, pair)).wait_recv()

        @pl.when(e >= frames)
        def _():
            remote(rx3, rx3, s3.at[0], r3.at[0], (tm, pair)).wait_recv()

        sums[all_frames] = jnp.zeros((2 * NBLK, LANES), F32)

        def add(f, carry):
            sums[f] = sums[orders[f, 0]] + rx3[f].reshape(2 * NBLK, LANES).astype(F32)
            return carry

        lax.fori_loop(0, all_frames, add, 0, unroll=4)

        def give(step, carry):
            t = (tm + step) % owners
            for i in range(bins_here):
                held = sums[orders[all_frames + t * bins_here + i, 0]].astype(BF16)
                tx4[t, i * 2 * NBLK:(i + 1) * 2 * NBLK, :] = held

            @pl.when(t != tm)
            def _():
                remote(tx4.at[t], rx4.at[me], s4.at[0], r4.at[me], (t, pair)).start()
            return carry

        lax.fori_loop(1, owners + 1, give, 0, unroll=2)
        pltpu.make_async_copy(tx4.at[tm], rx4.at[me], own_sems.at[4]).start()

    sources = SLICES // pairs

    def pass_on(d, other):
        return remote(rx4.at[d], rx4.at[d], s5.at[0], r4.at[d], (tm, other))

    def landing(d):
        def one(i, carry):
            held = rx4[d, pl.ds(pl.multiple_of(i * NBLK, NBLK), NBLK), :].astype(F32)
            landed[pl.ds(i // 2 * NBLK * 2 * SLICES + i % 2 * SLICES + d, NBLK, stride=2 * SLICES), :] = held
            return carry

        lax.fori_loop(0, 2 * bins_here, one, 0, unroll=2 * bins_here)

    def nearest(step):
        if owners != 8:
            return (tm + step) % sources
        return across(picked(step, (0, 1, 2, 3, 4, 5, 6, 7)))

    def first_hop(step, carry):
        i = nearest(step)
        d = i * pairs + pair

        @pl.when(d == me)
        def _():
            pltpu.make_async_copy(tx4.at[tm], rx4.at[d], own_sems.at[4]).wait()

        @pl.when(d != me)
        def _():
            remote(rx4.at[d], rx4.at[d], s4.at[0], r4.at[d], (tm, pair)).wait_recv()

        for n in range(1, halves):
            pass_on(d, (pair + 2 * n) % pairs).start()
        pass_on(d, pair + 1 - 2 * c).start()
        landing(d)
        return carry

    lax.fori_loop(0, sources, first_hop, 0)

    def second_hop(step, carry):
        i = nearest(step)
        for n in range(1, halves):
            d = i * pairs + (pair + 2 * n) % pairs
            remote(rx4.at[d], rx4.at[d], s4.at[0], r4.at[d], (tm, pair)).wait_recv()
            pass_on(d, pair + 1 - 2 * c).start()
            landing(d)
        beside(i, 0)
        return carry

    def beside(i, n):
        d = i * pairs + (pair + 1 - 2 * c + 2 * n) % pairs
        remote(rx4.at[d], rx4.at[d], s4.at[0], r4.at[d], (tm, pair)).wait_recv()
        landing(d)

    lax.fori_loop(0, sources, second_hop, 0)

    def third_hop(step, carry):
        for n in range(1, halves):
            beside(nearest(step), n)
        return carry

    lax.fori_loop(0, sources, third_hop, 0)

    place = lax.broadcasted_iota(I32, (GROUP_ST, LANES), 0)
    none = jnp.zeros((GROUP_ST, LANES), I32)
    span = 2 * SLICES

    def one_bin(b, carry):
        for k in range(slots):
            block = assignment[k]
            a, bb = block // NGRP, block % NGRP
            row, column = none + a, none + bb
            ahead, within = row < column, row == column
            here = (b * NBLK + block) * span
            there = (b * NBLK + bb * NGRP + a) * span
            for p in range(GROUP_ST):
                straight = landed[pl.ds(here + p * GROUP_ST, GROUP_ST), :]
                mirrored = landed[pl.ds(there + p, GROUP_ST, stride=GROUP_ST), :]
                upper = ahead | (within & (place >= p))
                real = jnp.where(upper, straight, mirrored)
                imag = jnp.where(upper, -mirrored, straight)
                imag = jnp.where(within & (place == p), 0.0, imag)
                out[b, k, 0, p * GROUP_ST:(p + 1) * GROUP_ST, :] = real.astype(BF16)
                out[b, k, 1, p * GROUP_ST:(p + 1) * GROUP_ST, :] = imag.astype(BF16)
        return carry

    lax.fori_loop(0, bins_here, one_bin, 0)

    rest = rxb.at[pl.ds(0, owners - 1)]
    remote(rest, rest, s0.at[1], r0.at[1], (tm, pair)).wait_send()

    @pl.when(c != h)
    def _():
        delay_copy().wait_send()

    def all_sent(ref, count, sem):
        rest = ref.at[pl.ds(0, count)]
        remote(rest, rest, sem, r4.at[0], (tm, pair)).wait_send()

    @pl.when(is00)
    def _():
        all_sent(rxu, 4, s1.at[0])

        @pl.when(below)
        def _():
            all_sent(rxu, 6, s1.at[1])

        @pl.when(jnp.logical_not(top))
        def _():
            all_sent(rxu, 2, s1.at[2])

    @pl.when(is10)
    def _():
        all_sent(rxu, 4, s1.at[0])

        @pl.when(below)
        def _():
            all_sent(rxu, 4, s1.at[1])

        @pl.when(jnp.logical_not(top))
        def _():
            all_sent(rxu, 2, s1.at[2])

    @pl.when(c == 1)
    def _():
        all_sent(rxu, 4, s1.at[0])

    @pl.when(is11 & below)
    def _():
        all_sent(rxu, 2, s1.at[1])

    @pl.when(e < frames)
    def _():
        all_sent(tx2, frames - 1, s2.at[0])

        @pl.when(me < SLICES)
        def _():
            all_sent(tx3, SLICES - 1, s3.at[0])

        @pl.when(me >= SLICES)
        def _():
            all_sent(tx3, SLICES, s3.at[0])

    @pl.when(e >= frames)
    def _():
        all_sent(tx2, frames, s2.at[0])

    @pl.when(me < SLICES)
    def _():
        all_sent(tx4, owners - 1, s4.at[0])

    all_sent(rx4, sources * (2 * halves - 1), s5.at[0])


VMEM = pl.BlockSpec(memory_space=pltpu.VMEM)
SMEM = pl.BlockSpec(memory_space=pltpu.SMEM)
ANY = pl.BlockSpec(memory_space=pl.ANY)


def body(voltages, delays, phase_model, phase_bins, assignment):
    owners, pairs = lax.axis_size("tm"), lax.axis_size("pair")
    devices = owners * pairs
    stations, samples = voltages.shape[1], voltages.shape[2]
    frames = samples // NCHAN
    slots = assignment.shape[0]
    all_frames = owners * frames
    bins_here = BINS // owners
    sk = stations * RADIX_A

    first, twist, second = section_tables(stations)
    span = (frames + AHEAD) * UNIT
    scratch = [
        pltpu.VMEM((2, 1, LANES), I32),
        pltpu.VMEM(first.shape, BF16),
        pltpu.VMEM(twist.shape, F32),
        pltpu.VMEM(second.shape, BF16),
        pltpu.VMEM((frames + AHEAD, 2, stations, NCHAN), BF16),
        pltpu.VMEM((2 * stations * (span + 8), LANES), F32),
        pltpu.VMEM((2 * sk, RADIX_B), BF16),
        pltpu.VMEM((sk, 2 * RADIX_B), BF16),
        pltpu.VMEM((stations, LANES, LANES), F32),
        pltpu.VMEM((OUTCH * stations, LANES), F32),
        pltpu.VMEM((8, NCHAN), F32),
        pltpu.VMEM((8 * UNIT, LANES), F32),
        pltpu.VMEM((2, QUADS, sk, LANES), F32),
        pltpu.VMEM((frames, OUTCH, stations, LANES), BF16),
        pltpu.VMEM((pairs, OUTCH, stations, LANES), BF16),
        pltpu.VMEM((pairs * stations // 2 * OUTCH, LANES), F32),
        pltpu.VMEM((2 * pairs * stations * pairs * stations, LANES), F32),
        pltpu.VMEM((SLICES, 2, NBLK, LANES), BF16),
        pltpu.VMEM((all_frames, 2, NBLK, LANES), BF16),
        pltpu.VMEM((all_frames + 1, 2 * NBLK, LANES), F32),
        pltpu.VMEM((owners, bins_here * 2 * NBLK, LANES), BF16),
        pltpu.VMEM((SLICES, bins_here * 2 * NBLK, LANES), BF16),
        pltpu.VMEM((bins_here * NBLK * 2 * SLICES, LANES), F32),
        pltpu.VMEM((1, LANES), I32),
        pltpu.VMEM((owners, 1, LANES), I32),
        pltpu.SMEM((1, LANES), I32),
        pltpu.VMEM((all_frames + BINS, LANES), I32),
        pltpu.SMEM((all_frames + BINS, LANES), I32),
        pltpu.SemaphoreType.DMA((4,)),
        pltpu.SemaphoreType.DMA((2,)),
        pltpu.SemaphoreType.DMA((2,)),
        pltpu.SemaphoreType.DMA((3,)),
        pltpu.SemaphoreType.DMA((frames + AHEAD, 2)),
        pltpu.SemaphoreType.DMA((1,)),
        pltpu.SemaphoreType.DMA((OUTCH // PART,)),
        pltpu.SemaphoreType.DMA((1,)),
        pltpu.SemaphoreType.DMA((1,)),
        pltpu.SemaphoreType.DMA((1,)),
        pltpu.SemaphoreType.DMA((SLICES,)),
        pltpu.SemaphoreType.DMA((1,)),
        pltpu.SemaphoreType.DMA((7,)),
        pltpu.SemaphoreType.DMA((4, 2)),
        pltpu.SemaphoreType.REGULAR,
    ]
    result = pl.pallas_call(
        functools.partial(fused_kernel, (owners, pairs, frames, stations, slots)),
        out_shape=pltpu.VMEM((bins_here, slots, 2, GROUP_ST * GROUP_ST, OUTCH), BF16),
        in_specs=[SMEM, SMEM, SMEM, ANY, ANY, ANY, ANY, ANY],
        out_specs=VMEM,
        scratch_shapes=scratch,
        compiler_params=pltpu.CompilerParams(
            collective_id=0, has_side_effects=True, vmem_limit_bytes=56 * 1024 * 1024),
        name="correlate",
    )(delays.T, phase_bins, assignment, voltages, phase_model, first, twist, second)
    return result.astype(F32)


def solution(mesh):
    in_specs = (P(None, "pair", "tm"), P("pair", "tm"), P(), P("tm"), P("pair"))
    out_specs = P("tm", "pair", None, None, None)
    return jax.shard_map(body, mesh=mesh, in_specs=in_specs, out_specs=out_specs, check_vma=False)
```

```python
import functools
import math

import jax
import jax.numpy as jnp
import numpy as np
from jax import lax
from jax.experimental import pallas as pl
from jax.experimental.pallas import tpu as pltpu
from jax.sharding import PartitionSpec as P

NCHAN = 8192
GROUP_ST = 8
RADIX_A = 16
CHAVG = 64
NGRP = 4
NBLK = 16
OUTCH = 128
BINS = 32
DELAY_MAX = 49152
LANES = 128
RADIX_B = NCHAN // RADIX_A
QUADS = RADIX_B // LANES
UNIT = NCHAN // LANES
AHEAD = DELAY_MAX // NCHAN
SLICES = GROUP_ST * GROUP_ST // 2
PART = 16
F32, BF16, I32 = jnp.float32, jnp.bfloat16, jnp.int32
MESH = pl.DeviceIdType.MESH


def section_tables(stations):
    a, b = np.arange(RADIX_A), np.arange(RADIX_B)
    angle = ((a[:, None] * a[None, :]) % RADIX_A).astype(np.float32) * np.float32(2.0 * math.pi / RADIX_A)
    cos_a = (np.cos(angle) * np.float32(1.0 / math.sqrt(RADIX_A))).astype(np.float32)
    sin_a = (np.sin(angle) * np.float32(1.0 / math.sqrt(RADIX_A))).astype(np.float32)
    small = np.stack([np.stack([cos_a, sin_a], 1), np.stack([-sin_a, cos_a], 1)], 0)
    first = np.einsum("st,pkrn->psktrn", np.eye(stations, dtype=np.float32), small)
    rows = 2 * stations * RADIX_A
    first = first.reshape(rows, rows)
    turn = (a[:, None] * b[None, :]).astype(np.float32) * np.float32(2.0 * math.pi / NCHAN)
    twist = np.stack([np.cos(turn), np.sin(turn)]).astype(np.float32)
    twist = np.tile(twist, (1, stations, 1))
    angle = ((b[:, None] * b[None, :]) % RADIX_B).astype(np.float32) * np.float32(2.0 * math.pi / RADIX_B)
    cos_b = (np.cos(angle) * np.float32(1.0 / math.sqrt(RADIX_B))).astype(np.float32)
    sin_b = (np.sin(angle) * np.float32(1.0 / math.sqrt(RADIX_B))).astype(np.float32)
    second = np.stack([np.stack([cos_b, -sin_b], 1), np.stack([sin_b, cos_b], 1)], 0)
    second = second.reshape(2, RADIX_B, 2, OUTCH // 2, 2, QUADS).transpose(0, 1, 5, 2, 4, 3)
    second = second.reshape(2 * RADIX_B, 2 * RADIX_B)
    return jnp.asarray(first, BF16), jnp.asarray(twist), jnp.asarray(second, BF16)


def sin_cos(x):
    turns = jnp.round(x * (2.0 / math.pi))
    r = x - turns * 1.5703125
    r = r - turns * 4.837512969970703125e-4
    r = r - turns * 7.54978995489188216e-8
    z = r * r
    s = r + r * z * ((-1.9515295891e-4 * z + 8.3321608736e-3) * z - 1.6666654611e-1)
    c = 1.0 - 0.5 * z + z * z * ((2.443315711809948e-5 * z - 1.388731625493765e-3) * z + 4.166664568298827e-2)
    size = jnp.abs(turns)
    odd = size == 1.0
    far = size == 2.0
    sine = jnp.where(odd, c, s)
    cosine = jnp.where(odd, s, c)
    sine = jnp.where(far | (turns == -1.0), -sine, sine)
    cosine = jnp.where(far | (turns == 1.0), -cosine, cosine)
    return sine, cosine


def fused_kernel(dims, delays, phase_bins, assignment, voltages, phase_model, first_hbm, twist_hbm, second_hbm, out,
                 small, first, twist, second, rxu, series, windows, turned, planes, rows, phases, phase_rows, trig,
                 tx2, rx2, gs, tscr, tx3, rx3, sums, tx4, rx4, landed, rxd, rxb, heard, tables, orders,
                 load_sems, s0, r0, s1, r1, s2, r2, s3, r3, s4, r4, s5, own_sems, unit_sems, crossed):
    owners, pairs, frames, stations, slots = dims
    devices, layers, halves = owners * pairs, owners // 2, pairs // 2
    all_frames = owners * frames
    bins_here = BINS // owners
    sk = stations * RADIX_A
    depth = (frames + AHEAD) * UNIT + 8
    tm, pair = lax.axis_index("tm"), lax.axis_index("pair")
    u, h, m, c = tm // 2, tm % 2, pair // 2, pair % 2
    me = tm * pairs + pair
    mine = 2 * m + h
    e = jnp.where(m < 2, (h + m) % 2 * 2 + m, frames)
    top = u == layers - 1

    def place_of(device):
        return (device // pairs, device % pairs)

    def remote(src, dst, send_sem, recv_sem, where):
        return pltpu.make_async_remote_copy(
            src_ref=src, dst_ref=dst, send_sem=send_sem, recv_sem=recv_sem, device_id=where, device_id_type=MESH)

    loads = [
        pltpu.make_async_copy(first_hbm, first, load_sems.at[0]),
        pltpu.make_async_copy(twist_hbm, twist, load_sems.at[1]),
        pltpu.make_async_copy(second_hbm, second, load_sems.at[2]),
        pltpu.make_async_copy(
            phase_model.at[pl.ds(pl.multiple_of(mine * stations // 8 * 8, 8), 8)], phases, load_sems.at[3]),
    ]
    for copy in loads:
        copy.start()

    lane = lax.broadcasted_iota(I32, (1, LANES), 1)
    listed, marked = jnp.zeros((1, LANES), I32), jnp.zeros((1, LANES), I32)
    for i in range(stations * frames):
        listed = jnp.where(lane == i, delays[i // stations, i % stations], listed)
    for i in range(frames):
        marked = jnp.where(lane == tm * frames + i, phase_bins[i] + 1, marked)
    small[0] = listed
    small[1] = marked

    barrier = pltpu.get_barrier_semaphore()

    def greet(step, carry):
        pl.semaphore_signal(barrier, inc=1, device_id=place_of((me + step) % devices), device_id_type=MESH)
        return carry

    lax.fori_loop(1, devices, greet, 0, unroll=True) if devices < 64 else lax.fori_loop(1, devices, greet, 0)
    pl.semaphore_wait(barrier, devices - 1)

    def delay_copy():
        return remote(small.at[0], rxd, s0.at[0], r0.at[0], (2 * u + c, 2 * m + h))

    def own_delays():
        return pltpu.make_async_copy(small.at[0], rxd, own_sems.at[0])

    @pl.when(c == h)
    def _():
        own_delays().start()

    @pl.when(c != h)
    def _():
        delay_copy().start()

    def start_bins(step, carry):
        remote(small.at[1], rxb.at[tm], s0.at[1], r0.at[1], ((tm + step) % owners, pair)).start()
        return carry

    lax.fori_loop(1, owners, start_bins, 0)
    own_bins = pltpu.make_async_copy(small.at[1], rxb.at[tm], own_sems.at[5])
    own_bins.start()

    def at(layer, half, core):
        return (2 * layer + half, 2 * m + core)

    def sample_copy(group, src, where, slot, r):
        return remote(src, rxu.at[slot, r], s1.at[group], r1.at[slot, r], where)

    def own_unit(i, r):
        return voltages.at[r, :, pl.ds(i * NCHAN, NCHAN)]

    def own_copy(i, r):
        return pltpu.make_async_copy(own_unit(i, r), rxu.at[i, r], unit_sems.at[i, r])

    def arrived(slot, r):
        sample_copy(0, rxu.at[slot, r], at(u, h, c), slot, r).wait_recv()

    below = u > 0
    lower = jnp.maximum(u - 1, 0)
    is00, is10 = (h == 0) & (c == 0), (h == 1) & (c == 0)
    is01, is11 = (h == 0) & (c == 1), (h == 1) & (c == 1)
    both = [(i, r) for i in range(4) for r in range(2)]

    @pl.when(is10)
    def _():
        for i, r in both:
            sample_copy(0, own_unit(i, r), at(u, 0, 0), 4 + i, r).start()

    @pl.when(is01)
    def _():
        for i, r in both:
            sample_copy(0, own_unit(i, r), at(u, 1, 0), i, r).start()

    @pl.when(is11)
    def _():
        for i, r in both:
            sample_copy(0, own_unit(i, r), at(u, 1, 0), 4 + i, r).start()

        @pl.when(below)
        def _():
            for i, r in both[:4]:
                sample_copy(1, own_unit(i, r), at(lower, 1, 1), 8 + i, r).start()

    @pl.when(c == h)
    def _():
        for i, r in both:
            own_copy(i, r).start()

    @pl.when(is00 & below)
    def _():
        for i, r in both:
            where, slot = (at(lower, 0, 0), 8 + i) if i < 2 else (at(lower, 0, 1), 4 + i)
            sample_copy(1, own_unit(i, r), where, slot, r).start()

    for copy in loads:
        copy.wait()

    def spread(j, carry):
        phase_rows[pl.ds(j, 8, stride=UNIT), :] = phases[:, pl.ds(pl.multiple_of(j * LANES, LANES), LANES)]
        return carry

    lax.fori_loop(0, UNIT, spread, 0, unroll=8)
    skip = mine * stations % 8

    def one_phase(s, carry):
        held = phase_rows[pl.ds(pl.multiple_of((skip + s) * UNIT, UNIT), UNIT), :].T
        angles = jnp.concatenate([held[:CHAVG], held[CHAVG:]], 1)
        sine, cosine = sin_cos(angles)
        here = pl.ds(pl.multiple_of(s * RADIX_A, RADIX_A), RADIX_A)
        for g in range(QUADS):
            trig[0, g, here, :] = cosine[g * RADIX_A:(g + 1) * RADIX_A]
            trig[1, g, here, :] = sine[g * RADIX_A:(g + 1) * RADIX_A]
        return carry

    lax.fori_loop(0, stations, one_phase, 0, unroll=2)

    @pl.when(c == h)
    def _():
        own_delays().wait()

    @pl.when(c != h)
    def _():
        delay_copy().wait_recv()

    hear = pltpu.make_async_copy(rxd, heard, own_sems.at[1])
    hear.start()
    hear.wait()

    def widen(slot, r):
        def one(j, carry):
            held = rxu[slot, r, :, pl.ds(pl.multiple_of(j * LANES, LANES), LANES)].astype(F32)
            series[pl.ds(r * stations * depth + slot * UNIT + j, stations, stride=depth), :] = held
            return carry
        lax.fori_loop(0, UNIT, one, 0, unroll=16)

    def take(slot):
        for r in range(2):
            arrived(slot, r)
            widen(slot, r)

    def blank(slot):
        def one(i, carry):
            series[pl.ds(pl.multiple_of(i * depth + slot * UNIT, 8), UNIT), :] = jnp.zeros((UNIT, LANES), F32)
            return carry
        lax.fori_loop(0, 2 * stations, one, 0)

    def clear_tail(i, carry):
        series[pl.ds(pl.multiple_of(i * depth + (frames + AHEAD) * UNIT, 8), 8), :] = jnp.zeros((8, LANES), F32)
        return carry

    lax.fori_loop(0, 2 * stations, clear_tail, 0)

    def cross(slot):
        for r in range(2):
            arrived(slot, r)
            sample_copy(0, rxu.at[slot, r], at(u, 0, 1), slot - 4, r).start()
            if slot < 6:
                @pl.when(below)
                def _(slot=slot, r=r):
                    sample_copy(1, rxu.at[slot, r], at(lower, 0, 1), slot + 4, r).start()

                @pl.when(jnp.logical_not(top))
                def _(slot=slot, r=r):
                    arrived(slot + 4, r)
                    sample_copy(2, rxu.at[slot + 4, r], at(u, 0, 1), slot, r).start()
                    widen(slot + 4, r)
            widen(slot, r)

    @pl.when(c == h)
    def _():
        for i, r in both:
            own_copy(i, r).wait()
            widen(i, r)

    @pl.when(is00)
    def _():
        for slot in range(4, 8):
            cross(slot)

    @pl.when(is10)
    def _():
        for slot in range(4):
            for r in range(2):
                arrived(slot, r)

                @pl.when(below)
                def _(slot=slot, r=r):
                    where, into = (at(lower, 1, 0), 8 + slot) if slot < 2 else (at(lower, 1, 1), 4 + slot)
                    sample_copy(1, rxu.at[slot, r], where, into, r).start()
                if slot >= 2:
                    @pl.when(jnp.logical_not(top))
                    def _(slot=slot, r=r):
                        arrived(slot + 6, r)
                        sample_copy(2, rxu.at[slot + 6, r], at(u, 1, 1), slot + 2, r).start()
                        widen(slot + 6, r)
                widen(slot, r)
        for slot in range(4, 8):
            take(slot)

        @pl.when(top)
        def _():
            pl.semaphore_signal(crossed, inc=1, device_id=at(u, 1, 1), device_id_type=MESH)

    @pl.when(is01)
    def _():
        for slot in range(4):
            take(slot)

    @pl.when((c == 1) & jnp.logical_not(top))
    def _():
        for slot in range(4, 7):
            take(slot)

    @pl.when((c == 1) & top)
    def _():
        for slot in range(4, 8):
            blank(slot)

    @pl.when(top)
    def _():
        for slot in range(8, 10):
            blank(slot)

    @pl.when(is11 & top)
    def _():
        pl.semaphore_wait(crossed, 1)

    lane16 = lax.broadcasted_iota(I32, (RADIX_A, LANES), 1)

    def frame_copy(j, part):
        rows_of = pl.ds(part * PART, PART)
        where = (2 * u + (j + 1) // 2 % 2, j % 2 * 2 + c)
        return remote(tx2.at[j, rows_of], rx2.at[mine, rows_of], s2.at[0], r2.at[part], where)

    def own_frame():
        return pltpu.make_async_copy(tx2.at[e], rx2.at[mine], own_sems.at[6])

    def dispatch(f):
        @pl.when(f == e)
        def _():
            own_frame().start()

        @pl.when(f != e)
        def _():
            for part in range(OUTCH // PART):
                frame_copy(f, part).start()

    def spectra(step, carry):
        there_h = jnp.where(step == 1, h, jnp.where(step == 3, h, 1 - h))
        there_m = jnp.where((step == 1) | (step == 2), (m + 1) % 2, m)
        f = jnp.where((c == 0) & (m < 2), (there_h + there_m) % 2 * 2 + there_m, step)

        for slot in range(7, 10):
            @pl.when((step == slot - 6) & (c == 1) & jnp.logical_not(top))
            def _(slot=slot):
                take(slot)

        for s in range(stations):
            offset = f * NCHAN + heard[0, f * stations + s]
            row, shift = offset // LANES, offset % LANES
            for r in range(2):
                parts = [
                    pltpu.roll(
                        series[pl.ds((r * stations + s) * depth + row + q, RADIX_A, stride=QUADS), :],
                        (LANES - shift) % LANES, 1)
                    for q in range(QUADS + 1)
                ]
                for q in range(QUADS):
                    cut = jnp.where(lane16 < LANES - shift, parts[q], parts[q + 1])
                    windows[(2 * s + r) * RADIX_A:(2 * s + r + 1) * RADIX_A, q * LANES:(q + 1) * LANES] = cut.astype(BF16)
        passed = jnp.dot(first[...], windows[...], preferred_element_type=F32)
        real, imag = passed[:sk], passed[sk:]
        turned[:, 0:RADIX_B] = (real * twist[0] + imag * twist[1]).astype(BF16)
        turned[:, RADIX_B:] = (imag * twist[0] - real * twist[1]).astype(BF16)
        for g in range(QUADS):
            channels = jnp.dot(turned[...], second[:, g * 2 * LANES:(g + 1) * 2 * LANES], preferred_element_type=F32)
            real, imag = channels[:, :LANES], channels[:, LANES:]
            cosine, sine = trig[0, g], trig[1, g]
            turned_re = (real * cosine - imag * sine).reshape(stations, RADIX_A, LANES)
            turned_im = (real * sine + imag * cosine).reshape(stations, RADIX_A, LANES)
            planes[:, g * RADIX_A:(g + 1) * RADIX_A, :] = turned_re
            planes[:, CHAVG + g * RADIX_A:CHAVG + (g + 1) * RADIX_A, :] = turned_im
        for s in range(stations):
            rows[pl.ds(s, OUTCH, stride=stations), :] = planes[s].T
        tx2[f] = rows[...].astype(BF16).reshape(OUTCH, stations, LANES)

        @pl.when(c == 0)
        def _():
            dispatch(f)

        @pl.when((c == 1) & (step >= 1))
        def _():
            dispatch(step - 1)

        return carry


    lax.fori_loop(0, frames, spectra, 0)

    @pl.when(c == 1)
    def _():
        for j in range(frames - 1, frames):
            dispatch(j)

    own_bins.wait()
    rest = rxb.at[pl.ds(0, owners - 1)]
    remote(rest, rest, s0.at[1], r0.at[1], (tm, pair)).wait_recv()
    line = rxb[0]
    for t in range(1, owners):
        line = line + rxb[t]
    span = jnp.broadcast_to(line, (all_frames, LANES))
    across = lax.broadcasted_iota(I32, (all_frames, LANES), 1)
    down = lax.broadcasted_iota(I32, (all_frames, LANES), 0)
    column = jnp.max(jnp.where(across == down, span, 0), 1, keepdims=True)
    found = jnp.max(jnp.where((span == column) & (across < down), across, -1), 1, keepdims=True)
    tables[0:all_frames] = jnp.broadcast_to(jnp.where(found < 0, all_frames, found), (all_frames, LANES))
    down = lax.broadcasted_iota(I32, (BINS, LANES), 0)
    across = lax.broadcasted_iota(I32, (BINS, LANES), 1)
    found = jnp.max(jnp.where(jnp.broadcast_to(line, (BINS, LANES)) == down + 1, across, -1), 1, keepdims=True)
    tables[all_frames:] = jnp.broadcast_to(jnp.where(found < 0, all_frames, found), (BINS, LANES))
    tell = pltpu.make_async_copy(tables, orders, own_sems.at[2])
    tell.start()

    lane32 = lax.broadcasted_iota(I32, (pairs * stations, LANES), 1)
    half = pairs * stations // 2

    @pl.when(e < frames)
    def _():
        own_frame().wait()

        def gram(row, carry):
            o = row % (OUTCH // 2) * 2 + row // (OUTCH // 2)
            left = jnp.concatenate([rx2[g, row].astype(F32) for g in range(pairs)], 0)
            swapped = pltpu.roll(left, CHAVG, 1)
            swapped = jnp.where(lane32 < CHAVG, -swapped, swapped)
            both = jnp.concatenate([left, swapped], 0).astype(BF16)
            right = jnp.concatenate([both, both], 0)
            made = lax.dot_general(left.astype(BF16), right, (((1,), (1,)), ((), ())), preferred_element_type=F32)
            gs[pl.ds(o, half, stride=OUTCH), :] = jnp.where(lane32[:half] < CHAVG, made[:half], made[half:])
            return carry

        def one_part(part, carry):
            rest = rx2.at[pl.ds(0, pairs - 1), pl.ds(0, PART)]
            remote(rest, rest, s2.at[0], r2.at[part], (tm, pair)).wait_recv()
            lax.fori_loop(0, PART, lambda i, inner: gram(part * PART + i, inner), 0, unroll=16)
            return carry

        lax.fori_loop(0, OUTCH // PART, one_part, 0)
        def turn(i, carry):
            block = gs[pl.ds(pl.multiple_of(i * OUTCH, OUTCH), OUTCH), :].T * (1.0 / CHAVG)
            for upper in range(2):
                row = i + half * upper
                a, p = row // GROUP_ST, row % GROUP_ST
                for ri in range(2):
                    for b in range(NGRP):
                        top_row = upper * CHAVG + ri * 32 + b * GROUP_ST
                        tscr[pl.ds(p * 256 + ri * 128 + a * NGRP + b, GROUP_ST, stride=NBLK), :] = block[top_row:top_row + GROUP_ST]
            return carry

        lax.fori_loop(0, half, turn, 0, unroll=8)

        def pack(p, carry):
            real = tscr[pl.ds(pl.multiple_of(p * 256, 256), 128), :].reshape(GROUP_ST, NBLK, LANES)
            imag = tscr[pl.ds(pl.multiple_of(p * 256 + 128, 128), 128), :].reshape(GROUP_ST, NBLK, LANES)
            q = lax.broadcasted_iota(I32, (GROUP_ST, NBLK, LANES), 0)
            ab = lax.broadcasted_iota(I32, (GROUP_ST, NBLK, LANES), 1)
            a, b = ab // NGRP, ab % NGRP
            upper = (a < b) | ((a == b) & (p <= q))
            tx3[pl.ds(p % 4 * GROUP_ST, GROUP_ST), p // 4] = jnp.where(upper, real, imag).astype(BF16)
            return carry

        lax.fori_loop(0, GROUP_ST, pack, 0, unroll=2)
        frame = tm // 2 * 2 * frames + c * frames + e

        def send(step, carry):
            d = (me + SLICES // 2 + step) % SLICES

            @pl.when(d != me)
            def _():
                remote(tx3.at[d], rx3.at[frame], s3.at[0], r3.at[0], place_of(d)).start()

            @pl.when(d == me)
            def _():
                pltpu.make_async_copy(tx3.at[d], rx3.at[frame], own_sems.at[3]).start()
            return carry

        lax.fori_loop(0, SLICES, send, 0, unroll=16)

    tell.wait()

    def picked(step, order):
        value = order[0]
        for i in range(1, len(order)):
            value = jnp.where(step == i, order[i], value)
        return value

    def across(k):
        return (tm + k) % 2 + (tm // 2 + k // 2) % 2 * 2 + (tm // 4 + k // 4) % 2 * 4

    @pl.when(me < SLICES)
    def _():
        @pl.when(e < frames)
        def _():
            pltpu.make_async_copy(tx3.at[0], rx3.at[0], own_sems.at[3]).wait()
            rest = rx3.at[pl.ds(0, all_frames - 1)]
            remote(rest, rest, s3.at[0], r3.at[0], (tm, pair)).wait_recv()

        @pl.when(e >= frames)
        def _():
            remote(rx3, rx3, s3.at[0], r3.at[0], (tm, pair)).wait_recv()

        sums[all_frames] = jnp.zeros((2 * NBLK, LANES), F32)

        def add(f, carry):
            sums[f] = sums[orders[f, 0]] + rx3[f].reshape(2 * NBLK, LANES).astype(F32)
            return carry

        lax.fori_loop(0, all_frames, add, 0, unroll=4)

        def give(step, carry):
            t = (tm + step) % owners
            for i in range(bins_here):
                held = sums[orders[all_frames + t * bins_here + i, 0]].astype(BF16)
                tx4[t, i * 2 * NBLK:(i + 1) * 2 * NBLK, :] = held

            @pl.when(t != tm)
            def _():
                remote(tx4.at[t], rx4.at[me], s4.at[0], r4.at[me], (t, pair)).start()
            return carry

        lax.fori_loop(1, owners + 1, give, 0, unroll=2)
        pltpu.make_async_copy(tx4.at[tm], rx4.at[me], own_sems.at[4]).start()

    sources = SLICES // pairs

    def pass_on(d, other):
        return remote(rx4.at[d], rx4.at[d], s5.at[0], r4.at[d], (tm, other))

    def landing(d):
        def one(i, carry):
            held = rx4[d, pl.ds(pl.multiple_of(i * NBLK, NBLK), NBLK), :].astype(F32)
            landed[pl.ds(i // 2 * NBLK * 2 * SLICES + i % 2 * SLICES + d, NBLK, stride=2 * SLICES), :] = held
            return carry

        lax.fori_loop(0, 2 * bins_here, one, 0, unroll=2 * bins_here)

    def nearest(step):
        if owners != 8:
            return (tm + step) % sources
        return across(picked(step, (0, 1, 2, 3, 4, 5, 6, 7)))

    def first_hop(step, carry):
        i = nearest(step)
        d = i * pairs + pair

        @pl.when(d == me)
        def _():
            pltpu.make_async_copy(tx4.at[tm], rx4.at[d], own_sems.at[4]).wait()

        @pl.when(d != me)
        def _():
            remote(rx4.at[d], rx4.at[d], s4.at[0], r4.at[d], (tm, pair)).wait_recv()

        for n in range(1, halves):
            pass_on(d, (pair + 2 * n) % pairs).start()
        pass_on(d, pair + 1 - 2 * c).start()
        landing(d)
        return carry

    lax.fori_loop(0, sources, first_hop, 0)

    def second_hop(step, carry):
        i = nearest(step)
        for n in range(1, halves):
            d = i * pairs + (pair + 2 * n) % pairs
            remote(rx4.at[d], rx4.at[d], s4.at[0], r4.at[d], (tm, pair)).wait_recv()
            pass_on(d, pair + 1 - 2 * c).start()
            landing(d)
        beside(i, 0)
        return carry

    def beside(i, n):
        d = i * pairs + (pair + 1 - 2 * c + 2 * n) % pairs
        remote(rx4.at[d], rx4.at[d], s4.at[0], r4.at[d], (tm, pair)).wait_recv()
        landing(d)

    lax.fori_loop(0, sources, second_hop, 0)

    def third_hop(step, carry):
        for n in range(1, halves):
            beside(nearest(step), n)
        return carry

    lax.fori_loop(0, sources, third_hop, 0)

    place = lax.broadcasted_iota(I32, (GROUP_ST, LANES), 0)
    none = jnp.zeros((GROUP_ST, LANES), I32)
    span = 2 * SLICES

    def one_bin(b, carry):
        for k in range(slots):
            block = assignment[k]
            a, bb = block // NGRP, block % NGRP
            row, column = none + a, none + bb
            ahead, within = row < column, row == column
            here = (b * NBLK + block) * span
            there = (b * NBLK + bb * NGRP + a) * span
            for p in range(GROUP_ST):
                straight = landed[pl.ds(here + p * GROUP_ST, GROUP_ST), :]
                mirrored = landed[pl.ds(there + p, GROUP_ST, stride=GROUP_ST), :]
                upper = ahead | (within & (place >= p))
                real = jnp.where(upper, straight, mirrored)
                imag = jnp.where(upper, -mirrored, straight)
                imag = jnp.where(within & (place == p), 0.0, imag)
                out[b, k, 0, p * GROUP_ST:(p + 1) * GROUP_ST, :] = real
                out[b, k, 1, p * GROUP_ST:(p + 1) * GROUP_ST, :] = imag
        return carry

    lax.fori_loop(0, bins_here, one_bin, 0)

    rest = rxb.at[pl.ds(0, owners - 1)]
    remote(rest, rest, s0.at[1], r0.at[1], (tm, pair)).wait_send()

    @pl.when(c != h)
    def _():
        delay_copy().wait_send()

    def all_sent(ref, count, sem):
        rest = ref.at[pl.ds(0, count)]
        remote(rest, rest, sem, r4.at[0], (tm, pair)).wait_send()

    @pl.when(is00)
    def _():
        all_sent(rxu, 4, s1.at[0])

        @pl.when(below)
        def _():
            all_sent(rxu, 6, s1.at[1])

        @pl.when(jnp.logical_not(top))
        def _():
            all_sent(rxu, 2, s1.at[2])

    @pl.when(is10)
    def _():
        all_sent(rxu, 4, s1.at[0])

        @pl.when(below)
        def _():
            all_sent(rxu, 4, s1.at[1])

        @pl.when(jnp.logical_not(top))
        def _():
            all_sent(rxu, 2, s1.at[2])

    @pl.when(c == 1)
    def _():
        all_sent(rxu, 4, s1.at[0])

    @pl.when(is11 & below)
    def _():
        all_sent(rxu, 2, s1.at[1])

    @pl.when(e < frames)
    def _():
        all_sent(tx2, frames - 1, s2.at[0])

        @pl.when(me < SLICES)
        def _():
            all_sent(tx3, SLICES - 1, s3.at[0])

        @pl.when(me >= SLICES)
        def _():
            all_sent(tx3, SLICES, s3.at[0])

    @pl.when(e >= frames)
    def _():
        all_sent(tx2, frames, s2.at[0])

    @pl.when(me < SLICES)
    def _():
        all_sent(tx4, owners - 1, s4.at[0])

    all_sent(rx4, sources * (2 * halves - 1), s5.at[0])


VMEM = pl.BlockSpec(memory_space=pltpu.VMEM)
SMEM = pl.BlockSpec(memory_space=pltpu.SMEM)
ANY = pl.BlockSpec(memory_space=pl.ANY)


def body(voltages, delays, phase_model, phase_bins, assignment):
    owners, pairs = lax.axis_size("tm"), lax.axis_size("pair")
    devices = owners * pairs
    stations, samples = voltages.shape[1], voltages.shape[2]
    frames = samples // NCHAN
    slots = assignment.shape[0]
    all_frames = owners * frames
    bins_here = BINS // owners
    sk = stations * RADIX_A

    first, twist, second = section_tables(stations)
    span = (frames + AHEAD) * UNIT
    scratch = [
        pltpu.VMEM((2, 1, LANES), I32),
        pltpu.VMEM(first.shape, BF16),
        pltpu.VMEM(twist.shape, F32),
        pltpu.VMEM(second.shape, BF16),
        pltpu.VMEM((frames + AHEAD, 2, stations, NCHAN), BF16),
        pltpu.VMEM((2 * stations * (span + 8), LANES), F32),
        pltpu.VMEM((2 * sk, RADIX_B), BF16),
        pltpu.VMEM((sk, 2 * RADIX_B), BF16),
        pltpu.VMEM((stations, LANES, LANES), F32),
        pltpu.VMEM((OUTCH * stations, LANES), F32),
        pltpu.VMEM((8, NCHAN), F32),
        pltpu.VMEM((8 * UNIT, LANES), F32),
        pltpu.VMEM((2, QUADS, sk, LANES), F32),
        pltpu.VMEM((frames, OUTCH, stations, LANES), BF16),
        pltpu.VMEM((pairs, OUTCH, stations, LANES), BF16),
        pltpu.VMEM((pairs * stations // 2 * OUTCH, LANES), F32),
        pltpu.VMEM((2 * pairs * stations * pairs * stations, LANES), F32),
        pltpu.VMEM((SLICES, 2, NBLK, LANES), BF16),
        pltpu.VMEM((all_frames, 2, NBLK, LANES), BF16),
        pltpu.VMEM((all_frames + 1, 2 * NBLK, LANES), F32),
        pltpu.VMEM((owners, bins_here * 2 * NBLK, LANES), BF16),
        pltpu.VMEM((SLICES, bins_here * 2 * NBLK, LANES), BF16),
        pltpu.VMEM((bins_here * NBLK * 2 * SLICES, LANES), F32),
        pltpu.VMEM((1, LANES), I32),
        pltpu.VMEM((owners, 1, LANES), I32),
        pltpu.SMEM((1, LANES), I32),
        pltpu.VMEM((all_frames + BINS, LANES), I32),
        pltpu.SMEM((all_frames + BINS, LANES), I32),
        pltpu.SemaphoreType.DMA((4,)),
        pltpu.SemaphoreType.DMA((2,)),
        pltpu.SemaphoreType.DMA((2,)),
        pltpu.SemaphoreType.DMA((3,)),
        pltpu.SemaphoreType.DMA((frames + AHEAD, 2)),
        pltpu.SemaphoreType.DMA((1,)),
        pltpu.SemaphoreType.DMA((OUTCH // PART,)),
        pltpu.SemaphoreType.DMA((1,)),
        pltpu.SemaphoreType.DMA((1,)),
        pltpu.SemaphoreType.DMA((1,)),
        pltpu.SemaphoreType.DMA((SLICES,)),
        pltpu.SemaphoreType.DMA((1,)),
        pltpu.SemaphoreType.DMA((7,)),
        pltpu.SemaphoreType.DMA((4, 2)),
        pltpu.SemaphoreType.REGULAR,
    ]
    result = pl.pallas_call(
        functools.partial(fused_kernel, (owners, pairs, frames, stations, slots)),
        out_shape=pltpu.VMEM((bins_here, slots, 2, GROUP_ST * GROUP_ST, OUTCH), F32),
        in_specs=[SMEM, SMEM, SMEM, ANY, ANY, ANY, ANY, ANY],
        out_specs=VMEM,
        scratch_shapes=scratch,
        compiler_params=pltpu.CompilerParams(
            collective_id=0, has_side_effects=True, vmem_limit_bytes=56 * 1024 * 1024),
        name="correlate",
    )(delays.T, phase_bins, assignment, voltages, phase_model, first, twist, second)
    return result


def solution(mesh):
    in_specs = (P(None, "pair", "tm"), P("pair", "tm"), P(), P("tm"), P("pair"))
    out_specs = P("tm", "pair", None, None, None)
    return jax.shard_map(body, mesh=mesh, in_specs=in_specs, out_specs=out_specs, check_vma=False)
```

```python
import functools
import math

import jax
import jax.numpy as jnp
import numpy as np
from jax import lax
from jax.experimental import pallas as pl
from jax.experimental.pallas import tpu as pltpu
from jax.sharding import PartitionSpec as P

NCHAN = 8192
GROUP_ST = 8
RADIX_A = 16
CHAVG = 64
NGRP = 4
NBLK = 16
OUTCH = 128
BINS = 32
DELAY_MAX = 49152
LANES = 128
RADIX_B = NCHAN // RADIX_A
QUADS = RADIX_B // LANES
UNIT = NCHAN // LANES
AHEAD = DELAY_MAX // NCHAN
SLICES = GROUP_ST * GROUP_ST // 2
PART = 16
F32, BF16, I32 = jnp.float32, jnp.bfloat16, jnp.int32
MESH = pl.DeviceIdType.MESH


def section_tables(stations):
    a, b = np.arange(RADIX_A), np.arange(RADIX_B)
    angle = ((a[:, None] * a[None, :]) % RADIX_A).astype(np.float32) * np.float32(2.0 * math.pi / RADIX_A)
    cos_a = (np.cos(angle) * np.float32(1.0 / math.sqrt(RADIX_A))).astype(np.float32)
    sin_a = (np.sin(angle) * np.float32(1.0 / math.sqrt(RADIX_A))).astype(np.float32)
    small = np.stack([np.stack([cos_a, sin_a], 1), np.stack([-sin_a, cos_a], 1)], 0)
    first = np.einsum("st,pkrn->psktrn", np.eye(stations, dtype=np.float32), small)
    rows = 2 * stations * RADIX_A
    first = first.reshape(rows, rows)
    turn = (a[:, None] * b[None, :]).astype(np.float32) * np.float32(2.0 * math.pi / NCHAN)
    twist = np.stack([np.cos(turn), np.sin(turn)]).astype(np.float32)
    twist = np.tile(twist, (1, stations, 1))
    angle = ((b[:, None] * b[None, :]) % RADIX_B).astype(np.float32) * np.float32(2.0 * math.pi / RADIX_B)
    cos_b = (np.cos(angle) * np.float32(1.0 / math.sqrt(RADIX_B))).astype(np.float32)
    sin_b = (np.sin(angle) * np.float32(1.0 / math.sqrt(RADIX_B))).astype(np.float32)
    second = np.stack([np.stack([cos_b, -sin_b], 1), np.stack([sin_b, cos_b], 1)], 0)
    second = second.reshape(2, RADIX_B, 2, OUTCH // 2, 2, QUADS).transpose(0, 1, 5, 2, 4, 3)
    second = second.reshape(2 * RADIX_B, 2 * RADIX_B)
    return jnp.asarray(first, BF16), jnp.asarray(twist), jnp.asarray(second, BF16)


def sin_cos(x):
    turns = jnp.round(x * (2.0 / math.pi))
    r = x - turns * 1.5703125
    r = r - turns * 4.837512969970703125e-4
    r = r - turns * 7.54978995489188216e-8
    z = r * r
    s = r + r * z * ((-1.9515295891e-4 * z + 8.3321608736e-3) * z - 1.6666654611e-1)
    c = 1.0 - 0.5 * z + z * z * ((2.443315711809948e-5 * z - 1.388731625493765e-3) * z + 4.166664568298827e-2)
    size = jnp.abs(turns)
    odd = size == 1.0
    far = size == 2.0
    sine = jnp.where(odd, c, s)
    cosine = jnp.where(odd, s, c)
    sine = jnp.where(far | (turns == -1.0), -sine, sine)
    cosine = jnp.where(far | (turns == 1.0), -cosine, cosine)
    return sine, cosine


def fused_kernel(dims, delays, phase_bins, assignment, voltages, phase_model, first_hbm, twist_hbm, second_hbm, out,
                 small, first, twist, second, rxu, series, windows, turned, planes, rows, phases, phase_rows, trig,
                 tx2, rx2, gs, tscr, tx3, rx3, sums, tx4, rx4, landed, rxd, rxb, heard, tables, orders,
                 load_sems, s0, r0, s1, r1, s2, r2, s3, r3, s4, r4, s5, own_sems, unit_sems, crossed):
    owners, pairs, frames, stations, slots = dims
    devices, layers, halves = owners * pairs, owners // 2, pairs // 2
    all_frames = owners * frames
    bins_here = BINS // owners
    sk = stations * RADIX_A
    depth = (frames + AHEAD) * UNIT + 8
    tm, pair = lax.axis_index("tm"), lax.axis_index("pair")
    u, h, m, c = tm // 2, tm % 2, pair // 2, pair % 2
    me = tm * pairs + pair
    mine = 2 * m + h
    e = jnp.where(m < 2, (h + m) % 2 * 2 + m, frames)
    top = u == layers - 1

    def place_of(device):
        return (device // pairs, device % pairs)

    def remote(src, dst, send_sem, recv_sem, where):
        return pltpu.make_async_remote_copy(
            src_ref=src, dst_ref=dst, send_sem=send_sem, recv_sem=recv_sem, device_id=where, device_id_type=MESH)

    loads = [
        pltpu.make_async_copy(first_hbm, first, load_sems.at[0]),
        pltpu.make_async_copy(twist_hbm, twist, load_sems.at[1]),
        pltpu.make_async_copy(second_hbm, second, load_sems.at[2]),
        pltpu.make_async_copy(
            phase_model.at[pl.ds(pl.multiple_of(mine * stations // 8 * 8, 8), 8)], phases, load_sems.at[3]),
    ]
    for copy in loads:
        copy.start()

    barrier = pltpu.get_barrier_semaphore()

    def greet(step, carry):
        pl.semaphore_signal(barrier, inc=1, device_id=place_of((me + step) % devices), device_id_type=MESH)
        return carry

    lax.fori_loop(1, devices, greet, 0, unroll=True) if devices < 64 else lax.fori_loop(1, devices, greet, 0)
    lane = lax.broadcasted_iota(I32, (1, LANES), 1)
    listed, marked = jnp.zeros((1, LANES), I32), jnp.zeros((1, LANES), I32)
    for i in range(stations * frames):
        listed = jnp.where(lane == i, delays[i // stations, i % stations], listed)
    for i in range(frames):
        marked = jnp.where(lane == tm * frames + i, phase_bins[i] + 1, marked)
    small[0] = listed
    small[1] = marked
    pl.semaphore_wait(barrier, devices - 1)

    def delay_copy():
        return remote(small.at[0], rxd, s0.at[0], r0.at[0], (2 * u + c, 2 * m + h))

    def own_delays():
        return pltpu.make_async_copy(small.at[0], rxd, own_sems.at[0])

    @pl.when(c == h)
    def _():
        own_delays().start()

    @pl.when(c != h)
    def _():
        delay_copy().start()

    def start_bins(step, carry):
        remote(small.at[1], rxb.at[tm], s0.at[1], r0.at[1], ((tm + step) % owners, pair)).start()
        return carry

    lax.fori_loop(1, owners, start_bins, 0)
    own_bins = pltpu.make_async_copy(small.at[1], rxb.at[tm], own_sems.at[5])
    own_bins.start()

    def at(layer, half, core):
        return (2 * layer + half, 2 * m + core)

    def sample_copy(group, src, where, slot, r):
        return remote(src, rxu.at[slot, r], s1.at[group], r1.at[slot, r], where)

    def own_unit(i, r):
        return voltages.at[r, :, pl.ds(i * NCHAN, NCHAN)]

    def own_copy(i, r):
        return pltpu.make_async_copy(own_unit(i, r), rxu.at[i, r], unit_sems.at[i, r])

    def arrived(slot, r):
        sample_copy(0, rxu.at[slot, r], at(u, h, c), slot, r).wait_recv()

    below = u > 0
    lower = jnp.maximum(u - 1, 0)
    is00, is10 = (h == 0) & (c == 0), (h == 1) & (c == 0)
    is01, is11 = (h == 0) & (c == 1), (h == 1) & (c == 1)
    both = [(i, r) for i in range(4) for r in range(2)]

    @pl.when(is10)
    def _():
        for i, r in both:
            sample_copy(0, own_unit(i, r), at(u, 0, 0), 4 + i, r).start()

    @pl.when(is01)
    def _():
        for i, r in both:
            sample_copy(0, own_unit(i, r), at(u, 1, 0), i, r).start()

    @pl.when(is11)
    def _():
        for i, r in both:
            sample_copy(0, own_unit(i, r), at(u, 1, 0), 4 + i, r).start()

        @pl.when(below)
        def _():
            for i, r in both[:4]:
                sample_copy(1, own_unit(i, r), at(lower, 1, 1), 8 + i, r).start()

    @pl.when(c == h)
    def _():
        for i, r in both:
            own_copy(i, r).start()

    @pl.when(is00 & below)
    def _():
        for i, r in both:
            where, slot = (at(lower, 0, 0), 8 + i) if i < 2 else (at(lower, 0, 1), 4 + i)
            sample_copy(1, own_unit(i, r), where, slot, r).start()

    for copy in loads:
        copy.wait()

    def spread(j, carry):
        phase_rows[pl.ds(j, 8, stride=UNIT), :] = phases[:, pl.ds(pl.multiple_of(j * LANES, LANES), LANES)]
        return carry

    lax.fori_loop(0, UNIT, spread, 0, unroll=8)
    skip = mine * stations % 8

    def one_phase(s, carry):
        held = phase_rows[pl.ds(pl.multiple_of((skip + s) * UNIT, UNIT), UNIT), :].T
        angles = jnp.concatenate([held[:CHAVG], held[CHAVG:]], 1)
        sine, cosine = sin_cos(angles)
        here = pl.ds(pl.multiple_of(s * RADIX_A, RADIX_A), RADIX_A)
        for g in range(QUADS):
            trig[0, g, here, :] = cosine[g * RADIX_A:(g + 1) * RADIX_A]
            trig[1, g, here, :] = sine[g * RADIX_A:(g + 1) * RADIX_A]
        return carry

    lax.fori_loop(0, stations, one_phase, 0, unroll=2)

    @pl.when(c == h)
    def _():
        own_delays().wait()

    @pl.when(c != h)
    def _():
        delay_copy().wait_recv()

    hear = pltpu.make_async_copy(rxd, heard, own_sems.at[1])
    hear.start()
    hear.wait()

    def widen(slot, r):
        def one(j, carry):
            held = rxu[slot, r, :, pl.ds(pl.multiple_of(j * LANES, LANES), LANES)].astype(F32)
            series[pl.ds(r * stations * depth + slot * UNIT + j, stations, stride=depth), :] = held
            return carry
        lax.fori_loop(0, UNIT, one, 0, unroll=16)

    def take(slot):
        for r in range(2):
            arrived(slot, r)
            widen(slot, r)

    def blank(slot):
        def one(i, carry):
            series[pl.ds(pl.multiple_of(i * depth + slot * UNIT, 8), UNIT), :] = jnp.zeros((UNIT, LANES), F32)
            return carry
        lax.fori_loop(0, 2 * stations, one, 0)

    def clear_tail(i, carry):
        series[pl.ds(pl.multiple_of(i * depth + (frames + AHEAD) * UNIT, 8), 8), :] = jnp.zeros((8, LANES), F32)
        return carry

    lax.fori_loop(0, 2 * stations, clear_tail, 0)

    def cross(slot):
        for r in range(2):
            arrived(slot, r)
            sample_copy(0, rxu.at[slot, r], at(u, 0, 1), slot - 4, r).start()
            if slot < 6:
                @pl.when(below)
                def _(slot=slot, r=r):
                    sample_copy(1, rxu.at[slot, r], at(lower, 0, 1), slot + 4, r).start()

                @pl.when(jnp.logical_not(top))
                def _(slot=slot, r=r):
                    arrived(slot + 4, r)
                    sample_copy(2, rxu.at[slot + 4, r], at(u, 0, 1), slot, r).start()
                    widen(slot + 4, r)
            widen(slot, r)

    @pl.when(c == h)
    def _():
        for i, r in both:
            own_copy(i, r).wait()
            widen(i, r)

    @pl.when(is00)
    def _():
        for slot in range(4, 8):
            cross(slot)

    @pl.when(is10)
    def _():
        for slot in range(4):
            for r in range(2):
                arrived(slot, r)

                @pl.when(below)
                def _(slot=slot, r=r):
                    where, into = (at(lower, 1, 0), 8 + slot) if slot < 2 else (at(lower, 1, 1), 4 + slot)
                    sample_copy(1, rxu.at[slot, r], where, into, r).start()
                if slot >= 2:
                    @pl.when(jnp.logical_not(top))
                    def _(slot=slot, r=r):
                        arrived(slot + 6, r)
                        sample_copy(2, rxu.at[slot + 6, r], at(u, 1, 1), slot + 2, r).start()
                        widen(slot + 6, r)
                widen(slot, r)
        for slot in range(4, 8):
            take(slot)

        @pl.when(top)
        def _():
            pl.semaphore_signal(crossed, inc=1, device_id=at(u, 1, 1), device_id_type=MESH)

    @pl.when(is01)
    def _():
        for slot in range(4):
            take(slot)

    @pl.when((c == 1) & jnp.logical_not(top))
    def _():
        for slot in range(4, 7):
            take(slot)

    @pl.when((c == 1) & top)
    def _():
        for slot in range(4, 8):
            blank(slot)

    @pl.when(top)
    def _():
        for slot in range(8, 10):
            blank(slot)

    @pl.when(is11 & top)
    def _():
        pl.semaphore_wait(crossed, 1)

    lane16 = lax.broadcasted_iota(I32, (RADIX_A, LANES), 1)

    def frame_copy(j, part):
        rows_of = pl.ds(part * PART, PART)
        where = (2 * u + (j + 1) // 2 % 2, j % 2 * 2 + c)
        return remote(tx2.at[j, rows_of], rx2.at[mine, rows_of], s2.at[0], r2.at[part], where)

    def own_frame():
        return pltpu.make_async_copy(tx2.at[e], rx2.at[mine], own_sems.at[6])

    def dispatch(f):
        @pl.when(f == e)
        def _():
            own_frame().start()

        @pl.when(f != e)
        def _():
            for part in range(OUTCH // PART):
                frame_copy(f, part).start()

    def spectra(step, carry):
        there_h = jnp.where(step == 1, h, jnp.where(step == 3, h, 1 - h))
        there_m = jnp.where((step == 1) | (step == 2), (m + 1) % 2, m)
        f = jnp.where((c == 0) & (m < 2), (there_h + there_m) % 2 * 2 + there_m, step)

        for slot in range(7, 10):
            @pl.when((step == slot - 6) & (c == 1) & jnp.logical_not(top))
            def _(slot=slot):
                take(slot)

        for s in range(stations):
            offset = f * NCHAN + heard[0, f * stations + s]
            row, shift = offset // LANES, offset % LANES
            for r in range(2):
                parts = [
                    pltpu.roll(
                        series[pl.ds((r * stations + s) * depth + row + q, RADIX_A, stride=QUADS), :],
                        (LANES - shift) % LANES, 1)
                    for q in range(QUADS + 1)
                ]
                for q in range(QUADS):
                    cut = jnp.where(lane16 < LANES - shift, parts[q], parts[q + 1])
                    windows[(2 * s + r) * RADIX_A:(2 * s + r + 1) * RADIX_A, q * LANES:(q + 1) * LANES] = cut.astype(BF16)
        passed = jnp.dot(first[...], windows[...], preferred_element_type=F32)
        real, imag = passed[:sk], passed[sk:]
        turned[:, 0:RADIX_B] = (real * twist[0] + imag * twist[1]).astype(BF16)
        turned[:, RADIX_B:] = (imag * twist[0] - real * twist[1]).astype(BF16)
        for g in range(QUADS):
            channels = jnp.dot(turned[...], second[:, g * 2 * LANES:(g + 1) * 2 * LANES], preferred_element_type=F32)
            real, imag = channels[:, :LANES], channels[:, LANES:]
            cosine, sine = trig[0, g], trig[1, g]
            turned_re = (real * cosine - imag * sine).reshape(stations, RADIX_A, LANES)
            turned_im = (real * sine + imag * cosine).reshape(stations, RADIX_A, LANES)
            planes[:, g * RADIX_A:(g + 1) * RADIX_A, :] = turned_re
            planes[:, CHAVG + g * RADIX_A:CHAVG + (g + 1) * RADIX_A, :] = turned_im
        for s in range(stations):
            rows[pl.ds(s, OUTCH, stride=stations), :] = planes[s].T
        tx2[f] = rows[...].astype(BF16).reshape(OUTCH, stations, LANES)

        @pl.when(c == 0)
        def _():
            dispatch(f)

        @pl.when((c == 1) & (step >= 1))
        def _():
            dispatch(step - 1)

        return carry


    lax.fori_loop(0, frames, spectra, 0)

    @pl.when(c == 1)
    def _():
        for j in range(frames - 1, frames):
            dispatch(j)

    own_bins.wait()
    rest = rxb.at[pl.ds(0, owners - 1)]
    remote(rest, rest, s0.at[1], r0.at[1], (tm, pair)).wait_recv()
    line = rxb[0]
    for t in range(1, owners):
        line = line + rxb[t]
    span = jnp.broadcast_to(line, (all_frames, LANES))
    across = lax.broadcasted_iota(I32, (all_frames, LANES), 1)
    down = lax.broadcasted_iota(I32, (all_frames, LANES), 0)
    column = jnp.max(jnp.where(across == down, span, 0), 1, keepdims=True)
    found = jnp.max(jnp.where((span == column) & (across < down), across, -1), 1, keepdims=True)
    tables[0:all_frames] = jnp.broadcast_to(jnp.where(found < 0, all_frames, found), (all_frames, LANES))
    down = lax.broadcasted_iota(I32, (BINS, LANES), 0)
    across = lax.broadcasted_iota(I32, (BINS, LANES), 1)
    found = jnp.max(jnp.where(jnp.broadcast_to(line, (BINS, LANES)) == down + 1, across, -1), 1, keepdims=True)
    tables[all_frames:] = jnp.broadcast_to(jnp.where(found < 0, all_frames, found), (BINS, LANES))
    tell = pltpu.make_async_copy(tables, orders, own_sems.at[2])
    tell.start()

    lane32 = lax.broadcasted_iota(I32, (pairs * stations, LANES), 1)
    half = pairs * stations // 2

    @pl.when(e < frames)
    def _():
        own_frame().wait()

        def gram(row, carry):
            o = row % (OUTCH // 2) * 2 + row // (OUTCH // 2)
            left = jnp.concatenate([rx2[g, row].astype(F32) for g in range(pairs)], 0)
            swapped = pltpu.roll(left, CHAVG, 1)
            swapped = jnp.where(lane32 < CHAVG, -swapped, swapped)
            both = jnp.concatenate([left, swapped], 0).astype(BF16)
            right = jnp.concatenate([both, both], 0)
            made = lax.dot_general(left.astype(BF16), right, (((1,), (1,)), ((), ())), preferred_element_type=F32)
            gs[pl.ds(o, half, stride=OUTCH), :] = jnp.where(lane32[:half] < CHAVG, made[:half], made[half:])
            return carry

        def one_part(part, carry):
            rest = rx2.at[pl.ds(0, pairs - 1), pl.ds(0, PART)]
            remote(rest, rest, s2.at[0], r2.at[part], (tm, pair)).wait_recv()
            lax.fori_loop(0, PART, lambda i, inner: gram(part * PART + i, inner), 0, unroll=16)
            return carry

        lax.fori_loop(0, OUTCH // PART, one_part, 0)
        def turn(i, carry):
            block = gs[pl.ds(pl.multiple_of(i * OUTCH, OUTCH), OUTCH), :].T * (1.0 / CHAVG)
            for upper in range(2):
                row = i + half * upper
                a, p = row // GROUP_ST, row % GROUP_ST
                for ri in range(2):
                    for b in range(NGRP):
                        top_row = upper * CHAVG + ri * 32 + b * GROUP_ST
                        tscr[pl.ds(p * 256 + ri * 128 + a * NGRP + b, GROUP_ST, stride=NBLK), :] = block[top_row:top_row + GROUP_ST]
            return carry

        lax.fori_loop(0, half, turn, 0, unroll=8)

        def pack(p, carry):
            real = tscr[pl.ds(pl.multiple_of(p * 256, 256), 128), :].reshape(GROUP_ST, NBLK, LANES)
            imag = tscr[pl.ds(pl.multiple_of(p * 256 + 128, 128), 128), :].reshape(GROUP_ST, NBLK, LANES)
            q = lax.broadcasted_iota(I32, (GROUP_ST, NBLK, LANES), 0)
            ab = lax.broadcasted_iota(I32, (GROUP_ST, NBLK, LANES), 1)
            a, b = ab // NGRP, ab % NGRP
            upper = (a < b) | ((a == b) & (p <= q))
            tx3[pl.ds(p % 4 * GROUP_ST, GROUP_ST), p // 4] = jnp.where(upper, real, imag).astype(BF16)
            return carry

        lax.fori_loop(0, GROUP_ST, pack, 0, unroll=2)
        frame = tm // 2 * 2 * frames + c * frames + e

        def send(step, carry):
            d = (me + SLICES // 2 + step) % SLICES

            @pl.when(d != me)
            def _():
                remote(tx3.at[d], rx3.at[frame], s3.at[0], r3.at[0], place_of(d)).start()

            @pl.when(d == me)
            def _():
                pltpu.make_async_copy(tx3.at[d], rx3.at[frame], own_sems.at[3]).start()
            return carry

        lax.fori_loop(0, SLICES, send, 0, unroll=16)

    tell.wait()

    def picked(step, order):
        value = order[0]
        for i in range(1, len(order)):
            value = jnp.where(step == i, order[i], value)
        return value

    def across(k):
        return (tm + k) % 2 + (tm // 2 + k // 2) % 2 * 2 + (tm // 4 + k // 4) % 2 * 4

    @pl.when(me < SLICES)
    def _():
        @pl.when(e < frames)
        def _():
            pltpu.make_async_copy(tx3.at[0], rx3.at[0], own_sems.at[3]).wait()
            rest = rx3.at[pl.ds(0, all_frames - 1)]
            remote(rest, rest, s3.at[0], r3.at[0], (tm, pair)).wait_recv()

        @pl.when(e >= frames)
        def _():
            remote(rx3, rx3, s3.at[0], r3.at[0], (tm, pair)).wait_recv()

        sums[all_frames] = jnp.zeros((2 * NBLK, LANES), F32)

        def add(f, carry):
            sums[f] = sums[orders[f, 0]] + rx3[f].reshape(2 * NBLK, LANES).astype(F32)
            return carry

        lax.fori_loop(0, all_frames, add, 0, unroll=4)

        def give(step, carry):
            t = (tm + step) % owners
            for i in range(bins_here):
                held = sums[orders[all_frames + t * bins_here + i, 0]].astype(BF16)
                tx4[t, i * 2 * NBLK:(i + 1) * 2 * NBLK, :] = held

            @pl.when(t != tm)
            def _():
                remote(tx4.at[t], rx4.at[me], s4.at[0], r4.at[me], (t, pair)).start()
            return carry

        lax.fori_loop(1, owners + 1, give, 0, unroll=2)
        pltpu.make_async_copy(tx4.at[tm], rx4.at[me], own_sems.at[4]).start()

    sources = SLICES // pairs

    def pass_on(d, other):
        return remote(rx4.at[d], rx4.at[d], s5.at[0], r4.at[d], (tm, other))

    def landing(d):
        def one(i, carry):
            held = rx4[d, pl.ds(pl.multiple_of(i * NBLK, NBLK), NBLK), :].astype(F32)
            landed[pl.ds(i // 2 * NBLK * 2 * SLICES + i % 2 * SLICES + d, NBLK, stride=2 * SLICES), :] = held
            return carry

        lax.fori_loop(0, 2 * bins_here, one, 0, unroll=2 * bins_here)

    def nearest(step):
        if owners != 8:
            return (tm + step) % sources
        return across(picked(step, (0, 1, 2, 3, 4, 5, 6, 7)))

    def first_hop(step, carry):
        i = nearest(step)
        d = i * pairs + pair

        @pl.when(d == me)
        def _():
            pltpu.make_async_copy(tx4.at[tm], rx4.at[d], own_sems.at[4]).wait()

        @pl.when(d != me)
        def _():
            remote(rx4.at[d], rx4.at[d], s4.at[0], r4.at[d], (tm, pair)).wait_recv()

        for n in range(1, halves):
            pass_on(d, (pair + 2 * n) % pairs).start()
        pass_on(d, pair + 1 - 2 * c).start()
        landing(d)
        return carry

    lax.fori_loop(0, sources, first_hop, 0)

    def second_hop(step, carry):
        i = nearest(step)
        for n in range(1, halves):
            d = i * pairs + (pair + 2 * n) % pairs
            remote(rx4.at[d], rx4.at[d], s4.at[0], r4.at[d], (tm, pair)).wait_recv()
            pass_on(d, pair + 1 - 2 * c).start()
            landing(d)
        beside(i, 0)
        return carry

    def beside(i, n):
        d = i * pairs + (pair + 1 - 2 * c + 2 * n) % pairs
        remote(rx4.at[d], rx4.at[d], s4.at[0], r4.at[d], (tm, pair)).wait_recv()
        landing(d)

    lax.fori_loop(0, sources, second_hop, 0)

    def third_hop(step, carry):
        for n in range(1, halves):
            beside(nearest(step), n)
        return carry

    lax.fori_loop(0, sources, third_hop, 0)

    place = lax.broadcasted_iota(I32, (GROUP_ST, LANES), 0)
    none = jnp.zeros((GROUP_ST, LANES), I32)
    span = 2 * SLICES

    def one_bin(b, carry):
        for k in range(slots):
            block = assignment[k]
            a, bb = block // NGRP, block % NGRP
            row, column = none + a, none + bb
            ahead, within = row < column, row == column
            here = (b * NBLK + block) * span
            there = (b * NBLK + bb * NGRP + a) * span
            for p in range(GROUP_ST):
                straight = landed[pl.ds(here + p * GROUP_ST, GROUP_ST), :]
                mirrored = landed[pl.ds(there + p, GROUP_ST, stride=GROUP_ST), :]
                upper = ahead | (within & (place >= p))
                real = jnp.where(upper, straight, mirrored)
                imag = jnp.where(upper, -mirrored, straight)
                imag = jnp.where(within & (place == p), 0.0, imag)
                out[b, k, 0, p * GROUP_ST:(p + 1) * GROUP_ST, :] = real
                out[b, k, 1, p * GROUP_ST:(p + 1) * GROUP_ST, :] = imag
        return carry

    lax.fori_loop(0, bins_here, one_bin, 0)

    rest = rxb.at[pl.ds(0, owners - 1)]
    remote(rest, rest, s0.at[1], r0.at[1], (tm, pair)).wait_send()

    @pl.when(c != h)
    def _():
        delay_copy().wait_send()

    def all_sent(ref, count, sem):
        rest = ref.at[pl.ds(0, count)]
        remote(rest, rest, sem, r4.at[0], (tm, pair)).wait_send()

    @pl.when(is00)
    def _():
        all_sent(rxu, 4, s1.at[0])

        @pl.when(below)
        def _():
            all_sent(rxu, 6, s1.at[1])

        @pl.when(jnp.logical_not(top))
        def _():
            all_sent(rxu, 2, s1.at[2])

    @pl.when(is10)
    def _():
        all_sent(rxu, 4, s1.at[0])

        @pl.when(below)
        def _():
            all_sent(rxu, 4, s1.at[1])

        @pl.when(jnp.logical_not(top))
        def _():
            all_sent(rxu, 2, s1.at[2])

    @pl.when(c == 1)
    def _():
        all_sent(rxu, 4, s1.at[0])

    @pl.when(is11 & below)
    def _():
        all_sent(rxu, 2, s1.at[1])

    @pl.when(e < frames)
    def _():
        all_sent(tx2, frames - 1, s2.at[0])

        @pl.when(me < SLICES)
        def _():
            all_sent(tx3, SLICES - 1, s3.at[0])

        @pl.when(me >= SLICES)
        def _():
            all_sent(tx3, SLICES, s3.at[0])

    @pl.when(e >= frames)
    def _():
        all_sent(tx2, frames, s2.at[0])

    @pl.when(me < SLICES)
    def _():
        all_sent(tx4, owners - 1, s4.at[0])

    all_sent(rx4, sources * (2 * halves - 1), s5.at[0])


VMEM = pl.BlockSpec(memory_space=pltpu.VMEM)
SMEM = pl.BlockSpec(memory_space=pltpu.SMEM)
ANY = pl.BlockSpec(memory_space=pl.ANY)


def body(voltages, delays, phase_model, phase_bins, assignment):
    owners, pairs = lax.axis_size("tm"), lax.axis_size("pair")
    devices = owners * pairs
    stations, samples = voltages.shape[1], voltages.shape[2]
    frames = samples // NCHAN
    slots = assignment.shape[0]
    all_frames = owners * frames
    bins_here = BINS // owners
    sk = stations * RADIX_A

    first, twist, second = section_tables(stations)
    span = (frames + AHEAD) * UNIT
    scratch = [
        pltpu.VMEM((2, 1, LANES), I32),
        pltpu.VMEM(first.shape, BF16),
        pltpu.VMEM(twist.shape, F32),
        pltpu.VMEM(second.shape, BF16),
        pltpu.VMEM((frames + AHEAD, 2, stations, NCHAN), BF16),
        pltpu.VMEM((2 * stations * (span + 8), LANES), F32),
        pltpu.VMEM((2 * sk, RADIX_B), BF16),
        pltpu.VMEM((sk, 2 * RADIX_B), BF16),
        pltpu.VMEM((stations, LANES, LANES), F32),
        pltpu.VMEM((OUTCH * stations, LANES), F32),
        pltpu.VMEM((8, NCHAN), F32),
        pltpu.VMEM((8 * UNIT, LANES), F32),
        pltpu.VMEM((2, QUADS, sk, LANES), F32),
        pltpu.VMEM((frames, OUTCH, stations, LANES), BF16),
        pltpu.VMEM((pairs, OUTCH, stations, LANES), BF16),
        pltpu.VMEM((pairs * stations // 2 * OUTCH, LANES), F32),
        pltpu.VMEM((2 * pairs * stations * pairs * stations, LANES), F32),
        pltpu.VMEM((SLICES, 2, NBLK, LANES), BF16),
        pltpu.VMEM((all_frames, 2, NBLK, LANES), BF16),
        pltpu.VMEM((all_frames + 1, 2 * NBLK, LANES), F32),
        pltpu.VMEM((owners, bins_here * 2 * NBLK, LANES), BF16),
        pltpu.VMEM((SLICES, bins_here * 2 * NBLK, LANES), BF16),
        pltpu.VMEM((bins_here * NBLK * 2 * SLICES, LANES), F32),
        pltpu.VMEM((1, LANES), I32),
        pltpu.VMEM((owners, 1, LANES), I32),
        pltpu.SMEM((1, LANES), I32),
        pltpu.VMEM((all_frames + BINS, LANES), I32),
        pltpu.SMEM((all_frames + BINS, LANES), I32),
        pltpu.SemaphoreType.DMA((4,)),
        pltpu.SemaphoreType.DMA((2,)),
        pltpu.SemaphoreType.DMA((2,)),
        pltpu.SemaphoreType.DMA((3,)),
        pltpu.SemaphoreType.DMA((frames + AHEAD, 2)),
        pltpu.SemaphoreType.DMA((1,)),
        pltpu.SemaphoreType.DMA((OUTCH // PART,)),
        pltpu.SemaphoreType.DMA((1,)),
        pltpu.SemaphoreType.DMA((1,)),
        pltpu.SemaphoreType.DMA((1,)),
        pltpu.SemaphoreType.DMA((SLICES,)),
        pltpu.SemaphoreType.DMA((1,)),
        pltpu.SemaphoreType.DMA((7,)),
        pltpu.SemaphoreType.DMA((4, 2)),
        pltpu.SemaphoreType.REGULAR,
    ]
    result = pl.pallas_call(
        functools.partial(fused_kernel, (owners, pairs, frames, stations, slots)),
        out_shape=pltpu.VMEM((bins_here, slots, 2, GROUP_ST * GROUP_ST, OUTCH), F32),
        in_specs=[SMEM, SMEM, SMEM, ANY, ANY, ANY, ANY, ANY],
        out_specs=VMEM,
        scratch_shapes=scratch,
        compiler_params=pltpu.CompilerParams(
            collective_id=0, has_side_effects=True, vmem_limit_bytes=56 * 1024 * 1024),
        name="correlate",
    )(delays.T, phase_bins, assignment, voltages, phase_model, first, twist, second)
    return result


def solution(mesh):
    in_specs = (P(None, "pair", "tm"), P("pair", "tm"), P(), P("tm"), P("pair"))
    out_specs = P("tm", "pair", None, None, None)
    return jax.shard_map(body, mesh=mesh, in_specs=in_specs, out_specs=out_specs, check_vma=False)
```
